32 devices in a mesh: fsdp: 8 (over y, x, core), dp: 4 (over z).
Axes of the slice: x: 2, y: 2, z: 4, core: 2. Of those that a mesh axis runs over, the one named last changes fastest.
Arguments:
- hidden: bfloat16 [8192, 14336], P(('fsdp', 'dp')), may hold values from -6 to 6
- cotangent: bfloat16 [8192, 4096], P(('fsdp', 'dp')), may hold values from -6 to 6
- tiles: bfloat16 [64, 128, 128], P('fsdp'), may hold values from -0.25 to 0.25
- tile_rows: int32 [64], P('fsdp'), may hold values from 0 to 111, as said below
- tile_cols: int32 [64], P('fsdp'), may hold values from 0 to 31, as said below
- counts: int32 [8], P('fsdp'), may hold values from 1 to 8, as said below
Outputs:
- layer_out: bfloat16 [8192, 4096], P(('fsdp', 'dp'))
- hidden_grad: bfloat16 [8192, 14336], P(('fsdp', 'dp'))
- weight_grad: float32 [64, 128, 128], P('fsdp')
The draws below stay inside these ranges and needn't reach their ends.
Inputs may be any that keep to these rules, and one draw needn't show every extreme that they name: `tile_rows`: every slot (live or not) names a different block; the row block is below 112. `tile_cols`: the column block is below 32. `counts`: some owner has all 8 slots live in every draw.
All inputs are finite; a program needn't handle non-finite values.
Results may differ from the reference program's by a relative error of at most 0.0085.
Values may be sent and summed in bfloat16 or wider, within the bound.
A program may use at most 192 MiB of HBM per device.

```python
import math
import jax
import jax.numpy as jnp
from jax import lax

D = 4096
FF = 14336
TILE = 128
MAXB = 8
SLOTS = 64
TOKENS = 8192
N_FSDP = 8


def chosen_blocks(key):
    ordering = jax.random.permutation(jax.random.fold_in(key, 11), FF // TILE * (D // TILE))
    picked = ordering[:SLOTS].astype(jnp.int32)
    return jnp.sort(picked).astype(jnp.int32)


def draw_tile_rows(key, part):
    return (chosen_blocks(key) // (D // TILE)).astype(jnp.int32)


def draw_tile_cols(key, part):
    return (chosen_blocks(key) % (D // TILE)).astype(jnp.int32)


def draw_counts(key, part):
    drawn = jax.random.randint(jax.random.fold_in(key, 3), (N_FSDP,), 1, MAXB + 1)
    fullest = jax.random.randint(jax.random.fold_in(key, 5), (), 0, N_FSDP)
    return jnp.where(jnp.arange(N_FSDP) == fullest, MAXB, drawn).astype(jnp.int32)


def draw_hidden(key, part):
    own_key = jax.random.fold_in(key, 21)
    rough_key = jax.random.fold_in(key, 22)
    position = jnp.arange(FF, dtype=jnp.float32) / TILE
    level = jnp.floor(position) / max(FF // TILE - 1, 1)
    rough = jax.random.uniform(rough_key, (FF,), jnp.float32, 0.8, 1.25)
    column_scale = 0.6 * jnp.exp(level * jnp.log(2.0 / 0.6)) * rough
    values = jax.random.truncated_normal(own_key, -2.4, 2.4, (TOKENS, FF), jnp.float32) * column_scale[None, :]
    return values.astype(jnp.bfloat16)


def draw_cotangent(key, part):
    own_key = jax.random.fold_in(key, 23)
    values = jax.random.truncated_normal(own_key, -6.0, 6.0, (TOKENS, D), jnp.float32)
    return values.astype(jnp.bfloat16)


def block_scale(key, dims, cuts, low, high):
    level = 1.0
    for dim, shards_of in cuts:
        draws = jax.random.uniform(jax.random.fold_in(jax.random.fold_in(key, 6), dim), (shards_of,), jnp.float32, low / len(cuts), high / len(cuts))
        level = level * jnp.repeat(jnp.exp(draws), dims[dim] // shards_of).reshape((-1,) + (1,) * (len(dims) - 1 - dim))
    return level


def bell_draw(stream_key, dims, scale, limit, cuts=(), held_as=jnp.bfloat16):
    gain = block_scale(stream_key, dims, cuts, -0.22, 0.18) if cuts else 1.0
    array = jax.random.normal(stream_key, dims, jnp.float32) * scale * gain
    return jnp.minimum(jnp.maximum(array, -limit), limit).astype(held_as)


def setup_inputs(seed: int = 0) -> dict:
    arg_keys = jax.random.split(jax.random.key(seed), 7)
    return {
        "hidden": draw_hidden(jax.random.fold_in(arg_keys[6], 71), 0),
        "cotangent": draw_cotangent(jax.random.fold_in(arg_keys[6], 71), 0),
        "tiles": bell_draw(arg_keys[2], (SLOTS, TILE, TILE), (TILE * MAXB // 2) ** -0.5, 0.25, ((0, 8),)),
        "tile_rows": draw_tile_rows(jax.random.fold_in(arg_keys[6], 71), 0),
        "tile_cols": draw_tile_cols(jax.random.fold_in(arg_keys[6], 71), 0),
        "counts": draw_counts(jax.random.fold_in(arg_keys[6], 71), 0),
    }


def reference(hidden, cotangent, tiles, tile_rows, tile_cols, counts):
    slot_total = tiles.shape[0]
    per_owner = slot_total // N_FSDP
    edge_len = tiles.shape[1]
    slot_index = jnp.arange(slot_total, dtype=jnp.int32)
    live_slots = slot_index % per_owner < counts[slot_index // per_owner]
    masked = jnp.where(live_slots[:, None, None], tiles, jnp.zeros_like(tiles))

    def advance(totals, inputs_now):
        layer_acc, grad_acc = totals
        weight_block, row_id, col_id = inputs_now
        row_at = (row_id * edge_len).astype(jnp.int32)
        col_at = (col_id * edge_len).astype(jnp.int32)
        picked = lax.dynamic_slice_in_dim(hidden, row_at, edge_len, 1)
        upstream = lax.dynamic_slice_in_dim(cotangent, col_at, edge_len, 1)
        forward = jnp.dot(picked, weight_block, preferred_element_type=jnp.float32)
        layer_acc = lax.dynamic_update_slice_in_dim(layer_acc, lax.dynamic_slice_in_dim(layer_acc, col_at, edge_len, 1) + forward, col_at, 1)
        backward = jnp.dot(upstream, weight_block.T, preferred_element_type=jnp.float32)
        grad_acc = lax.dynamic_update_slice_in_dim(grad_acc, lax.dynamic_slice_in_dim(grad_acc, row_at, edge_len, 1) + backward, row_at, 1)
        weight_term = jnp.dot(picked.T, upstream, preferred_element_type=jnp.float32)
        return ((layer_acc, grad_acc), weight_term)
    start_totals = (jnp.zeros(cotangent.shape, jnp.float32), jnp.zeros(hidden.shape, jnp.float32))
    (layer_acc, grad_acc), weight_terms = lax.scan(advance, start_totals, (masked, tile_rows, tile_cols))
    raw_grad = jnp.where(live_slots[:, None, None], weight_terms, jnp.zeros_like(weight_terms))
    squares = jnp.sum(raw_grad * raw_grad)
    entries = jnp.sum(counts).astype(jnp.float32) * edge_len * edge_len
    spread = jnp.sqrt(squares / entries)
    root_tokens = math.sqrt(TOKENS)
    factor = jnp.minimum(1.0, 0.5 * root_tokens / spread) / root_tokens
    return (layer_acc.astype(jnp.bfloat16), grad_acc.astype(jnp.bfloat16), raw_grad * factor)
```

```python
import functools
import math

import jax
import jax.numpy as jnp
from jax import lax
from jax.experimental import pallas as pl
from jax.experimental.pallas import tpu as pltpu
from jax.sharding import PartitionSpec as P

MESH = pl.DeviceIdType.MESH
F32 = jnp.float32
BF16 = jnp.bfloat16


def exchange_kernel(
    n, dp, root,
    rows_s, cols_s, cnt_s, tiles_hbm, hid_hbm, cot_hbm,
    meta_out, tiles_out, wg_out,
    hid_v, cot_v, tiles_v, meta_v, meta_s, acc, sbuf, rbuf, fin, zs, zr, za, sqz, sqf,
    in_sem, out_sem, meta_ss, meta_rs, ag_ss, ag_rs, rs_ss, rs_rs,
    zs_ss, zs_rs, za_ss, za_rs, qz_ss, qz_rs, qf_ss, qf_rs,
):
    me = lax.axis_index("fsdp")
    z = lax.axis_index("dp")
    maxb, edge = tiles_hbm.shape[0], tiles_hbm.shape[1]
    half = maxb // 2
    per = maxb // dp
    stages = n.bit_length() - 1
    chip_bits = stages - 1
    orders = [list(range(1, stages)), list(range(stages - 1, 0, -1))]
    core = lax.rem(me, 2)

    def bit_of(b):
        return lax.rem(me // (2 ** b), 2)

    def flip(value_me, b):
        return value_me + (1 - 2 * bit_of(b)) * (2 ** b)

    def fetch(source, target, sem):
        def step(i, carry):
            at = pl.ds(pl.multiple_of(i * edge, edge), edge)
            pltpu.make_async_copy(source.at[:, at], target.at[i], sem).start()
            return carry
        lax.fori_loop(0, target.shape[0], step, 0)

    own_copy = pltpu.make_async_copy(tiles_hbm, tiles_v.at[me], in_sem.at[2])
    own_copy.start()
    fetch(cot_hbm, cot_v, in_sem.at[1])
    fetch(hid_hbm, hid_v, in_sem.at[0])

    barrier = pltpu.get_barrier_semaphore()
    for k in range(1, n):
        pl.semaphore_signal(
            barrier, inc=1, device_id={"fsdp": lax.rem(me + k, n)}, device_id_type=MESH
        )
    for k in range(1, dp):
        pl.semaphore_signal(
            barrier, inc=1, device_id={"dp": lax.rem(z + k, dp)}, device_id_type=MESH
        )
    lane = lax.broadcasted_iota(jnp.int32, (8, 128), 1)
    sub = lax.broadcasted_iota(jnp.int32, (8, 128), 0)
    meta = jnp.where(sub == 2, cnt_s[0], 0)
    for j in range(maxb):
        meta = jnp.where((sub == 0) & (lane == j), rows_s[j], meta)
        meta = jnp.where((sub == 1) & (lane == j), cols_s[j], meta)
    meta_v[me] = meta
    own_copy.wait()
    pl.semaphore_wait(barrier, n - 1 + dp - 1)

    meta_copies = []
    for k in range(1, n):
        copy = pltpu.make_async_remote_copy(
            meta_v.at[me], meta_v.at[me], meta_ss.at[k - 1], meta_rs.at[k - 1],
            device_id={"fsdp": lax.rem(me + k, n)}, device_id_type=MESH,
        )
        copy.start()
        meta_copies.append(copy)

    ag_copies = {}

    def ag_send(p, i, e):
        bits = orders[p] + [0]
        owner = me
        for t in range(len(bits)):
            if (e >> t) & 1:
                owner = flip(owner, bits[t])
        piece = tiles_v.at[owner, pl.ds(p * half, half)]
        where = 2 ** i - 1 + e
        copy = pltpu.make_async_remote_copy(
            piece, piece, ag_ss.at[p, where], ag_rs.at[p, where],
            device_id={"fsdp": flip(me, bits[i])}, device_id_type=MESH,
        )
        copy.start()
        ag_copies[p, i, e] = copy

    for i in range(stages):
        for p in range(2):
            ag_send(p, i, 0)

    for copy in meta_copies:
        copy.wait_recv()
    to_smem = pltpu.make_async_copy(meta_v, meta_s, in_sem.at[3])
    to_smem.start()
    to_smem.wait()
    meta_back = pltpu.make_async_copy(meta_v, meta_out, out_sem.at[0])
    meta_back.start()
    pltpu.make_async_copy(cot_v, cot_v, in_sem.at[1]).wait()
    pltpu.make_async_copy(hid_v, hid_v, in_sem.at[0]).wait()

    def owner_at(p, e, core_bit):
        owner = core_bit
        for t, b in enumerate(orders[p]):
            ebit = lax.rem(e // (2 ** (chip_bits - 1 - t)), 2)
            owner = owner + lax.rem(bit_of(b) + 1 + ebit, 2) * (2 ** b)
        return owner

    def term(owner, j):
        return lax.dot_general(
            hid_v[meta_s[owner, 0, j]], cot_v[meta_s[owner, 1, j]],
            (((0,), (0,)), ((), ())), preferred_element_type=F32,
        )

    chips = n // 2
    offsets = [0]
    for t in range(stages):
        offsets.append(offsets[-1] + (n >> (t + 1)))

    def rs_copy(p, t, e):
        where = offsets[t] + e
        bit = 0 if t == 0 else orders[p][t - 1]
        return pltpu.make_async_remote_copy(
            sbuf.at[p, where], rbuf.at[p, where], rs_ss.at[p, where], rs_rs.at[p, where],
            device_id={"fsdp": flip(me, bit)}, device_id_type=MESH,
        )

    def foreign(e, carry):
        for p in range(2):
            owner = owner_at(p, e, 1 - core)
            for j in range(half):
                sbuf[p, e, j] = term(owner, p * half + j).astype(BF16)
            rs_copy(p, 0, e).start()
        return carry

    lax.fori_loop(0, chips, foreign, 0)

    for i in range(chip_bits):
        for p in range(2):
            for e in range(2 ** i):
                ag_copies[p, i, e].wait_recv()
                for i2 in range(i + 1, stages):
                    ag_send(p, i2, e + 2 ** i)

    def own(e, carry):
        for p in range(2):
            owner = owner_at(p, e, core)
            for j in range(half):
                acc[p, e, j] = term(owner, p * half + j)
        return carry

    lax.fori_loop(0, chips, own, 0)

    start = 0
    for t in range(stages):
        m = n >> (t + 1)
        sent = m // 2
        for e in range(m):
            for p in range(2):
                rs_copy(p, t, e).wait_recv()
                total = acc[p, start + e] + rbuf[p, offsets[t] + e].astype(F32)
                if e < sent:
                    sbuf[p, offsets[t + 1] + e] = total.astype(BF16)
                    rs_copy(p, t + 1, e).start()
                elif m > 1:
                    acc[p, start + e] = total
                else:
                    fin[pl.ds(p * half, half)] = total
                    for q in range(half // per):
                        zs[p * (half // per) + q] = total[q * per:(q + 1) * per].astype(BF16)
        start += sent

    def z_peer(r):
        return lax.rem(z + r, dp)

    z_copies = []
    for r in range(1, dp):
        copy = pltpu.make_async_remote_copy(
            zs.at[z_peer(r)], zr.at[r - 1], zs_ss.at[r - 1], zs_rs.at[r - 1],
            device_id={"dp": z_peer(r)}, device_id_type=MESH,
        )
        copy.start()
        z_copies.append(copy)

    for p in range(2):
        for e in range(2 ** chip_bits):
            ag_copies[p, chip_bits, e].wait_recv()
    tiles_back = pltpu.make_async_copy(tiles_v, tiles_out, out_sem.at[1])
    tiles_back.start()

    piece = fin[pl.ds(z * per, per)]
    for r in range(1, dp):
        z_copies[r - 1].wait_recv()
        piece = piece + zr[r - 1].astype(F32)
    slot = z * per + lax.broadcasted_iota(jnp.int32, piece.shape, 0)
    piece = piece * jnp.clip(cnt_s[0] - slot, 0, 1).astype(F32)
    za[z] = piece.astype(BF16)
    sqz[z] = jnp.sum((piece * piece).reshape(-1, 8, 128), axis=0)
    a_copies, q_copies = [], []
    for r in range(1, dp):
        copy = pltpu.make_async_remote_copy(
            sqz.at[z], sqz.at[z], qz_ss.at[r - 1], qz_rs.at[r - 1],
            device_id={"dp": z_peer(r)}, device_id_type=MESH,
        )
        copy.start()
        q_copies.append(copy)
    for r in range(1, dp):
        copy = pltpu.make_async_remote_copy(
            za.at[z], za.at[z], za_ss.at[r - 1], za_rs.at[r - 1],
            device_id={"dp": z_peer(r)}, device_id_type=MESH,
        )
        copy.start()
        a_copies.append(copy)
    for copy in q_copies:
        copy.wait_recv()
    sqf[me] = jnp.sum(sqz[...], axis=0)
    f_copies = []
    for k in range(1, n):
        copy = pltpu.make_async_remote_copy(
            sqf.at[me], sqf.at[me], qf_ss.at[k - 1], qf_rs.at[k - 1],
            device_id={"fsdp": lax.rem(me + k, n)}, device_id_type=MESH,
        )
        copy.start()
        f_copies.append(copy)
    entries = meta_s[0, 2, 0]
    for k in range(1, n):
        entries = entries + meta_s[k, 2, 0]
    for copy in a_copies + f_copies:
        copy.wait_recv()
    squares = jnp.sum(jnp.sum(sqf[...], axis=0), axis=(0, 1), keepdims=True)
    live = jnp.full((1, 1), entries, jnp.int32).astype(F32) * edge * edge
    spread = jnp.sqrt(squares / live)
    factor = jnp.minimum(1.0, 0.5 * root / spread) / root
    for q in range(dp):
        for i in range(per):
            wg_out[q * per + i] = za[q, i].astype(F32) * factor

    for copy in meta_copies + list(ag_copies.values()) + z_copies + q_copies + a_copies + f_copies:
        copy.wait_send()
    for t in range(stages):
        for e in range(n >> (t + 1)):
            for p in range(2):
                rs_copy(p, t, e).wait_send()
    meta_back.wait()
    tiles_back.wait()


def project_kernel(
    n, maxb,
    meta_s, tiles_hbm, hid_hbm, cot_hbm,
    layer_hbm, grad_hbm,
    tiles_v, cot_v, hid_v, gacc, gout, lacc, lout, zero_v, values,
    row_left, row_seen, col_left, col_seen,
    in_sem, hid_sem, g_sem, l_sem,
):
    edge = zero_v.shape[1]
    tile_copy = pltpu.make_async_copy(tiles_hbm, tiles_v, in_sem.at[0])
    cot_copy = pltpu.make_async_copy(cot_hbm, cot_v, in_sem.at[1])
    tile_copy.start()
    cot_copy.start()
    zero_v[...] = jnp.zeros_like(zero_v)

    def clear(left, seen):
        def step(i, carry):
            left[i] = 0
            seen[i] = 0
            return carry
        lax.fori_loop(0, left.shape[0], step, 0)

    clear(row_left, row_seen)
    clear(col_left, col_seen)

    def columns(i):
        return pl.ds(pl.multiple_of(i * edge, edge), edge)

    def each_live(visit):
        def owner(o, carry):
            def slot(j, inner):
                visit(o, j, meta_s[o, 0, j], meta_s[o, 1, j])
                return inner
            return lax.fori_loop(0, meta_s[o, 2, 0], slot, carry)
        lax.fori_loop(0, n, owner, 0)

    def fetch(o, j, row, col):
        pltpu.make_async_copy(hid_hbm.at[:, columns(row)], hid_v.at[o, j], hid_sem).start()
        row_left[row] = row_left[row] + 1
        col_left[col] = col_left[col] + 1

    each_live(fetch)

    def blank(left, target, sem):
        def step(i, carry):
            @pl.when(left[i] == 0)
            def _():
                pltpu.make_async_copy(zero_v, target.at[:, columns(i)], sem).start()
            return carry
        lax.fori_loop(0, left.shape[0], step, 0)

    blank(row_left, grad_hbm, g_sem)
    blank(col_left, layer_hbm, l_sem)
    tile_copy.wait()
    cot_copy.wait()

    def add_block(at, value, left, seen, total, out, target, sem):
        remaining = left[at] - 1
        first = seen[at] == 0
        left[at] = remaining
        seen[at] = 1

        @pl.when(first & (remaining == 0))
        def _():
            out[at] = value[...].astype(BF16)

        @pl.when(first & (remaining > 0))
        def _():
            total[at] = value[...]

        @pl.when(jnp.logical_not(first))
        def _():
            summed = total[at] + value[...]
            total[at] = summed
            out[at] = summed.astype(BF16)

        @pl.when(remaining == 0)
        def _():
            pltpu.make_async_copy(out.at[at], target.at[:, columns(at)], sem).start()

    def backward(o, carry):
        for j in range(maxb):
            values[j] = lax.dot_general(
                cot_v[:, columns(meta_s[o, 1, j])], tiles_v[o, j], (((1,), (1,)), ((), ())),
                preferred_element_type=F32,
            )

        def slot(j, inner):
            add_block(
                meta_s[o, 0, j], values.at[j], row_left, row_seen, gacc, gout, grad_hbm, g_sem
            )
            return inner

        return lax.fori_loop(0, meta_s[o, 2, 0], slot, carry)

    lax.fori_loop(0, n, backward, 0)

    def arrived(o, j, row, col):
        pltpu.make_async_copy(hid_hbm.at[:, columns(row)], hid_v.at[o, j], hid_sem).wait()

    each_live(arrived)

    def forward(o, carry):
        for j in range(maxb):
            values[j] = jnp.dot(hid_v[o, j], tiles_v[o, j], preferred_element_type=F32)

        def slot(j, inner):
            add_block(
                meta_s[o, 1, j], values.at[j], col_left, col_seen, lacc, lout, layer_hbm, l_sem
            )
            return inner

        return lax.fori_loop(0, meta_s[o, 2, 0], slot, carry)

    lax.fori_loop(0, n, forward, 0)
    pltpu.make_async_copy(grad_hbm, grad_hbm, g_sem).wait()
    pltpu.make_async_copy(layer_hbm, layer_hbm, l_sem).wait()


def fused_kernel(
    n, dp, root,
    rows_s, cols_s, cnt_s, tiles_hbm, hid_hbm, cot_hbm,
    grad_out, layer_out, wg_out, table_out,
    hid_v, cot_v, tiles_v, meta_v, full_v, full_s, table_s,
    acc, sbuf, rbuf, fin, zs, zr, za, sqf, grad_q, layer_q,
    in_sem, meta_ss, meta_rs, ag_ss, ag_rs, rs_ss, rs_rs,
    zs_ss, zs_rs, za_ss, za_rs, sq_ss, sq_rs,
):
    me = lax.axis_index("fsdp")
    z = lax.axis_index("dp")
    maxb, edge = tiles_hbm.shape[0], tiles_hbm.shape[1]
    slots = n * maxb
    half = maxb // 2
    rows_z = 2 * edge // dp
    stages = n.bit_length() - 1
    chip_bits = stages - 1
    chips = n // 2
    orders = [list(range(1, stages)), list(range(stages - 1, 0, -1))]

    def bit_of(b):
        return lax.rem(me // (2 ** b), 2)

    def relative(x):
        other = me
        for b in range(stages):
            if (x >> b) & 1:
                other = other + (1 - 2 * bit_of(b)) * (2 ** b)
        return other

    def z_peer(r):
        return lax.rem(z + r, dp)

    def fetch(source, target, sem):
        def step(i, carry):
            at = pl.ds(pl.multiple_of(i * edge, edge), edge)
            pltpu.make_async_copy(source.at[:, at], target.at[i], sem).start()
            return carry
        lax.fori_loop(0, target.shape[0], step, 0)

    own_copy = pltpu.make_async_copy(tiles_hbm, tiles_v.at[0], in_sem.at[2])
    own_copy.start()
    barrier = pltpu.get_barrier_semaphore()
    for x in range(1, n):
        pl.semaphore_signal(
            barrier, inc=1, device_id={"fsdp": relative(x)}, device_id_type=MESH
        )
    for r in range(1, dp):
        pl.semaphore_signal(
            barrier, inc=1, device_id={"dp": z_peer(r)}, device_id_type=MESH
        )
    fetch(cot_hbm, cot_v, in_sem.at[1])
    fetch(hid_hbm, hid_v, in_sem.at[0])

    lane = lax.broadcasted_iota(jnp.int32, (8, 128), 1)
    sub = lax.broadcasted_iota(jnp.int32, (8, 128), 0)
    meta = jnp.where(sub == 2, cnt_s[0], 0)
    for j in range(maxb):
        here = lax.rem(lane, maxb) == j
        meta = jnp.where((sub == 0) & here, rows_s[j], meta)
        meta = jnp.where((sub == 1) & here, cols_s[j], meta)
    meta_v[0] = meta
    grad_q[slots] = jnp.zeros(grad_q.shape[1:], F32)
    layer_q[slots] = jnp.zeros(layer_q.shape[1:], F32)
    grad_out[slots] = jnp.zeros(grad_out.shape[1:], BF16)
    layer_out[slots] = jnp.zeros(layer_out.shape[1:], BF16)
    own_copy.wait()
    pl.semaphore_wait(barrier, n - 1 + dp - 1)

    meta_copies = []
    for x in range(1, n):
        copy = pltpu.make_async_remote_copy(
            meta_v.at[0], meta_v.at[x], meta_ss.at[x - 1], meta_rs.at[x - 1],
            device_id={"fsdp": relative(x)}, device_id_type=MESH,
        )
        copy.start()
        meta_copies.append(copy)

    ag_copies = {}
    ag_done = set()

    def ag_send(p, i, e):
        bits = orders[p] + [0]
        owner = 0
        for t in range(len(bits)):
            if (e >> t) & 1:
                owner |= 1 << bits[t]
        where = 2 ** i - 1 + e
        part = pl.ds(p * half, half)
        copy = pltpu.make_async_remote_copy(
            tiles_v.at[owner, part], tiles_v.at[owner | (1 << bits[i]), part],
            ag_ss.at[p, where], ag_rs.at[p, where],
            device_id={"fsdp": relative(1 << bits[i])}, device_id_type=MESH,
        )
        copy.start()
        ag_copies[p, i, e] = copy

    def ag_wait(p, i, e):
        if (p, i, e) not in ag_done:
            ag_done.add((p, i, e))
            ag_copies[p, i, e].wait_recv()

    for i in range(stages):
        for p in range(2):
            ag_send(p, i, 0)

    for copy in meta_copies:
        copy.wait_recv()
    full = jnp.zeros((8, 128), jnp.int32)
    for x in range(n):
        full = jnp.where(lane // maxb == x, meta_v[x], full)
    full_v[...] = full
    to_smem = pltpu.make_async_copy(full_v, full_s, in_sem.at[3])
    to_smem.start()

    wide = lax.broadcasted_iota(jnp.int32, (slots, 128), 1)
    tall = lax.broadcasted_iota(jnp.int32, (slots, 128), 0)
    alive = lax.rem(lane[0:1], maxb) < full[2:3]
    table = jnp.full((8, 128), slots, jnp.int32)
    for k in range(2):
        named = jnp.broadcast_to(jnp.where(alive, full[k:k + 1], -1), (slots, 128))
        named_t = jnp.sum(jnp.where(wide == tall, named, 0), axis=1, keepdims=True)
        before = jnp.max(
            jnp.where((named_t == named) & (tall < wide), tall, -1), axis=0, keepdims=True
        )
        last = jnp.max(jnp.where(named_t == wide, tall, -1), axis=0, keepdims=True)
        table = jnp.where(sub == k, jnp.where(before < 0, slots, before), table)
        table = jnp.where(sub == 2 + k, jnp.where(last < 0, slots, last), table)
    table_out[...] = table
    table_copy = pltpu.make_async_copy(table_out, table_s, in_sem.at[4])
    table_copy.start()
    to_smem.wait()
    pltpu.make_async_copy(cot_v, cot_v, in_sem.at[1]).wait()
    pltpu.make_async_copy(hid_v, hid_v, in_sem.at[0]).wait()

    def term(q):
        return lax.dot_general(
            hid_v[full_s[0, q]], cot_v[full_s[1, q]],
            (((0,), (0,)), ((), ())), preferred_element_type=F32,
        )

    def owner_at(p, e):
        owner = 0
        for t, b in enumerate(orders[p]):
            if not (e >> (chip_bits - 1 - t)) & 1:
                owner |= 1 << b
        return owner

    offsets = [0]
    for t in range(stages):
        offsets.append(offsets[-1] + (n >> (t + 1)))

    def rs_copy(p, t, e, c):
        where = offsets[t] + e
        bit = 0 if t == 0 else orders[p][t - 1]
        return pltpu.make_async_remote_copy(
            sbuf.at[p, where, c], rbuf.at[p, where, c],
            rs_ss.at[p, where, c], rs_rs.at[p, where, c],
            device_id={"fsdp": relative(1 << bit)}, device_id_type=MESH,
        )

    def foreign(c):
        for e in range(chips):
            for p in range(2):
                q = (owner_at(p, e) | 1) * maxb + p * half + c
                sbuf[p, e, c] = term(q).astype(BF16)
                rs_copy(p, 0, e, c).start()

    def own(c):
        for e in range(chips):
            for p in range(2):
                acc[p, e, c] = term(owner_at(p, e) * maxb + p * half + c)

    starts = [0]
    for t in range(stages):
        starts.append(starts[-1] + (n >> (t + 1)) // 2)

    def reduce_step(t, c):
        m = n >> (t + 1)
        for e in range(m):
            for p in range(2):
                rs_copy(p, t, e, c).wait_recv()
                total = acc[p, starts[t] + e, c] + rbuf[p, offsets[t] + e, c].astype(F32)
                if e < m // 2:
                    sbuf[p, offsets[t + 1] + e, c] = total.astype(BF16)
                    rs_copy(p, t + 1, e, c).start()
                elif m > 1:
                    acc[p, starts[t] + e, c] = total
                else:
                    at = pl.ds(p * edge, edge)
                    fin[c, at] = total
                    zs[c, at] = total.astype(BF16)
        if m == 1:
            for r in range(1, dp):
                z_copy(c, r).start()

    def z_rows(index):
        return pl.ds(pl.multiple_of(index * rows_z, rows_z), rows_z)

    def z_copy(c, r):
        return pltpu.make_async_remote_copy(
            zs.at[c, z_rows(z_peer(r))], zr.at[c, r - 1], zs_ss.at[c, r - 1], zs_rs.at[c, r - 1],
            device_id={"dp": z_peer(r)}, device_id_type=MESH,
        )

    def a_copy(c, r):
        return pltpu.make_async_remote_copy(
            za.at[c, z_rows(z)], za.at[c, z_rows(z)], za_ss.at[c, r - 1], za_rs.at[c, r - 1],
            device_id={"dp": z_peer(r)}, device_id_type=MESH,
        )

    def z_step(c, squares):
        piece = fin[c, z_rows(z)]
        for r in range(1, dp):
            z_copy(c, r).wait_recv()
            piece = piece + zr[c, r - 1].astype(F32)
        row = z * rows_z + lax.broadcasted_iota(jnp.int32, piece.shape, 0)
        slot = (row // edge) * half + c
        piece = piece * jnp.clip(cnt_s[0] - slot, 0, 1).astype(F32)
        za[c, z_rows(z)] = piece.astype(BF16)
        for r in range(1, dp):
            a_copy(c, r).start()
        return squares + jnp.sum((piece * piece).reshape(-1, 8, 128), axis=0)

    def project(x):
        def load(j):
            q = x * maxb + j
            backward = lax.dot_general(
                cot_v[full_s[1, q]], tiles_v[x, j], (((1,), (1,)), ((), ())),
                preferred_element_type=F32,
            )
            forward = jnp.dot(hid_v[full_s[0, q]], tiles_v[x, j], preferred_element_type=F32)
            return q, backward, forward
        for j in range(maxb):
            q, backward, forward = load(j)
            backward = backward + grad_q[table_s[0, q]]
            grad_q[q] = backward
            grad_out[q] = backward.astype(BF16)
            forward = forward + layer_q[table_s[1, q]]
            layer_q[q] = forward
            layer_out[q] = forward.astype(BF16)

    def arrived(x):
        for p in range(2):
            bits = orders[p] + [0]
            index = [t for t in range(stages) if (x >> bits[t]) & 1]
            if index:
                e = sum(1 << t for t in index[:-1])
                ag_wait(p, index[-1], e)

    foreign(0)

    def first(c, carry):
        @pl.when(c + 1 < half)
        def _():
            foreign(c + 1)
        own(c)
        reduce_step(0, c)
        return carry

    lax.fori_loop(0, half, first, 0)

    for i in range(chip_bits):
        for p in range(2):
            ag_wait(p, i, 0)
            ag_send(p, chip_bits, 2 ** i)
    table_copy.wait()
    early = [x for x in range(n) if bin(x >> 1).count("1") < 2]
    for x in early:
        arrived(x)

    def second(k, carry):
        project(k)
        reduce_step(1, k)
        return carry

    lax.fori_loop(0, half, second, 0)
    for i in range(1, chip_bits):
        for p in range(2):
            for e in range(1, 2 ** i):
                ag_wait(p, i - 1, e - 2 ** (i - 1))
                ag_send(p, i, e)

    def third(k, carry):
        @pl.when(half + k < len(early))
        def _():
            project(half + k)
        reduce_step(2, k)
        return carry

    lax.fori_loop(0, half, third, 0)

    for i in range(1, chip_bits):
        for p in range(2):
            for e in range(1, 2 ** i):
                ag_wait(p, i, e)
                ag_send(p, chip_bits, e + 2 ** i)

    squares = lax.fori_loop(0, half, z_step, jnp.zeros((8, 128), F32))
    place = me * dp + z
    sqf[place] = jnp.sum(squares, axis=0, keepdims=True)
    sq_copies = []
    for x in range(n):
        for r in range(dp):
            if x or r:
                copy = pltpu.make_async_remote_copy(
                    sqf.at[place], sqf.at[place], sq_ss, sq_rs,
                    device_id={"fsdp": relative(x), "dp": z_peer(r)}, device_id_type=MESH,
                )
                copy.start()
                sq_copies.append(copy)

    for x in range(len(early), n):
        arrived(x)

    def rest(x, carry):
        project(x)
        return carry

    lax.fori_loop(len(early), n, rest, 0)

    entries = full_s[2, 0]
    for x in range(1, n):
        entries = entries + full_s[2, x * maxb]
    others = sqf.at[pl.ds(0, n * dp - 1)]
    pltpu.make_async_copy(others, others, sq_rs).wait()
    squares = jnp.sum(jnp.sum(sqf[...], axis=0), axis=1, keepdims=True)
    live = jnp.full((1, 1), entries, jnp.int32).astype(F32) * edge * edge
    spread = jnp.sqrt(squares / live)
    factor = jnp.minimum(1.0, 0.5 * root / spread) / root

    def finish(c, carry):
        for r in range(1, dp):
            a_copy(c, r).wait_recv()
        for p in range(2):
            wg_out[p * half + c] = za[c, pl.ds(p * edge, edge)].astype(F32) * factor
        return carry

    lax.fori_loop(0, half, finish, 0)

    for copy in meta_copies + list(ag_copies.values()):
        copy.wait_send()
    pltpu.make_async_copy(others, others, sq_ss).wait()

    def drain(c, carry):
        for t in range(stages):
            for e in range(n >> (t + 1)):
                for p in range(2):
                    rs_copy(p, t, e, c).wait_send()
        for r in range(1, dp):
            z_copy(c, r).wait_send()
            a_copy(c, r).wait_send()
        return carry

    lax.fori_loop(0, half, drain, 0)


def write_kernel(
    grad_v, layer_v, wg_v, table_v,
    layer_hbm, grad_hbm, wg_hbm,
    table_s, t_sem, w_sem, g_sem, l_sem,
):
    edge = grad_v.shape[2]
    table_copy = pltpu.make_async_copy(table_v, table_s, t_sem)
    table_copy.start()
    wg_copy = pltpu.make_async_copy(wg_v, wg_hbm, w_sem)
    wg_copy.start()
    table_copy.wait()

    def write(row, source, target, sem):
        def step(i, carry):
            at = pl.ds(pl.multiple_of(i * edge, edge), edge)
            pltpu.make_async_copy(source.at[table_s[row, i]], target.at[:, at], sem).start()
            return carry
        lax.fori_loop(0, target.shape[1] // edge, step, 0)

    write(2, grad_v, grad_hbm, g_sem)
    write(3, layer_v, layer_hbm, l_sem)
    pltpu.make_async_copy(grad_hbm, grad_hbm, g_sem).wait()
    pltpu.make_async_copy(layer_hbm, layer_hbm, l_sem).wait()
    wg_copy.wait()


def fused(n, dp, hidden, cotangent, tiles, tile_rows, tile_cols, counts):
    tokens, width_ff = hidden.shape
    width_model = cotangent.shape[1]
    maxb, edge, _ = tiles.shape
    blocks_ff, blocks_model = width_ff // edge, width_model // edge
    root = math.sqrt(tokens * n * dp)
    slots, half = n * maxb, maxb // 2
    rows_z = 2 * edge // dp
    hbm = pl.BlockSpec(memory_space=pltpu.HBM)
    smem = pl.BlockSpec(memory_space=pltpu.SMEM)
    vmem = pl.BlockSpec(memory_space=pltpu.VMEM)
    dma = pltpu.SemaphoreType.DMA
    grad, layer, weight, table = pl.pallas_call(
        functools.partial(fused_kernel, n, dp, root),
        out_shape=(
            pltpu.VMEM((slots + 1, tokens, edge), BF16),
            pltpu.VMEM((slots + 1, tokens, edge), BF16),
            pltpu.VMEM((maxb, edge, edge), F32),
            pltpu.VMEM((8, 128), jnp.int32),
        ),
        in_specs=[smem, smem, smem, hbm, hbm, hbm],
        out_specs=(vmem, vmem, vmem, vmem),
        scratch_shapes=[
            pltpu.VMEM((blocks_ff, tokens, edge), BF16),
            pltpu.VMEM((blocks_model, tokens, edge), BF16),
            pltpu.VMEM((n, maxb, edge, edge), BF16),
            pltpu.VMEM((n, 8, 128), jnp.int32),
            pltpu.VMEM((8, 128), jnp.int32),
            pltpu.SMEM((8, 128), jnp.int32),
            pltpu.SMEM((8, 128), jnp.int32),
            pltpu.VMEM((2, n // 2, half, edge, edge), F32),
            pltpu.VMEM((2, n - 1, half, edge, edge), BF16),
            pltpu.VMEM((2, n - 1, half, edge, edge), BF16),
            pltpu.VMEM((half, 2 * edge, edge), F32),
            pltpu.VMEM((half, 2 * edge, edge), BF16),
            pltpu.VMEM((half, dp - 1, rows_z, edge), BF16),
            pltpu.VMEM((half, 2 * edge, edge), BF16),
            pltpu.VMEM((n * dp, 1, 128), F32),
            pltpu.VMEM((slots + 1, tokens, edge), F32),
            pltpu.VMEM((slots + 1, tokens, edge), F32),
            dma((5,)),
            dma((n - 1,)), dma((n - 1,)),
            dma((2, n - 1)), dma((2, n - 1)),
            dma((2, n - 1, half)), dma((2, n - 1, half)),
            dma((half, dp - 1)), dma((half, dp - 1)),
            dma((half, dp - 1)), dma((half, dp - 1)),
            dma, dma,
        ],
        compiler_params=pltpu.CompilerParams(
            collective_id=0, has_side_effects=True, vmem_limit_bytes=44 * 2 ** 20
        ),
        name="fused",
    )(tile_rows, tile_cols, counts, tiles, hidden, cotangent)
    return pl.pallas_call(
        write_kernel,
        out_shape=(
            jax.ShapeDtypeStruct(cotangent.shape, BF16),
            jax.ShapeDtypeStruct(hidden.shape, BF16),
            jax.ShapeDtypeStruct(tiles.shape, F32),
        ),
        in_specs=[vmem, vmem, vmem, vmem],
        out_specs=(hbm, hbm, hbm),
        scratch_shapes=[pltpu.SMEM((8, 128), jnp.int32), dma, dma, dma, dma],
        compiler_params=pltpu.CompilerParams(vmem_limit_bytes=16 * 2 ** 20),
        name="write",
    )(grad, layer, weight, table)


def shards(n, dp, hidden, cotangent, tiles, tile_rows, tile_cols, counts):
    tokens, width_ff = hidden.shape
    width_model = cotangent.shape[1]
    maxb, edge, _ = tiles.shape
    blocks_ff, blocks_model = width_ff // edge, width_model // edge
    root = math.sqrt(tokens * n * dp)
    half, per = maxb // 2, maxb // dp
    sums = n * maxb * tokens * edge * 12
    if n == 8 and dp % 2 == 0 and max(n * maxb, blocks_ff, blocks_model) <= 128 and sums <= 28 * 2 ** 20:
        return fused(n, dp, hidden, cotangent, tiles, tile_rows, tile_cols, counts)
    hbm = pl.BlockSpec(memory_space=pl.ANY)
    smem = pl.BlockSpec(memory_space=pltpu.SMEM)
    vmem = pl.BlockSpec(memory_space=pltpu.VMEM)
    dma = pltpu.SemaphoreType.DMA
    meta, gathered, weight_grad = pl.pallas_call(
        functools.partial(exchange_kernel, n, dp, root),
        out_shape=(
            jax.ShapeDtypeStruct((n, 8, 128), jnp.int32),
            jax.ShapeDtypeStruct((n, maxb, edge, edge), BF16),
            jax.ShapeDtypeStruct((maxb, edge, edge), F32),
        ),
        in_specs=[smem, smem, smem, hbm, hbm, hbm],
        out_specs=(hbm, hbm, vmem),
        scratch_shapes=[
            pltpu.VMEM((blocks_ff, tokens, edge), BF16),
            pltpu.VMEM((blocks_model, tokens, edge), BF16),
            pltpu.VMEM((n, maxb, edge, edge), BF16),
            pltpu.VMEM((n, 8, 128), jnp.int32),
            pltpu.SMEM((n, 8, 128), jnp.int32),
            pltpu.VMEM((2, n // 2, half, edge, edge), F32),
            pltpu.VMEM((2, n - 1, half, edge, edge), BF16),
            pltpu.VMEM((2, n - 1, half, edge, edge), BF16),
            pltpu.VMEM((maxb, edge, edge), F32),
            pltpu.VMEM((dp, per, edge, edge), BF16),
            pltpu.VMEM((dp - 1, per, edge, edge), BF16),
            pltpu.VMEM((dp, per, edge, edge), BF16),
            pltpu.VMEM((dp, 8, 128), F32),
            pltpu.VMEM((n, 8, 128), F32),
            dma((4,)), dma((2,)),
            dma((n - 1,)), dma((n - 1,)),
            dma((2, n - 1)), dma((2, n - 1)),
            dma((2, n - 1)), dma((2, n - 1)),
            dma((dp - 1,)), dma((dp - 1,)),
            dma((dp - 1,)), dma((dp - 1,)),
            dma((dp - 1,)), dma((dp - 1,)),
            dma((n - 1,)), dma((n - 1,)),
        ],
        compiler_params=pltpu.CompilerParams(
            collective_id=0, has_side_effects=True, vmem_limit_bytes=60 * 2 ** 20
        ),
        name="exchange",
    )(tile_rows, tile_cols, counts, tiles, hidden, cotangent)

    layer_out, hidden_grad = pl.pallas_call(
        functools.partial(project_kernel, n, maxb),
        out_shape=(
            jax.ShapeDtypeStruct(cotangent.shape, BF16),
            jax.ShapeDtypeStruct(hidden.shape, BF16),
        ),
        in_specs=[smem, hbm, hbm, hbm],
        out_specs=(hbm, hbm),
        scratch_shapes=[
            pltpu.VMEM((n, maxb, edge, edge), BF16),
            pltpu.VMEM(cotangent.shape, BF16),
            pltpu.VMEM((n, maxb, tokens, edge), BF16),
            pltpu.VMEM((blocks_ff, tokens, edge), F32),
            pltpu.VMEM((blocks_ff, tokens, edge), BF16),
            pltpu.VMEM((blocks_model, tokens, edge), F32),
            pltpu.VMEM((blocks_model, tokens, edge), BF16),
            pltpu.VMEM((tokens, edge), BF16),
            pltpu.VMEM((maxb, tokens, edge), F32),
            pltpu.SMEM((blocks_ff,), jnp.int32),
            pltpu.SMEM((blocks_ff,), jnp.int32),
            pltpu.SMEM((blocks_model,), jnp.int32),
            pltpu.SMEM((blocks_model,), jnp.int32),
            dma((2,)), dma, dma, dma,
        ],
        compiler_params=pltpu.CompilerParams(vmem_limit_bytes=62 * 2 ** 20),
        name="project",
    )(meta, gathered, hidden, cotangent)
    return layer_out, hidden_grad, weight_grad


def solution(mesh):
    placed = (
        P(("fsdp", "dp"), None),
        P(("fsdp", "dp"), None),
        P("fsdp", None, None),
        P("fsdp"),
        P("fsdp"),
        P("fsdp"),
    )
    return jax.shard_map(
        functools.partial(shards, mesh.shape["fsdp"], mesh.shape["dp"]),
        mesh=mesh,
        in_specs=placed,
        out_specs=(P(("fsdp", "dp"), None), P(("fsdp", "dp"), None), P("fsdp", None, None)),
        check_vma=False,
    )
```

```python
import functools
import math

import jax
import jax.numpy as jnp
from jax import lax
from jax.experimental import pallas as pl
from jax.experimental.pallas import tpu as pltpu
from jax.sharding import PartitionSpec as P

MESH = pl.DeviceIdType.MESH
F32 = jnp.float32
BF16 = jnp.bfloat16


def exchange_kernel(
    n, dp, root,
    rows_s, cols_s, cnt_s, tiles_hbm, hid_hbm, cot_hbm,
    meta_out, tiles_out, wg_out,
    hid_v, cot_v, tiles_v, meta_v, meta_s, acc, sbuf, rbuf, fin, zs, zr, za, sqz, sqf,
    in_sem, out_sem, meta_ss, meta_rs, ag_ss, ag_rs, rs_ss, rs_rs,
    zs_ss, zs_rs, za_ss, za_rs, qz_ss, qz_rs, qf_ss, qf_rs,
):
    me = lax.axis_index("fsdp")
    z = lax.axis_index("dp")
    maxb, edge = tiles_hbm.shape[0], tiles_hbm.shape[1]
    half = maxb // 2
    per = maxb // dp
    stages = n.bit_length() - 1
    chip_bits = stages - 1
    orders = [list(range(1, stages)), list(range(stages - 1, 0, -1))]
    core = lax.rem(me, 2)

    def bit_of(b):
        return lax.rem(me // (2 ** b), 2)

    def flip(value_me, b):
        return value_me + (1 - 2 * bit_of(b)) * (2 ** b)

    def fetch(source, target, sem):
        def step(i, carry):
            at = pl.ds(pl.multiple_of(i * edge, edge), edge)
            pltpu.make_async_copy(source.at[:, at], target.at[i], sem).start()
            return carry
        lax.fori_loop(0, target.shape[0], step, 0)

    own_copy = pltpu.make_async_copy(tiles_hbm, tiles_v.at[me], in_sem.at[2])
    own_copy.start()
    fetch(cot_hbm, cot_v, in_sem.at[1])
    fetch(hid_hbm, hid_v, in_sem.at[0])

    barrier = pltpu.get_barrier_semaphore()
    for k in range(1, n):
        pl.semaphore_signal(
            barrier, inc=1, device_id={"fsdp": lax.rem(me + k, n)}, device_id_type=MESH
        )
    for k in range(1, dp):
        pl.semaphore_signal(
            barrier, inc=1, device_id={"dp": lax.rem(z + k, dp)}, device_id_type=MESH
        )
    lane = lax.broadcasted_iota(jnp.int32, (8, 128), 1)
    sub = lax.broadcasted_iota(jnp.int32, (8, 128), 0)
    meta = jnp.where(sub == 2, cnt_s[0], 0)
    for j in range(maxb):
        meta = jnp.where((sub == 0) & (lane == j), rows_s[j], meta)
        meta = jnp.where((sub == 1) & (lane == j), cols_s[j], meta)
    meta_v[me] = meta
    own_copy.wait()
    pl.semaphore_wait(barrier, n - 1 + dp - 1)

    meta_copies = []
    for k in range(1, n):
        copy = pltpu.make_async_remote_copy(
            meta_v.at[me], meta_v.at[me], meta_ss.at[k - 1], meta_rs.at[k - 1],
            device_id={"fsdp": lax.rem(me + k, n)}, device_id_type=MESH,
        )
        copy.start()
        meta_copies.append(copy)

    ag_copies = {}

    def ag_send(p, i, e):
        bits = orders[p] + [0]
        owner = me
        for t in range(len(bits)):
            if (e >> t) & 1:
                owner = flip(owner, bits[t])
        piece = tiles_v.at[owner, pl.ds(p * half, half)]
        where = 2 ** i - 1 + e
        copy = pltpu.make_async_remote_copy(
            piece, piece, ag_ss.at[p, where], ag_rs.at[p, where],
            device_id={"fsdp": flip(me, bits[i])}, device_id_type=MESH,
        )
        copy.start()
        ag_copies[p, i, e] = copy

    for i in range(stages):
        for p in range(2):
            ag_send(p, i, 0)

    for copy in meta_copies:
        copy.wait_recv()
    to_smem = pltpu.make_async_copy(meta_v, meta_s, in_sem.at[3])
    to_smem.start()
    to_smem.wait()
    meta_back = pltpu.make_async_copy(meta_v, meta_out, out_sem.at[0])
    meta_back.start()
    pltpu.make_async_copy(cot_v, cot_v, in_sem.at[1]).wait()
    pltpu.make_async_copy(hid_v, hid_v, in_sem.at[0]).wait()

    def owner_at(p, e, core_bit):
        owner = core_bit
        for t, b in enumerate(orders[p]):
            ebit = lax.rem(e // (2 ** (chip_bits - 1 - t)), 2)
            owner = owner + lax.rem(bit_of(b) + 1 + ebit, 2) * (2 ** b)
        return owner

    def term(owner, j):
        return lax.dot_general(
            hid_v[meta_s[owner, 0, j]], cot_v[meta_s[owner, 1, j]],
            (((0,), (0,)), ((), ())), preferred_element_type=F32,
        )

    chips = n // 2
    offsets = [0]
    for t in range(stages):
        offsets.append(offsets[-1] + (n >> (t + 1)))

    def rs_copy(p, t, e):
        where = offsets[t] + e
        bit = 0 if t == 0 else orders[p][t - 1]
        return pltpu.make_async_remote_copy(
            sbuf.at[p, where], rbuf.at[p, where], rs_ss.at[p, where], rs_rs.at[p, where],
            device_id={"fsdp": flip(me, bit)}, device_id_type=MESH,
        )

    def foreign(e, carry):
        for p in range(2):
            owner = owner_at(p, e, 1 - core)
            for j in range(half):
                sbuf[p, e, j] = term(owner, p * half + j).astype(BF16)
            rs_copy(p, 0, e).start()
        return carry

    lax.fori_loop(0, chips, foreign, 0)

    for i in range(chip_bits):
        for p in range(2):
            for e in range(2 ** i):
                ag_copies[p, i, e].wait_recv()
                for i2 in range(i + 1, stages):
                    ag_send(p, i2, e + 2 ** i)

    def own(e, carry):
        for p in range(2):
            owner = owner_at(p, e, core)
            for j in range(half):
                acc[p, e, j] = term(owner, p * half + j)
        return carry

    lax.fori_loop(0, chips, own, 0)

    start = 0
    for t in range(stages):
        m = n >> (t + 1)
        sent = m // 2
        for e in range(m):
            for p in range(2):
                rs_copy(p, t, e).wait_recv()
                total = acc[p, start + e] + rbuf[p, offsets[t] + e].astype(F32)
                if e < sent:
                    sbuf[p, offsets[t + 1] + e] = total.astype(BF16)
                    rs_copy(p, t + 1, e).start()
                elif m > 1:
                    acc[p, start + e] = total
                else:
                    fin[pl.ds(p * half, half)] = total
                    for q in range(half // per):
                        zs[p * (half // per) + q] = total[q * per:(q + 1) * per].astype(BF16)
        start += sent

    def z_peer(r):
        return lax.rem(z + r, dp)

    z_copies = []
    for r in range(1, dp):
        copy = pltpu.make_async_remote_copy(
            zs.at[z_peer(r)], zr.at[r - 1], zs_ss.at[r - 1], zs_rs.at[r - 1],
            device_id={"dp": z_peer(r)}, device_id_type=MESH,
        )
        copy.start()
        z_copies.append(copy)

    for p in range(2):
        for e in range(2 ** chip_bits):
            ag_copies[p, chip_bits, e].wait_recv()
    tiles_back = pltpu.make_async_copy(tiles_v, tiles_out, out_sem.at[1])
    tiles_back.start()

    piece = fin[pl.ds(z * per, per)]
    for r in range(1, dp):
        z_copies[r - 1].wait_recv()
        piece = piece + zr[r - 1].astype(F32)
    slot = z * per + lax.broadcasted_iota(jnp.int32, piece.shape, 0)
    piece = piece * jnp.clip(cnt_s[0] - slot, 0, 1).astype(F32)
    za[z] = piece.astype(BF16)
    sqz[z] = jnp.sum((piece * piece).reshape(-1, 8, 128), axis=0)
    a_copies, q_copies = [], []
    for r in range(1, dp):
        copy = pltpu.make_async_remote_copy(
            sqz.at[z], sqz.at[z], qz_ss.at[r - 1], qz_rs.at[r - 1],
            device_id={"dp": z_peer(r)}, device_id_type=MESH,
        )
        copy.start()
        q_copies.append(copy)
    for r in range(1, dp):
        copy = pltpu.make_async_remote_copy(
            za.at[z], za.at[z], za_ss.at[r - 1], za_rs.at[r - 1],
            device_id={"dp": z_peer(r)}, device_id_type=MESH,
        )
        copy.start()
        a_copies.append(copy)
    for copy in q_copies:
        copy.wait_recv()
    sqf[me] = jnp.sum(sqz[...], axis=0)
    f_copies = []
    for k in range(1, n):
        copy = pltpu.make_async_remote_copy(
            sqf.at[me], sqf.at[me], qf_ss.at[k - 1], qf_rs.at[k - 1],
            device_id={"fsdp": lax.rem(me + k, n)}, device_id_type=MESH,
        )
        copy.start()
        f_copies.append(copy)
    entries = meta_s[0, 2, 0]
    for k in range(1, n):
        entries = entries + meta_s[k, 2, 0]
    for copy in a_copies + f_copies:
        copy.wait_recv()
    squares = jnp.sum(jnp.sum(sqf[...], axis=0), axis=(0, 1), keepdims=True)
    live = jnp.full((1, 1), entries, jnp.int32).astype(F32) * edge * edge
    spread = jnp.sqrt(squares / live)
    factor = jnp.minimum(1.0, 0.5 * root / spread) / root
    for q in range(dp):
        for i in range(per):
            wg_out[q * per + i] = za[q, i].astype(F32) * factor

    for copy in meta_copies + list(ag_copies.values()) + z_copies + q_copies + a_copies + f_copies:
        copy.wait_send()
    for t in range(stages):
        for e in range(n >> (t + 1)):
            for p in range(2):
                rs_copy(p, t, e).wait_send()
    meta_back.wait()
    tiles_back.wait()


def project_kernel(
    n, maxb,
    meta_s, tiles_hbm, hid_hbm, cot_hbm,
    layer_hbm, grad_hbm,
    tiles_v, cot_v, hid_v, gacc, gout, lacc, lout, zero_v, values,
    row_left, row_seen, col_left, col_seen,
    in_sem, hid_sem, g_sem, l_sem,
):
    edge = zero_v.shape[1]
    tile_copy = pltpu.make_async_copy(tiles_hbm, tiles_v, in_sem.at[0])
    cot_copy = pltpu.make_async_copy(cot_hbm, cot_v, in_sem.at[1])
    tile_copy.start()
    cot_copy.start()
    zero_v[...] = jnp.zeros_like(zero_v)

    def clear(left, seen):
        def step(i, carry):
            left[i] = 0
            seen[i] = 0
            return carry
        lax.fori_loop(0, left.shape[0], step, 0)

    clear(row_left, row_seen)
    clear(col_left, col_seen)

    def columns(i):
        return pl.ds(pl.multiple_of(i * edge, edge), edge)

    def each_live(visit):
        def owner(o, carry):
            def slot(j, inner):
                visit(o, j, meta_s[o, 0, j], meta_s[o, 1, j])
                return inner
            return lax.fori_loop(0, meta_s[o, 2, 0], slot, carry)
        lax.fori_loop(0, n, owner, 0)

    def fetch(o, j, row, col):
        pltpu.make_async_copy(hid_hbm.at[:, columns(row)], hid_v.at[o, j], hid_sem).start()
        row_left[row] = row_left[row] + 1
        col_left[col] = col_left[col] + 1

    each_live(fetch)

    def blank(left, target, sem):
        def step(i, carry):
            @pl.when(left[i] == 0)
            def _():
                pltpu.make_async_copy(zero_v, target.at[:, columns(i)], sem).start()
            return carry
        lax.fori_loop(0, left.shape[0], step, 0)

    blank(row_left, grad_hbm, g_sem)
    blank(col_left, layer_hbm, l_sem)
    tile_copy.wait()
    cot_copy.wait()

    def add_block(at, value, left, seen, total, out, target, sem):
        remaining = left[at] - 1
        first = seen[at] == 0
        left[at] = remaining
        seen[at] = 1

        @pl.when(first & (remaining == 0))
        def _():
            out[at] = value[...].astype(BF16)

        @pl.when(first & (remaining > 0))
        def _():
            total[at] = value[...]

        @pl.when(jnp.logical_not(first))
        def _():
            summed = total[at] + value[...]
            total[at] = summed
            out[at] = summed.astype(BF16)

        @pl.when(remaining == 0)
        def _():
            pltpu.make_async_copy(out.at[at], target.at[:, columns(at)], sem).start()

    def backward(o, carry):
        for j in range(maxb):
            values[j] = lax.dot_general(
                cot_v[:, columns(meta_s[o, 1, j])], tiles_v[o, j], (((1,), (1,)), ((), ())),
                preferred_element_type=F32,
            )

        def slot(j, inner):
            add_block(
                meta_s[o, 0, j], values.at[j], row_left, row_seen, gacc, gout, grad_hbm, g_sem
            )
            return inner

        return lax.fori_loop(0, meta_s[o, 2, 0], slot, carry)

    lax.fori_loop(0, n, backward, 0)

    def arrived(o, j, row, col):
        pltpu.make_async_copy(hid_hbm.at[:, columns(row)], hid_v.at[o, j], hid_sem).wait()

    each_live(arrived)

    def forward(o, carry):
        for j in range(maxb):
            values[j] = jnp.dot(hid_v[o, j], tiles_v[o, j], preferred_element_type=F32)

        def slot(j, inner):
            add_block(
                meta_s[o, 1, j], values.at[j], col_left, col_seen, lacc, lout, layer_hbm, l_sem
            )
            return inner

        return lax.fori_loop(0, meta_s[o, 2, 0], slot, carry)

    lax.fori_loop(0, n, forward, 0)
    pltpu.make_async_copy(grad_hbm, grad_hbm, g_sem).wait()
    pltpu.make_async_copy(layer_hbm, layer_hbm, l_sem).wait()


def fused_kernel(
    n, dp, root,
    rows_hbm, cols_hbm, cnt_s, tiles_hbm, hid_hbm, cot_hbm,
    grad_out, layer_out, wg_out, table_out,
    rows_s, cols_s, hid_v, cot_v, tiles_v, meta_v, full_v, full_s, table_s,
    acc, sbuf, rbuf, fin, zs, zr, za, sqf, grad_q, layer_q,
    in_sem, meta_ss, meta_rs, ag_ss, ag_rs, rs_ss, rs_rs,
    zs_ss, zs_rs, za_ss, za_rs, sq_ss, sq_rs,
):
    me = lax.axis_index("fsdp")
    z = lax.axis_index("dp")
    maxb, edge = tiles_hbm.shape[0], tiles_hbm.shape[1]
    slots = n * maxb
    half = maxb // 2
    rows_z = 2 * edge // dp
    stages = n.bit_length() - 1
    chip_bits = stages - 1
    chips = n // 2
    orders = [list(range(1, stages)), list(range(stages - 1, 0, -1))]

    def bit_of(b):
        return lax.rem(me // (2 ** b), 2)

    def relative(x):
        other = me
        for b in range(stages):
            if (x >> b) & 1:
                other = other + (1 - 2 * bit_of(b)) * (2 ** b)
        return other

    def z_peer(r):
        return lax.rem(z + r, dp)

    def fetch(source, target, sem):
        def step(i, carry):
            at = pl.ds(pl.multiple_of(i * edge, edge), edge)
            pltpu.make_async_copy(source.at[:, at], target.at[i], sem).start()
            return carry
        lax.fori_loop(0, target.shape[0], step, 0)

    rows_copy = pltpu.make_async_copy(rows_hbm, rows_s, in_sem.at[5])
    rows_copy.start()
    cols_copy = pltpu.make_async_copy(cols_hbm, cols_s, in_sem.at[6])
    cols_copy.start()
    own_copy = pltpu.make_async_copy(tiles_hbm, tiles_v.at[0], in_sem.at[2])
    own_copy.start()
    barrier = pltpu.get_barrier_semaphore()
    for x in range(1, n):
        pl.semaphore_signal(
            barrier, inc=1, device_id={"fsdp": relative(x)}, device_id_type=MESH
        )
    for r in range(1, dp):
        pl.semaphore_signal(
            barrier, inc=1, device_id={"dp": z_peer(r)}, device_id_type=MESH
        )
    fetch(cot_hbm, cot_v, in_sem.at[1])
    fetch(hid_hbm, hid_v, in_sem.at[0])

    lane = lax.broadcasted_iota(jnp.int32, (8, 128), 1)
    sub = lax.broadcasted_iota(jnp.int32, (8, 128), 0)
    meta = jnp.where(sub == 2, cnt_s[0], 0)
    rows_copy.wait()
    cols_copy.wait()
    for j in range(maxb):
        here = lax.rem(lane, maxb) == j
        meta = jnp.where((sub == 0) & here, rows_s[j], meta)
        meta = jnp.where((sub == 1) & here, cols_s[j], meta)
    meta_v[0] = meta
    grad_q[slots] = jnp.zeros(grad_q.shape[1:], F32)
    layer_q[slots] = jnp.zeros(layer_q.shape[1:], F32)
    grad_out[slots] = jnp.zeros(grad_out.shape[1:], BF16)
    layer_out[slots] = jnp.zeros(layer_out.shape[1:], BF16)
    own_copy.wait()
    pl.semaphore_wait(barrier, n - 1 + dp - 1)

    meta_copies = []
    for x in range(1, n):
        copy = pltpu.make_async_remote_copy(
            meta_v.at[0], meta_v.at[x], meta_ss.at[x - 1], meta_rs.at[x - 1],
            device_id={"fsdp": relative(x)}, device_id_type=MESH,
        )
        copy.start()
        meta_copies.append(copy)

    ag_copies = {}
    ag_done = set()

    def ag_send(p, i, e):
        bits = orders[p] + [0]
        owner = 0
        for t in range(len(bits)):
            if (e >> t) & 1:
                owner |= 1 << bits[t]
        where = 2 ** i - 1 + e
        part = pl.ds(p * half, half)
        copy = pltpu.make_async_remote_copy(
            tiles_v.at[owner, part], tiles_v.at[owner | (1 << bits[i]), part],
            ag_ss.at[p, where], ag_rs.at[p, where],
            device_id={"fsdp": relative(1 << bits[i])}, device_id_type=MESH,
        )
        copy.start()
        ag_copies[p, i, e] = copy

    def ag_wait(p, i, e):
        if (p, i, e) not in ag_done:
            ag_done.add((p, i, e))
            ag_copies[p, i, e].wait_recv()

    for i in range(stages):
        for p in range(2):
            ag_send(p, i, 0)

    for copy in meta_copies:
        copy.wait_recv()
    full = jnp.zeros((8, 128), jnp.int32)
    for x in range(n):
        full = jnp.where(lane // maxb == x, meta_v[x], full)
    full_v[...] = full
    to_smem = pltpu.make_async_copy(full_v, full_s, in_sem.at[3])
    to_smem.start()

    wide = lax.broadcasted_iota(jnp.int32, (slots, 128), 1)
    tall = lax.broadcasted_iota(jnp.int32, (slots, 128), 0)
    alive = lax.rem(lane[0:1], maxb) < full[2:3]
    table = jnp.full((8, 128), slots, jnp.int32)
    for k in range(2):
        named = jnp.broadcast_to(jnp.where(alive, full[k:k + 1], -1), (slots, 128))
        named_t = jnp.sum(jnp.where(wide == tall, named, 0), axis=1, keepdims=True)
        before = jnp.max(
            jnp.where((named_t == named) & (tall < wide), tall, -1), axis=0, keepdims=True
        )
        last = jnp.max(jnp.where(named_t == wide, tall, -1), axis=0, keepdims=True)
        table = jnp.where(sub == k, jnp.where(before < 0, slots, before), table)
        table = jnp.where(sub == 2 + k, jnp.where(last < 0, slots, last), table)
    table_out[...] = table
    table_copy = pltpu.make_async_copy(table_out, table_s, in_sem.at[4])
    table_copy.start()
    to_smem.wait()
    pltpu.make_async_copy(cot_v, cot_v, in_sem.at[1]).wait()
    pltpu.make_async_copy(hid_v, hid_v, in_sem.at[0]).wait()

    def term(q):
        return lax.dot_general(
            hid_v[full_s[0, q]], cot_v[full_s[1, q]],
            (((0,), (0,)), ((), ())), preferred_element_type=F32,
        )

    def owner_at(p, e):
        owner = 0
        for t, b in enumerate(orders[p]):
            if not (e >> (chip_bits - 1 - t)) & 1:
                owner |= 1 << b
        return owner

    offsets = [0]
    for t in range(stages):
        offsets.append(offsets[-1] + (n >> (t + 1)))

    def rs_copy(p, t, e, c):
        where = offsets[t] + e
        bit = 0 if t == 0 else orders[p][t - 1]
        return pltpu.make_async_remote_copy(
            sbuf.at[p, where, c], rbuf.at[p, where, c],
            rs_ss.at[p, where, c], rs_rs.at[p, where, c],
            device_id={"fsdp": relative(1 << bit)}, device_id_type=MESH,
        )

    def foreign(c):
        for e in range(chips):
            for p in range(2):
                q = (owner_at(p, e) | 1) * maxb + p * half + c
                sbuf[p, e, c] = term(q).astype(BF16)
                rs_copy(p, 0, e, c).start()

    def own(c):
        for e in range(chips):
            for p in range(2):
                acc[p, e, c] = term(owner_at(p, e) * maxb + p * half + c)

    starts = [0]
    for t in range(stages):
        starts.append(starts[-1] + (n >> (t + 1)) // 2)

    def reduce_step(t, c):
        m = n >> (t + 1)
        for e in range(m):
            for p in range(2):
                rs_copy(p, t, e, c).wait_recv()
                total = acc[p, starts[t] + e, c] + rbuf[p, offsets[t] + e, c].astype(F32)
                if e < m // 2:
                    sbuf[p, offsets[t + 1] + e, c] = total.astype(BF16)
                    rs_copy(p, t + 1, e, c).start()
                elif m > 1:
                    acc[p, starts[t] + e, c] = total
                else:
                    at = pl.ds(p * edge, edge)
                    fin[c, at] = total
                    zs[c, at] = total.astype(BF16)
        if m == 1:
            for r in range(1, dp):
                z_copy(c, r).start()

    def z_rows(index):
        return pl.ds(pl.multiple_of(index * rows_z, rows_z), rows_z)

    def z_copy(c, r):
        return pltpu.make_async_remote_copy(
            zs.at[c, z_rows(z_peer(r))], zr.at[c, r - 1], zs_ss.at[c, r - 1], zs_rs.at[c, r - 1],
            device_id={"dp": z_peer(r)}, device_id_type=MESH,
        )

    def a_copy(c, r):
        return pltpu.make_async_remote_copy(
            za.at[c, z_rows(z)], za.at[c, z_rows(z)], za_ss.at[c, r - 1], za_rs.at[c, r - 1],
            device_id={"dp": z_peer(r)}, device_id_type=MESH,
        )

    def z_step(c, squares):
        piece = fin[c, z_rows(z)]
        for r in range(1, dp):
            z_copy(c, r).wait_recv()
            piece = piece + zr[c, r - 1].astype(F32)
        row = z * rows_z + lax.broadcasted_iota(jnp.int32, piece.shape, 0)
        slot = (row // edge) * half + c
        piece = piece * jnp.clip(cnt_s[0] - slot, 0, 1).astype(F32)
        za[c, z_rows(z)] = piece.astype(BF16)
        for r in range(1, dp):
            a_copy(c, r).start()
        return squares + jnp.sum((piece * piece).reshape(-1, 8, 128), axis=0)

    def project(x):
        def load(j):
            q = x * maxb + j
            backward = lax.dot_general(
                cot_v[full_s[1, q]], tiles_v[x, j], (((1,), (1,)), ((), ())),
                preferred_element_type=F32,
            )
            forward = jnp.dot(hid_v[full_s[0, q]], tiles_v[x, j], preferred_element_type=F32)
            return q, backward, forward
        for j in range(maxb):
            q, backward, forward = load(j)
            backward = backward + grad_q[table_s[0, q]]
            grad_q[q] = backward
            grad_out[q] = backward.astype(BF16)
            forward = forward + layer_q[table_s[1, q]]
            layer_q[q] = forward
            layer_out[q] = forward.astype(BF16)

    def arrived(x):
        for p in range(2):
            bits = orders[p] + [0]
            index = [t for t in range(stages) if (x >> bits[t]) & 1]
            if index:
                e = sum(1 << t for t in index[:-1])
                ag_wait(p, index[-1], e)

    foreign(0)

    def first(c, carry):
        @pl.when(c + 1 < half)
        def _():
            foreign(c + 1)
        own(c)
        reduce_step(0, c)
        return carry

    lax.fori_loop(0, half, first, 0)

    for i in range(chip_bits):
        for p in range(2):
            ag_wait(p, i, 0)
            ag_send(p, chip_bits, 2 ** i)
    table_copy.wait()
    early = [x for x in range(n) if bin(x >> 1).count("1") < 2]
    for x in early:
        arrived(x)

    def second(k, carry):
        project(k)
        reduce_step(1, k)
        return carry

    lax.fori_loop(0, half, second, 0)
    for i in range(1, chip_bits):
        for p in range(2):
            for e in range(1, 2 ** i):
                ag_wait(p, i - 1, e - 2 ** (i - 1))
                ag_send(p, i, e)

    def third(k, carry):
        @pl.when(half + k < len(early))
        def _():
            project(half + k)
        reduce_step(2, k)
        return carry

    lax.fori_loop(0, half, third, 0)

    for i in range(1, chip_bits):
        for p in range(2):
            for e in range(1, 2 ** i):
                ag_wait(p, i, e)
                ag_send(p, chip_bits, e + 2 ** i)

    squares = lax.fori_loop(0, half, z_step, jnp.zeros((8, 128), F32))
    place = me * dp + z
    sqf[place] = jnp.sum(squares, axis=0, keepdims=True)
    sq_copies = []
    for x in range(n):
        for r in range(dp):
            if x or r:
                copy = pltpu.make_async_remote_copy(
                    sqf.at[place], sqf.at[place], sq_ss, sq_rs,
                    device_id={"fsdp": relative(x), "dp": z_peer(r)}, device_id_type=MESH,
                )
                copy.start()
                sq_copies.append(copy)

    for x in range(len(early), n):
        arrived(x)

    def rest(x, carry):
        project(x)
        return carry

    lax.fori_loop(len(early), n, rest, 0)

    entries = full_s[2, 0]
    for x in range(1, n):
        entries = entries + full_s[2, x * maxb]
    others = sqf.at[pl.ds(0, n * dp - 1)]
    pltpu.make_async_copy(others, others, sq_rs).wait()
    squares = jnp.sum(jnp.sum(sqf[...], axis=0), axis=1, keepdims=True)
    live = jnp.full((1, 1), entries, jnp.int32).astype(F32) * edge * edge
    spread = jnp.sqrt(squares / live)
    factor = jnp.minimum(1.0, 0.5 * root / spread) / root

    def finish(c, carry):
        for r in range(1, dp):
            a_copy(c, r).wait_recv()
        for p in range(2):
            wg_out[p * half + c] = za[c, pl.ds(p * edge, edge)].astype(F32) * factor
        return carry

    lax.fori_loop(0, half, finish, 0)

    for copy in meta_copies + list(ag_copies.values()):
        copy.wait_send()
    pltpu.make_async_copy(others, others, sq_ss).wait()

    def drain(c, carry):
        for t in range(stages):
            for e in range(n >> (t + 1)):
                for p in range(2):
                    rs_copy(p, t, e, c).wait_send()
        for r in range(1, dp):
            z_copy(c, r).wait_send()
            a_copy(c, r).wait_send()
        return carry

    lax.fori_loop(0, half, drain, 0)


def write_kernel(
    grad_v, layer_v, wg_v, table_v,
    layer_hbm, grad_hbm, wg_hbm,
    table_s, t_sem, w_sem, g_sem, l_sem,
):
    edge = grad_v.shape[2]
    table_copy = pltpu.make_async_copy(table_v, table_s, t_sem)
    table_copy.start()
    wg_copy = pltpu.make_async_copy(wg_v, wg_hbm, w_sem)
    wg_copy.start()
    table_copy.wait()

    def write(row, source, target, sem):
        def step(i, carry):
            at = pl.ds(pl.multiple_of(i * edge, edge), edge)
            pltpu.make_async_copy(source.at[table_s[row, i]], target.at[:, at], sem).start()
            return carry
        lax.fori_loop(0, target.shape[1] // edge, step, 0)

    write(2, grad_v, grad_hbm, g_sem)
    write(3, layer_v, layer_hbm, l_sem)
    pltpu.make_async_copy(grad_hbm, grad_hbm, g_sem).wait()
    pltpu.make_async_copy(layer_hbm, layer_hbm, l_sem).wait()
    wg_copy.wait()


def fused(n, dp, hidden, cotangent, tiles, tile_rows, tile_cols, counts):
    tokens, width_ff = hidden.shape
    width_model = cotangent.shape[1]
    maxb, edge, _ = tiles.shape
    blocks_ff, blocks_model = width_ff // edge, width_model // edge
    root = math.sqrt(tokens * n * dp)
    slots, half = n * maxb, maxb // 2
    in_hbm = functools.partial(pltpu.with_memory_space_constraint, memory_space=pltpu.HBM)
    rows_z = 2 * edge // dp
    hbm = pl.BlockSpec(memory_space=pltpu.HBM)
    smem = pl.BlockSpec(memory_space=pltpu.SMEM)
    vmem = pl.BlockSpec(memory_space=pltpu.VMEM)
    dma = pltpu.SemaphoreType.DMA
    grad, layer, weight, table = pl.pallas_call(
        functools.partial(fused_kernel, n, dp, root),
        out_shape=(
            pltpu.VMEM((slots + 1, tokens, edge), BF16),
            pltpu.VMEM((slots + 1, tokens, edge), BF16),
            pltpu.VMEM((maxb, edge, edge), F32),
            pltpu.VMEM((8, 128), jnp.int32),
        ),
        in_specs=[hbm, hbm, smem, hbm, hbm, hbm],
        out_specs=(vmem, vmem, vmem, vmem),
        scratch_shapes=[
            pltpu.SMEM(tile_rows.shape, jnp.int32),
            pltpu.SMEM(tile_cols.shape, jnp.int32),
            pltpu.VMEM((blocks_ff, tokens, edge), BF16),
            pltpu.VMEM((blocks_model, tokens, edge), BF16),
            pltpu.VMEM((n, maxb, edge, edge), BF16),
            pltpu.VMEM((n, 8, 128), jnp.int32),
            pltpu.VMEM((8, 128), jnp.int32),
            pltpu.SMEM((8, 128), jnp.int32),
            pltpu.SMEM((8, 128), jnp.int32),
            pltpu.VMEM((2, n // 2, half, edge, edge), F32),
            pltpu.VMEM((2, n - 1, half, edge, edge), BF16),
            pltpu.VMEM((2, n - 1, half, edge, edge), BF16),
            pltpu.VMEM((half, 2 * edge, edge), F32),
            pltpu.VMEM((half, 2 * edge, edge), BF16),
            pltpu.VMEM((half, dp - 1, rows_z, edge), BF16),
            pltpu.VMEM((half, 2 * edge, edge), BF16),
            pltpu.VMEM((n * dp, 1, 128), F32),
            pltpu.VMEM((slots + 1, tokens, edge), F32),
            pltpu.VMEM((slots + 1, tokens, edge), F32),
            dma((7,)),
            dma((n - 1,)), dma((n - 1,)),
            dma((2, n - 1)), dma((2, n - 1)),
            dma((2, n - 1, half)), dma((2, n - 1, half)),
            dma((half, dp - 1)), dma((half, dp - 1)),
            dma((half, dp - 1)), dma((half, dp - 1)),
            dma, dma,
        ],
        compiler_params=pltpu.CompilerParams(
            collective_id=0, has_side_effects=True, vmem_limit_bytes=44 * 2 ** 20
        ),
        name="fused",
    )(in_hbm(tile_rows), in_hbm(tile_cols), counts, in_hbm(tiles), in_hbm(hidden), in_hbm(cotangent))
    return pl.pallas_call(
        write_kernel,
        out_shape=(
            jax.ShapeDtypeStruct(cotangent.shape, BF16),
            jax.ShapeDtypeStruct(hidden.shape, BF16),
            jax.ShapeDtypeStruct(tiles.shape, F32),
        ),
        in_specs=[vmem, vmem, vmem, vmem],
        out_specs=(hbm, hbm, hbm),
        scratch_shapes=[pltpu.SMEM((8, 128), jnp.int32), dma, dma, dma, dma],
        compiler_params=pltpu.CompilerParams(vmem_limit_bytes=16 * 2 ** 20),
        name="write",
    )(grad, layer, weight, table)


def shards(n, dp, hidden, cotangent, tiles, tile_rows, tile_cols, counts):
    tokens, width_ff = hidden.shape
    width_model = cotangent.shape[1]
    maxb, edge, _ = tiles.shape
    blocks_ff, blocks_model = width_ff // edge, width_model // edge
    root = math.sqrt(tokens * n * dp)
    half, per = maxb // 2, maxb // dp
    sums = n * maxb * tokens * edge * 12
    if n == 8 and dp % 2 == 0 and max(n * maxb, blocks_ff, blocks_model) <= 128 and sums <= 28 * 2 ** 20:
        return fused(n, dp, hidden, cotangent, tiles, tile_rows, tile_cols, counts)
    hbm = pl.BlockSpec(memory_space=pl.ANY)
    smem = pl.BlockSpec(memory_space=pltpu.SMEM)
    vmem = pl.BlockSpec(memory_space=pltpu.VMEM)
    dma = pltpu.SemaphoreType.DMA
    meta, gathered, weight_grad = pl.pallas_call(
        functools.partial(exchange_kernel, n, dp, root),
        out_shape=(
            jax.ShapeDtypeStruct((n, 8, 128), jnp.int32),
            jax.ShapeDtypeStruct((n, maxb, edge, edge), BF16),
            jax.ShapeDtypeStruct((maxb, edge, edge), F32),
        ),
        in_specs=[smem, smem, smem, hbm, hbm, hbm],
        out_specs=(hbm, hbm, vmem),
        scratch_shapes=[
            pltpu.VMEM((blocks_ff, tokens, edge), BF16),
            pltpu.VMEM((blocks_model, tokens, edge), BF16),
            pltpu.VMEM((n, maxb, edge, edge), BF16),
            pltpu.VMEM((n, 8, 128), jnp.int32),
            pltpu.SMEM((n, 8, 128), jnp.int32),
            pltpu.VMEM((2, n // 2, half, edge, edge), F32),
            pltpu.VMEM((2, n - 1, half, edge, edge), BF16),
            pltpu.VMEM((2, n - 1, half, edge, edge), BF16),
            pltpu.VMEM((maxb, edge, edge), F32),
            pltpu.VMEM((dp, per, edge, edge), BF16),
            pltpu.VMEM((dp - 1, per, edge, edge), BF16),
            pltpu.VMEM((dp, per, edge, edge), BF16),
            pltpu.VMEM((dp, 8, 128), F32),
            pltpu.VMEM((n, 8, 128), F32),
            dma((4,)), dma((2,)),
            dma((n - 1,)), dma((n - 1,)),
            dma((2, n - 1)), dma((2, n - 1)),
            dma((2, n - 1)), dma((2, n - 1)),
            dma((dp - 1,)), dma((dp - 1,)),
            dma((dp - 1,)), dma((dp - 1,)),
            dma((dp - 1,)), dma((dp - 1,)),
            dma((n - 1,)), dma((n - 1,)),
        ],
        compiler_params=pltpu.CompilerParams(
            collective_id=0, has_side_effects=True, vmem_limit_bytes=60 * 2 ** 20
        ),
        name="exchange",
    )(tile_rows, tile_cols, counts, tiles, hidden, cotangent)

    layer_out, hidden_grad = pl.pallas_call(
        functools.partial(project_kernel, n, maxb),
        out_shape=(
            jax.ShapeDtypeStruct(cotangent.shape, BF16),
            jax.ShapeDtypeStruct(hidden.shape, BF16),
        ),
        in_specs=[smem, hbm, hbm, hbm],
        out_specs=(hbm, hbm),
        scratch_shapes=[
            pltpu.VMEM((n, maxb, edge, edge), BF16),
            pltpu.VMEM(cotangent.shape, BF16),
            pltpu.VMEM((n, maxb, tokens, edge), BF16),
            pltpu.VMEM((blocks_ff, tokens, edge), F32),
            pltpu.VMEM((blocks_ff, tokens, edge), BF16),
            pltpu.VMEM((blocks_model, tokens, edge), F32),
            pltpu.VMEM((blocks_model, tokens, edge), BF16),
            pltpu.VMEM((tokens, edge), BF16),
            pltpu.VMEM((maxb, tokens, edge), F32),
            pltpu.SMEM((blocks_ff,), jnp.int32),
            pltpu.SMEM((blocks_ff,), jnp.int32),
            pltpu.SMEM((blocks_model,), jnp.int32),
            pltpu.SMEM((blocks_model,), jnp.int32),
            dma((2,)), dma, dma, dma,
        ],
        compiler_params=pltpu.CompilerParams(vmem_limit_bytes=62 * 2 ** 20),
        name="project",
    )(meta, gathered, hidden, cotangent)
    return layer_out, hidden_grad, weight_grad


def solution(mesh):
    placed = (
        P(("fsdp", "dp"), None),
        P(("fsdp", "dp"), None),
        P("fsdp", None, None),
        P("fsdp"),
        P("fsdp"),
        P("fsdp"),
    )
    return jax.shard_map(
        functools.partial(shards, mesh.shape["fsdp"], mesh.shape["dp"]),
        mesh=mesh,
        in_specs=placed,
        out_specs=(P(("fsdp", "dp"), None), P(("fsdp", "dp"), None), P("fsdp", None, None)),
        check_vma=False,
    )
```

```python
import functools
import math

import jax
import jax.numpy as jnp
from jax import lax
from jax.experimental import pallas as pl
from jax.experimental.pallas import tpu as pltpu
from jax.sharding import PartitionSpec as P

MESH = pl.DeviceIdType.MESH
F32 = jnp.float32
BF16 = jnp.bfloat16


def exchange_kernel(
    n, dp, root,
    rows_s, cols_s, cnt_s, tiles_hbm, hid_hbm, cot_hbm,
    meta_out, tiles_out, wg_out,
    hid_v, cot_v, tiles_v, meta_v, meta_s, acc, sbuf, rbuf, fin, zs, zr, za, sqz, sqf,
    in_sem, out_sem, meta_ss, meta_rs, ag_ss, ag_rs, rs_ss, rs_rs,
    zs_ss, zs_rs, za_ss, za_rs, qz_ss, qz_rs, qf_ss, qf_rs,
):
    me = lax.axis_index("fsdp")
    z = lax.axis_index("dp")
    maxb, edge = tiles_hbm.shape[0], tiles_hbm.shape[1]
    half = maxb // 2
    per = maxb // dp
    stages = n.bit_length() - 1
    chip_bits = stages - 1
    orders = [list(range(1, stages)), list(range(stages - 1, 0, -1))]
    core = lax.rem(me, 2)

    def bit_of(b):
        return lax.rem(me // (2 ** b), 2)

    def flip(value_me, b):
        return value_me + (1 - 2 * bit_of(b)) * (2 ** b)

    def fetch(source, target, sem):
        def step(i, carry):
            at = pl.ds(pl.multiple_of(i * edge, edge), edge)
            pltpu.make_async_copy(source.at[:, at], target.at[i], sem).start()
            return carry
        lax.fori_loop(0, target.shape[0], step, 0)

    own_copy = pltpu.make_async_copy(tiles_hbm, tiles_v.at[me], in_sem.at[2])
    own_copy.start()
    fetch(cot_hbm, cot_v, in_sem.at[1])
    fetch(hid_hbm, hid_v, in_sem.at[0])

    barrier = pltpu.get_barrier_semaphore()
    for k in range(1, n):
        pl.semaphore_signal(
            barrier, inc=1, device_id={"fsdp": lax.rem(me + k, n)}, device_id_type=MESH
        )
    for k in range(1, dp):
        pl.semaphore_signal(
            barrier, inc=1, device_id={"dp": lax.rem(z + k, dp)}, device_id_type=MESH
        )
    lane = lax.broadcasted_iota(jnp.int32, (8, 128), 1)
    sub = lax.broadcasted_iota(jnp.int32, (8, 128), 0)
    meta = jnp.where(sub == 2, cnt_s[0], 0)
    for j in range(maxb):
        meta = jnp.where((sub == 0) & (lane == j), rows_s[j], meta)
        meta = jnp.where((sub == 1) & (lane == j), cols_s[j], meta)
    meta_v[me] = meta
    own_copy.wait()
    pl.semaphore_wait(barrier, n - 1 + dp - 1)

    meta_copies = []
    for k in range(1, n):
        copy = pltpu.make_async_remote_copy(
            meta_v.at[me], meta_v.at[me], meta_ss.at[k - 1], meta_rs.at[k - 1],
            device_id={"fsdp": lax.rem(me + k, n)}, device_id_type=MESH,
        )
        copy.start()
        meta_copies.append(copy)

    ag_copies = {}

    def ag_send(p, i, e):
        bits = orders[p] + [0]
        owner = me
        for t in range(len(bits)):
            if (e >> t) & 1:
                owner = flip(owner, bits[t])
        piece = tiles_v.at[owner, pl.ds(p * half, half)]
        where = 2 ** i - 1 + e
        copy = pltpu.make_async_remote_copy(
            piece, piece, ag_ss.at[p, where], ag_rs.at[p, where],
            device_id={"fsdp": flip(me, bits[i])}, device_id_type=MESH,
        )
        copy.start()
        ag_copies[p, i, e] = copy

    for i in range(stages):
        for p in range(2):
            ag_send(p, i, 0)

    for copy in meta_copies:
        copy.wait_recv()
    to_smem = pltpu.make_async_copy(meta_v, meta_s, in_sem.at[3])
    to_smem.start()
    to_smem.wait()
    meta_back = pltpu.make_async_copy(meta_v, meta_out, out_sem.at[0])
    meta_back.start()
    pltpu.make_async_copy(cot_v, cot_v, in_sem.at[1]).wait()
    pltpu.make_async_copy(hid_v, hid_v, in_sem.at[0]).wait()

    def owner_at(p, e, core_bit):
        owner = core_bit
        for t, b in enumerate(orders[p]):
            ebit = lax.rem(e // (2 ** (chip_bits - 1 - t)), 2)
            owner = owner + lax.rem(bit_of(b) + 1 + ebit, 2) * (2 ** b)
        return owner

    def term(owner, j):
        return lax.dot_general(
            hid_v[meta_s[owner, 0, j]], cot_v[meta_s[owner, 1, j]],
            (((0,), (0,)), ((), ())), preferred_element_type=F32,
        )

    chips = n // 2
    offsets = [0]
    for t in range(stages):
        offsets.append(offsets[-1] + (n >> (t + 1)))

    def rs_copy(p, t, e):
        where = offsets[t] + e
        bit = 0 if t == 0 else orders[p][t - 1]
        return pltpu.make_async_remote_copy(
            sbuf.at[p, where], rbuf.at[p, where], rs_ss.at[p, where], rs_rs.at[p, where],
            device_id={"fsdp": flip(me, bit)}, device_id_type=MESH,
        )

    def foreign(e, carry):
        for p in range(2):
            owner = owner_at(p, e, 1 - core)
            for j in range(half):
                sbuf[p, e, j] = term(owner, p * half + j).astype(BF16)
            rs_copy(p, 0, e).start()
        return carry

    lax.fori_loop(0, chips, foreign, 0)

    for i in range(chip_bits):
        for p in range(2):
            for e in range(2 ** i):
                ag_copies[p, i, e].wait_recv()
                for i2 in range(i + 1, stages):
                    ag_send(p, i2, e + 2 ** i)

    def own(e, carry):
        for p in range(2):
            owner = owner_at(p, e, core)
            for j in range(half):
                acc[p, e, j] = term(owner, p * half + j)
        return carry

    lax.fori_loop(0, chips, own, 0)

    start = 0
    for t in range(stages):
        m = n >> (t + 1)
        sent = m // 2
        for e in range(m):
            for p in range(2):
                rs_copy(p, t, e).wait_recv()
                total = acc[p, start + e] + rbuf[p, offsets[t] + e].astype(F32)
                if e < sent:
                    sbuf[p, offsets[t + 1] + e] = total.astype(BF16)
                    rs_copy(p, t + 1, e).start()
                elif m > 1:
                    acc[p, start + e] = total
                else:
                    fin[pl.ds(p * half, half)] = total
                    for q in range(half // per):
                        zs[p * (half // per) + q] = total[q * per:(q + 1) * per].astype(BF16)
        start += sent

    def z_peer(r):
        return lax.rem(z + r, dp)

    z_copies = []
    for r in range(1, dp):
        copy = pltpu.make_async_remote_copy(
            zs.at[z_peer(r)], zr.at[r - 1], zs_ss.at[r - 1], zs_rs.at[r - 1],
            device_id={"dp": z_peer(r)}, device_id_type=MESH,
        )
        copy.start()
        z_copies.append(copy)

    for p in range(2):
        for e in range(2 ** chip_bits):
            ag_copies[p, chip_bits, e].wait_recv()
    tiles_back = pltpu.make_async_copy(tiles_v, tiles_out, out_sem.at[1])
    tiles_back.start()

    piece = fin[pl.ds(z * per, per)]
    for r in range(1, dp):
        z_copies[r - 1].wait_recv()
        piece = piece + zr[r - 1].astype(F32)
    slot = z * per + lax.broadcasted_iota(jnp.int32, piece.shape, 0)
    piece = piece * jnp.clip(cnt_s[0] - slot, 0, 1).astype(F32)
    za[z] = piece.astype(BF16)
    sqz[z] = jnp.sum((piece * piece).reshape(-1, 8, 128), axis=0)
    a_copies, q_copies = [], []
    for r in range(1, dp):
        copy = pltpu.make_async_remote_copy(
            sqz.at[z], sqz.at[z], qz_ss.at[r - 1], qz_rs.at[r - 1],
            device_id={"dp": z_peer(r)}, device_id_type=MESH,
        )
        copy.start()
        q_copies.append(copy)
    for r in range(1, dp):
        copy = pltpu.make_async_remote_copy(
            za.at[z], za.at[z], za_ss.at[r - 1], za_rs.at[r - 1],
            device_id={"dp": z_peer(r)}, device_id_type=MESH,
        )
        copy.start()
        a_copies.append(copy)
    for copy in q_copies:
        copy.wait_recv()
    sqf[me] = jnp.sum(sqz[...], axis=0)
    f_copies = []
    for k in range(1, n):
        copy = pltpu.make_async_remote_copy(
            sqf.at[me], sqf.at[me], qf_ss.at[k - 1], qf_rs.at[k - 1],
            device_id={"fsdp": lax.rem(me + k, n)}, device_id_type=MESH,
        )
        copy.start()
        f_copies.append(copy)
    entries = meta_s[0, 2, 0]
    for k in range(1, n):
        entries = entries + meta_s[k, 2, 0]
    for copy in a_copies + f_copies:
        copy.wait_recv()
    squares = jnp.sum(jnp.sum(sqf[...], axis=0), axis=(0, 1), keepdims=True)
    live = jnp.full((1, 1), entries, jnp.int32).astype(F32) * edge * edge
    spread = jnp.sqrt(squares / live)
    factor = jnp.minimum(1.0, 0.5 * root / spread) / root
    for q in range(dp):
        for i in range(per):
            wg_out[q * per + i] = za[q, i].astype(F32) * factor

    for copy in meta_copies + list(ag_copies.values()) + z_copies + q_copies + a_copies + f_copies:
        copy.wait_send()
    for t in range(stages):
        for e in range(n >> (t + 1)):
            for p in range(2):
                rs_copy(p, t, e).wait_send()
    meta_back.wait()
    tiles_back.wait()


def project_kernel(
    n, maxb,
    meta_s, tiles_hbm, hid_hbm, cot_hbm,
    layer_hbm, grad_hbm,
    tiles_v, cot_v, hid_v, gacc, gout, lacc, lout, zero_v, values,
    row_left, row_seen, col_left, col_seen,
    in_sem, hid_sem, g_sem, l_sem,
):
    edge = zero_v.shape[1]
    tile_copy = pltpu.make_async_copy(tiles_hbm, tiles_v, in_sem.at[0])
    cot_copy = pltpu.make_async_copy(cot_hbm, cot_v, in_sem.at[1])
    tile_copy.start()
    cot_copy.start()
    zero_v[...] = jnp.zeros_like(zero_v)

    def clear(left, seen):
        def step(i, carry):
            left[i] = 0
            seen[i] = 0
            return carry
        lax.fori_loop(0, left.shape[0], step, 0)

    clear(row_left, row_seen)
    clear(col_left, col_seen)

    def columns(i):
        return pl.ds(pl.multiple_of(i * edge, edge), edge)

    def each_live(visit):
        def owner(o, carry):
            def slot(j, inner):
                visit(o, j, meta_s[o, 0, j], meta_s[o, 1, j])
                return inner
            return lax.fori_loop(0, meta_s[o, 2, 0], slot, carry)
        lax.fori_loop(0, n, owner, 0)

    def fetch(o, j, row, col):
        pltpu.make_async_copy(hid_hbm.at[:, columns(row)], hid_v.at[o, j], hid_sem).start()
        row_left[row] = row_left[row] + 1
        col_left[col] = col_left[col] + 1

    each_live(fetch)

    def blank(left, target, sem):
        def step(i, carry):
            @pl.when(left[i] == 0)
            def _():
                pltpu.make_async_copy(zero_v, target.at[:, columns(i)], sem).start()
            return carry
        lax.fori_loop(0, left.shape[0], step, 0)

    blank(row_left, grad_hbm, g_sem)
    blank(col_left, layer_hbm, l_sem)
    tile_copy.wait()
    cot_copy.wait()

    def add_block(at, value, left, seen, total, out, target, sem):
        remaining = left[at] - 1
        first = seen[at] == 0
        left[at] = remaining
        seen[at] = 1

        @pl.when(first & (remaining == 0))
        def _():
            out[at] = value[...].astype(BF16)

        @pl.when(first & (remaining > 0))
        def _():
            total[at] = value[...]

        @pl.when(jnp.logical_not(first))
        def _():
            summed = total[at] + value[...]
            total[at] = summed
            out[at] = summed.astype(BF16)

        @pl.when(remaining == 0)
        def _():
            pltpu.make_async_copy(out.at[at], target.at[:, columns(at)], sem).start()

    def backward(o, carry):
        for j in range(maxb):
            values[j] = lax.dot_general(
                cot_v[:, columns(meta_s[o, 1, j])], tiles_v[o, j], (((1,), (1,)), ((), ())),
                preferred_element_type=F32,
            )

        def slot(j, inner):
            add_block(
                meta_s[o, 0, j], values.at[j], row_left, row_seen, gacc, gout, grad_hbm, g_sem
            )
            return inner

        return lax.fori_loop(0, meta_s[o, 2, 0], slot, carry)

    lax.fori_loop(0, n, backward, 0)

    def arrived(o, j, row, col):
        pltpu.make_async_copy(hid_hbm.at[:, columns(row)], hid_v.at[o, j], hid_sem).wait()

    each_live(arrived)

    def forward(o, carry):
        for j in range(maxb):
            values[j] = jnp.dot(hid_v[o, j], tiles_v[o, j], preferred_element_type=F32)

        def slot(j, inner):
            add_block(
                meta_s[o, 1, j], values.at[j], col_left, col_seen, lacc, lout, layer_hbm, l_sem
            )
            return inner

        return lax.fori_loop(0, meta_s[o, 2, 0], slot, carry)

    lax.fori_loop(0, n, forward, 0)
    pltpu.make_async_copy(grad_hbm, grad_hbm, g_sem).wait()
    pltpu.make_async_copy(layer_hbm, layer_hbm, l_sem).wait()


def fused_kernel(
    n, dp, root,
    rows_hbm, cols_hbm, cnt_s, tiles_hbm, hid_hbm, cot_hbm,
    grad_out, layer_out, wg_out, table_out,
    rows_s, cols_s, hid_v, cot_v, tiles_v, meta_v, full_v, full_s, table_s,
    acc, sbuf, rbuf, fin, zs, zr, za, sqf, grad_q, layer_q,
    in_sem, meta_ss, meta_rs, ag_ss, ag_rs, rs_ss, rs_rs,
    zs_ss, zs_rs, za_ss, za_rs, sq_ss, sq_rs,
):
    me = lax.axis_index("fsdp")
    z = lax.axis_index("dp")
    maxb, edge = tiles_hbm.shape[0], tiles_hbm.shape[1]
    slots = n * maxb
    half = maxb // 2
    rows_z = 2 * edge // dp
    stages = n.bit_length() - 1
    chip_bits = stages - 1
    chips = n // 2
    orders = [list(range(1, stages)), list(range(stages - 1, 0, -1))]

    def bit_of(b):
        return lax.rem(me // (2 ** b), 2)

    def relative(x):
        other = me
        for b in range(stages):
            if (x >> b) & 1:
                other = other + (1 - 2 * bit_of(b)) * (2 ** b)
        return other

    def z_peer(r):
        return lax.rem(z + r, dp)

    near = [x for x in range(n) if bin(x >> 1).count("1") < 2]
    far = [x for x in range(n) if x not in near]
    queue = [0, 1] + [x for x in near if x > 1 and x % 2 == 0]
    queue += [x for x in near if x > 1 and x % 2 == 1] + far
    place = [queue.index(x) for x in range(n)]

    def fetch(source, target, sem):
        def step(i, carry):
            at = pl.ds(pl.multiple_of(i * edge, edge), edge)
            pltpu.make_async_copy(source.at[:, at], target.at[i], sem).start()
            return carry
        lax.fori_loop(0, target.shape[0], step, 0)

    rows_copy = pltpu.make_async_copy(rows_hbm, rows_s, in_sem.at[5])
    rows_copy.start()
    cols_copy = pltpu.make_async_copy(cols_hbm, cols_s, in_sem.at[6])
    cols_copy.start()
    own_copy = pltpu.make_async_copy(tiles_hbm, tiles_v.at[0], in_sem.at[2])
    own_copy.start()
    barrier = pltpu.get_barrier_semaphore()
    for x in range(1, n):
        pl.semaphore_signal(
            barrier, inc=1, device_id={"fsdp": relative(x)}, device_id_type=MESH
        )
    for r in range(1, dp):
        pl.semaphore_signal(
            barrier, inc=1, device_id={"dp": z_peer(r)}, device_id_type=MESH
        )
    fetch(cot_hbm, cot_v, in_sem.at[1])
    fetch(hid_hbm, hid_v, in_sem.at[0])

    lane = lax.broadcasted_iota(jnp.int32, (8, 128), 1)
    sub = lax.broadcasted_iota(jnp.int32, (8, 128), 0)
    meta = jnp.where(sub == 2, cnt_s[0], 0)
    rows_copy.wait()
    cols_copy.wait()
    for j in range(maxb):
        here = lax.rem(lane, maxb) == j
        meta = jnp.where((sub == 0) & here, rows_s[j], meta)
        meta = jnp.where((sub == 1) & here, cols_s[j], meta)
    meta_v[0] = meta
    grad_q[slots] = jnp.zeros(grad_q.shape[1:], F32)
    layer_q[slots] = jnp.zeros(layer_q.shape[1:], F32)
    grad_out[slots] = jnp.zeros(grad_out.shape[1:], BF16)
    layer_out[slots] = jnp.zeros(layer_out.shape[1:], BF16)
    own_copy.wait()
    pl.semaphore_wait(barrier, n - 1 + dp - 1)

    meta_copies = []
    for x in range(1, n):
        copy = pltpu.make_async_remote_copy(
            meta_v.at[0], meta_v.at[x], meta_ss.at[x - 1], meta_rs.at[x - 1],
            device_id={"fsdp": relative(x)}, device_id_type=MESH,
        )
        copy.start()
        meta_copies.append(copy)

    ag_copies = {}
    ag_done = set()

    def ag_send(p, i, e, h):
        bits = orders[p] + [0]
        owner = 0
        for t in range(len(bits)):
            if (e >> t) & 1:
                owner |= 1 << bits[t]
        where = 2 ** i - 1 + e
        part = pl.ds(p * half + h * (half // 2), half // 2)
        copy = pltpu.make_async_remote_copy(
            tiles_v.at[place[owner], part], tiles_v.at[place[owner | (1 << bits[i])], part],
            ag_ss.at[p, where, h], ag_rs.at[p, where, h],
            device_id={"fsdp": relative(1 << bits[i])}, device_id_type=MESH,
        )
        copy.start()
        ag_copies[p, i, e, h] = copy

    def ag_wait(p, i, e, h):
        if (p, i, e, h) not in ag_done:
            ag_done.add((p, i, e, h))
            ag_copies[p, i, e, h].wait_recv()

    for i in range(stages):
        for p in range(2):
            for h in range(2):
                if h == 0 or i == 0 or i == chip_bits:
                    ag_send(p, i, 0, h)

    def collect(xs, full):
        for x in xs:
            if x:
                meta_copies[x - 1].wait_recv()
            full = jnp.where(lane // maxb == place[x], meta_v[x], full)
        return full

    def to_smem(k):
        return pltpu.make_async_copy(full_v.at[k], full_s.at[k], in_sem.at[3 + k])

    known = collect(near, jnp.zeros((8, 128), jnp.int32))
    full_v[0] = known
    to_smem(0).start()

    def term(x, j):
        k = 0 if x in near else 1
        q = place[x] * maxb + j
        return lax.dot_general(
            hid_v[full_s[k, 0, q]], cot_v[full_s[k, 1, q]],
            (((0,), (0,)), ((), ())), preferred_element_type=F32,
        )

    def owner_at(p, e):
        owner = 0
        for t, b in enumerate(orders[p]):
            if not (e >> (chip_bits - 1 - t)) & 1:
                owner |= 1 << b
        return owner

    offsets = [0]
    for t in range(stages):
        offsets.append(offsets[-1] + (n >> (t + 1)))

    def pair_copy(p, e):
        return pltpu.make_async_remote_copy(
            sbuf.at[p, e], rbuf.at[p, e], rs_ss.at[p, e, 0], rs_rs.at[p, e, 0],
            device_id={"fsdp": relative(1)}, device_id_type=MESH,
        )

    def rs_copy(p, t, e, c):
        where = offsets[t] + e
        return pltpu.make_async_remote_copy(
            sbuf.at[p, where, c], rbuf.at[p, where, c],
            rs_ss.at[p, where, c], rs_rs.at[p, where, c],
            device_id={"fsdp": relative(1 << orders[p][t - 1])}, device_id_type=MESH,
        )

    def foreign(e):
        for p in range(2):
            for c in range(half):
                sbuf[p, e, c] = term(owner_at(p, e) | 1, p * half + c).astype(BF16)
        for p in range(2):
            pair_copy(p, e).start()

    def own(e):
        for p in range(2):
            for c in range(half):
                acc[p, e, c] = term(owner_at(p, e), p * half + c)

    starts = [0]
    for t in range(stages):
        starts.append(starts[-1] + (n >> (t + 1)) // 2)

    paired = set()

    def pair_wait(p, e):
        if (p, e) not in paired:
            paired.add((p, e))
            pair_copy(p, e).wait_recv()

    def pass_on(e, cs):
        for p in range(2):
            pair_wait(p, e)
            for c in cs:
                total = acc[p, e, c] + rbuf[p, e, c].astype(F32)
                sbuf[p, offsets[1] + e, c] = total.astype(BF16)
            for c in cs:
                rs_copy(p, 1, e, c).start()

    def reduce_step(t, c):
        m = n >> (t + 1)
        for e in range(m):
            for p in range(2):
                at_e = starts[t] + e
                rs_copy(p, t, e, c).wait_recv()
                total = acc[p, at_e, c] + rbuf[p, offsets[t] + e, c].astype(F32)
                if t == 1:
                    total = total + rbuf[p, at_e, c].astype(F32)
                if e < m // 2:
                    sbuf[p, offsets[t + 1] + e, c] = total.astype(BF16)
                    rs_copy(p, t + 1, e, c).start()
                elif m > 1:
                    acc[p, at_e, c] = total
                else:
                    at = pl.ds(p * edge, edge)
                    fin[c, at] = total
                    zs[c, at] = total.astype(BF16)
        if m == 1:
            for r in range(1, dp):
                z_copy(c, r).start()

    def z_rows(index):
        return pl.ds(pl.multiple_of(index * rows_z, rows_z), rows_z)

    def z_copy(c, r):
        return pltpu.make_async_remote_copy(
            zs.at[c, z_rows(z_peer(r))], zr.at[c, r - 1], zs_ss.at[c, r - 1], zs_rs.at[c, r - 1],
            device_id={"dp": z_peer(r)}, device_id_type=MESH,
        )

    def a_copy(c, r):
        return pltpu.make_async_remote_copy(
            za.at[c, z_rows(z)], za.at[c, z_rows(z)], za_ss.at[c, r - 1], za_rs.at[c, r - 1],
            device_id={"dp": z_peer(r)}, device_id_type=MESH,
        )

    def z_step(c, squares):
        piece = fin[c, z_rows(z)]
        for r in range(1, dp):
            z_copy(c, r).wait_recv()
            piece = piece + zr[c, r - 1].astype(F32)
        row = z * rows_z + lax.broadcasted_iota(jnp.int32, piece.shape, 0)
        slot = (row // edge) * half + c
        piece = piece * jnp.clip(cnt_s[0] - slot, 0, 1).astype(F32)
        za[c, z_rows(z)] = piece.astype(BF16)
        for r in range(1, dp):
            a_copy(c, r).start()
        return squares + jnp.sum((piece * piece).reshape(-1, 8, 128), axis=0)

    def project(at):
        def load(j):
            q = at * maxb + j
            backward = lax.dot_general(
                cot_v[full_s[1, 1, q]], tiles_v[at, j], (((1,), (1,)), ((), ())),
                preferred_element_type=F32,
            )
            forward = jnp.dot(hid_v[full_s[1, 0, q]], tiles_v[at, j], preferred_element_type=F32)
            return q, backward, forward
        for j in range(maxb):
            q, backward, forward = load(j)
            backward = backward + grad_q[table_s[0, q]]
            grad_q[q] = backward
            grad_out[q] = backward.astype(BF16)
            forward = forward + layer_q[table_s[1, q]]
            layer_q[q] = forward
            layer_out[q] = forward.astype(BF16)

    def arrived(x):
        for p in range(2):
            bits = orders[p] + [0]
            index = [t for t in range(stages) if (x >> bits[t]) & 1]
            if index:
                e = sum(1 << t for t in index[:-1])
                for h in range(2):
                    ag_wait(p, index[-1], e, h)

    sent = sorted(range(chips // 2), key=lambda e: bin(owner_at(0, e)).count("1"))
    kept = list(range(chips // 2, chips))
    to_smem(0).wait()
    pltpu.make_async_copy(cot_v, cot_v, in_sem.at[1]).wait()
    pltpu.make_async_copy(hid_v, hid_v, in_sem.at[0]).wait()
    foreign(sent[0])
    full = collect(far, known)
    full_v[1] = full
    to_smem(1).start()
    own(sent[0])
    to_smem(1).wait()
    lead, middle, tail = range(half // 2), range(half // 2, half - 1), [half - 1]
    for k in range(1, len(sent)):
        foreign(sent[k])
        pass_on(sent[k - 1], lead)
        own(sent[k])
    for e in kept:
        foreign(e)
    pass_on(sent[-1], lead)
    for e in sent:
        pass_on(e, middle)

    wide = lax.broadcasted_iota(jnp.int32, (slots, 128), 1)
    tall = lax.broadcasted_iota(jnp.int32, (slots, 128), 0)
    alive = lax.rem(lane[0:1], maxb) < full[2:3]
    table = jnp.full((8, 128), slots, jnp.int32)
    for k in range(2):
        named = jnp.broadcast_to(jnp.where(alive, full[k:k + 1], -1), (slots, 128))
        named_t = jnp.sum(jnp.where(wide == tall, named, 0), axis=1, keepdims=True)
        before = jnp.max(
            jnp.where((named_t == named) & (tall < wide), tall, -1), axis=0, keepdims=True
        )
        last = jnp.max(jnp.where(named_t == wide, tall, -1), axis=0, keepdims=True)
        table = jnp.where(sub == k, jnp.where(before < 0, slots, before), table)
        table = jnp.where(sub == 2 + k, jnp.where(last < 0, slots, last), table)
    table_out[...] = table
    table_copy = pltpu.make_async_copy(table_out, table_s, in_sem.at[7])
    table_copy.start()
    for e in kept:
        own(e)
    table_copy.wait()

    def project_all(xs):
        for x in xs:
            arrived(x)
        first = place[xs[0]]

        def one(at, carry):
            project(at)
            return carry

        lax.fori_loop(first, first + len(xs), one, 0)

    def ag_pass(i, e, h):
        for p in range(2):
            ag_wait(p, i, e, h)
            ag_send(p, chip_bits, e + 2 ** i, h)

    project_all([0, 1])
    for h in range(2):
        for i in range(chip_bits if h == 0 else 1):
            ag_pass(i, 0, h)
    for e in kept:
        for p in range(2):
            pair_wait(p, e)
    reduce_step(1, 0)
    for e in sent:
        pass_on(e, tail)

    def second(c, carry):
        reduce_step(1, c)
        return carry

    lax.fori_loop(1, half, second, 0)

    for i in range(1, chip_bits):
        for p in range(2):
            ag_send(p, i, 0, 1)
    for i in range(1, chip_bits):
        for e in range(1, 2 ** i):
            for p in range(2):
                for h in range(2):
                    ag_wait(p, i - 1, e - 2 ** (i - 1), h)
                    ag_send(p, i, e, h)

    for t in range(2, stages):
        def third(c, carry):
            reduce_step(t, c)
            return carry

        lax.fori_loop(0, half, third, 0)

    for i in range(1, chip_bits):
        ag_pass(i, 0, 1)
    project_all([x for x in near if x > 1 and x % 2 == 0])
    squares = lax.fori_loop(0, half // 2, z_step, jnp.zeros((8, 128), F32))
    project_all([x for x in near if x > 1 and x % 2 == 1])
    for i in range(1, chip_bits):
        for e in range(1, 2 ** i):
            for h in range(2):
                ag_pass(i, e, h)
    squares = lax.fori_loop(half // 2, half, z_step, squares)
    device = me * dp + z
    sqf[device] = jnp.sum(squares, axis=0, keepdims=True)
    sq_copies = []
    for x in range(n):
        for r in range(dp):
            if x or r:
                copy = pltpu.make_async_remote_copy(
                    sqf.at[device], sqf.at[device], sq_ss, sq_rs,
                    device_id={"fsdp": relative(x), "dp": z_peer(r)}, device_id_type=MESH,
                )
                copy.start()
                sq_copies.append(copy)

    project_all(far)

    entries = full_s[1, 2, 0]
    for x in range(1, n):
        entries = entries + full_s[1, 2, x * maxb]
    others = sqf.at[pl.ds(0, n * dp - 1)]
    pltpu.make_async_copy(others, others, sq_rs).wait()
    squares = jnp.sum(jnp.sum(sqf[...], axis=0), axis=1, keepdims=True)
    live = jnp.full((1, 1), entries, jnp.int32).astype(F32) * edge * edge
    spread = jnp.sqrt(squares / live)
    factor = jnp.minimum(1.0, 0.5 * root / spread) / root

    def finish(c, carry):
        for r in range(1, dp):
            a_copy(c, r).wait_recv()
        for p in range(2):
            wg_out[p * half + c] = za[c, pl.ds(p * edge, edge)].astype(F32) * factor
        return carry

    lax.fori_loop(0, half, finish, 0)

    for copy in meta_copies + list(ag_copies.values()):
        copy.wait_send()
    pltpu.make_async_copy(others, others, sq_ss).wait()

    for e in range(chips):
        for p in range(2):
            pair_copy(p, e).wait_send()

    def drain(c, carry):
        for t in range(1, stages):
            for e in range(n >> (t + 1)):
                for p in range(2):
                    rs_copy(p, t, e, c).wait_send()
        for r in range(1, dp):
            z_copy(c, r).wait_send()
            a_copy(c, r).wait_send()
        return carry

    lax.fori_loop(0, half, drain, 0)


def write_kernel(
    grad_v, layer_v, wg_v, table_v,
    layer_hbm, grad_hbm, wg_hbm,
    table_s, t_sem, w_sem, g_sem, l_sem,
):
    edge = grad_v.shape[2]
    table_copy = pltpu.make_async_copy(table_v, table_s, t_sem)
    table_copy.start()
    wg_copy = pltpu.make_async_copy(wg_v, wg_hbm, w_sem)
    wg_copy.start()
    table_copy.wait()

    def write(row, source, target, sem):
        def step(i, carry):
            at = pl.ds(pl.multiple_of(i * edge, edge), edge)
            pltpu.make_async_copy(source.at[table_s[row, i]], target.at[:, at], sem).start()
            return carry
        lax.fori_loop(0, target.shape[1] // edge, step, 0)

    write(2, grad_v, grad_hbm, g_sem)
    write(3, layer_v, layer_hbm, l_sem)
    pltpu.make_async_copy(grad_hbm, grad_hbm, g_sem).wait()
    pltpu.make_async_copy(layer_hbm, layer_hbm, l_sem).wait()
    wg_copy.wait()


def fused(n, dp, hidden, cotangent, tiles, tile_rows, tile_cols, counts):
    tokens, width_ff = hidden.shape
    width_model = cotangent.shape[1]
    maxb, edge, _ = tiles.shape
    blocks_ff, blocks_model = width_ff // edge, width_model // edge
    root = math.sqrt(tokens * n * dp)
    slots, half = n * maxb, maxb // 2
    in_hbm = functools.partial(pltpu.with_memory_space_constraint, memory_space=pltpu.HBM)
    rows_z = 2 * edge // dp
    hbm = pl.BlockSpec(memory_space=pltpu.HBM)
    smem = pl.BlockSpec(memory_space=pltpu.SMEM)
    vmem = pl.BlockSpec(memory_space=pltpu.VMEM)
    dma = pltpu.SemaphoreType.DMA
    grad, layer, weight, table = pl.pallas_call(
        functools.partial(fused_kernel, n, dp, root),
        out_shape=(
            pltpu.VMEM((slots + 1, tokens, edge), BF16),
            pltpu.VMEM((slots + 1, tokens, edge), BF16),
            pltpu.VMEM((maxb, edge, edge), F32),
            pltpu.VMEM((8, 128), jnp.int32),
        ),
        in_specs=[hbm, hbm, smem, hbm, hbm, hbm],
        out_specs=(vmem, vmem, vmem, vmem),
        scratch_shapes=[
            pltpu.SMEM(tile_rows.shape, jnp.int32),
            pltpu.SMEM(tile_cols.shape, jnp.int32),
            pltpu.VMEM((blocks_ff, tokens, edge), BF16),
            pltpu.VMEM((blocks_model, tokens, edge), BF16),
            pltpu.VMEM((n, maxb, edge, edge), BF16),
            pltpu.VMEM((n, 8, 128), jnp.int32),
            pltpu.VMEM((2, 8, 128), jnp.int32),
            pltpu.SMEM((2, 8, 128), jnp.int32),
            pltpu.SMEM((8, 128), jnp.int32),
            pltpu.VMEM((2, n // 2, half, edge, edge), F32),
            pltpu.VMEM((2, n - 1, half, edge, edge), BF16),
            pltpu.VMEM((2, n - 1, half, edge, edge), BF16),
            pltpu.VMEM((half, 2 * edge, edge), F32),
            pltpu.VMEM((half, 2 * edge, edge), BF16),
            pltpu.VMEM((half, dp - 1, rows_z, edge), BF16),
            pltpu.VMEM((half, 2 * edge, edge), BF16),
            pltpu.VMEM((n * dp, 1, 128), F32),
            pltpu.VMEM((slots + 1, tokens, edge), F32),
            pltpu.VMEM((slots + 1, tokens, edge), F32),
            dma((8,)),
            dma((n - 1,)), dma((n - 1,)),
            dma((2, n - 1, 2)), dma((2, n - 1, 2)),
            dma((2, n - 1, half)), dma((2, n - 1, half)),
            dma((half, dp - 1)), dma((half, dp - 1)),
            dma((half, dp - 1)), dma((half, dp - 1)),
            dma, dma,
        ],
        compiler_params=pltpu.CompilerParams(
            collective_id=0, has_side_effects=True, vmem_limit_bytes=44 * 2 ** 20
        ),
        name="fused",
    )(in_hbm(tile_rows), in_hbm(tile_cols), counts, in_hbm(tiles), in_hbm(hidden), in_hbm(cotangent))
    return pl.pallas_call(
        write_kernel,
        out_shape=(
            jax.ShapeDtypeStruct(cotangent.shape, BF16),
            jax.ShapeDtypeStruct(hidden.shape, BF16),
            jax.ShapeDtypeStruct(tiles.shape, F32),
        ),
        in_specs=[vmem, vmem, vmem, vmem],
        out_specs=(hbm, hbm, hbm),
        scratch_shapes=[pltpu.SMEM((8, 128), jnp.int32), dma, dma, dma, dma],
        compiler_params=pltpu.CompilerParams(vmem_limit_bytes=16 * 2 ** 20),
        name="write",
    )(grad, layer, weight, table)


def shards(n, dp, hidden, cotangent, tiles, tile_rows, tile_cols, counts):
    tokens, width_ff = hidden.shape
    width_model = cotangent.shape[1]
    maxb, edge, _ = tiles.shape
    blocks_ff, blocks_model = width_ff // edge, width_model // edge
    root = math.sqrt(tokens * n * dp)
    half, per = maxb // 2, maxb // dp
    sums = n * maxb * tokens * edge * 12
    if n == 8 and dp % 2 == 0 and max(n * maxb, blocks_ff, blocks_model) <= 128 and sums <= 28 * 2 ** 20:
        return fused(n, dp, hidden, cotangent, tiles, tile_rows, tile_cols, counts)
    hbm = pl.BlockSpec(memory_space=pl.ANY)
    smem = pl.BlockSpec(memory_space=pltpu.SMEM)
    vmem = pl.BlockSpec(memory_space=pltpu.VMEM)
    dma = pltpu.SemaphoreType.DMA
    meta, gathered, weight_grad = pl.pallas_call(
        functools.partial(exchange_kernel, n, dp, root),
        out_shape=(
            jax.ShapeDtypeStruct((n, 8, 128), jnp.int32),
            jax.ShapeDtypeStruct((n, maxb, edge, edge), BF16),
            jax.ShapeDtypeStruct((maxb, edge, edge), F32),
        ),
        in_specs=[smem, smem, smem, hbm, hbm, hbm],
        out_specs=(hbm, hbm, vmem),
        scratch_shapes=[
            pltpu.VMEM((blocks_ff, tokens, edge), BF16),
            pltpu.VMEM((blocks_model, tokens, edge), BF16),
            pltpu.VMEM((n, maxb, edge, edge), BF16),
            pltpu.VMEM((n, 8, 128), jnp.int32),
            pltpu.SMEM((n, 8, 128), jnp.int32),
            pltpu.VMEM((2, n // 2, half, edge, edge), F32),
            pltpu.VMEM((2, n - 1, half, edge, edge), BF16),
            pltpu.VMEM((2, n - 1, half, edge, edge), BF16),
            pltpu.VMEM((maxb, edge, edge), F32),
            pltpu.VMEM((dp, per, edge, edge), BF16),
            pltpu.VMEM((dp - 1, per, edge, edge), BF16),
            pltpu.VMEM((dp, per, edge, edge), BF16),
            pltpu.VMEM((dp, 8, 128), F32),
            pltpu.VMEM((n, 8, 128), F32),
            dma((4,)), dma((2,)),
            dma((n - 1,)), dma((n - 1,)),
            dma((2, n - 1)), dma((2, n - 1)),
            dma((2, n - 1)), dma((2, n - 1)),
            dma((dp - 1,)), dma((dp - 1,)),
            dma((dp - 1,)), dma((dp - 1,)),
            dma((dp - 1,)), dma((dp - 1,)),
            dma((n - 1,)), dma((n - 1,)),
        ],
        compiler_params=pltpu.CompilerParams(
            collective_id=0, has_side_effects=True, vmem_limit_bytes=60 * 2 ** 20
        ),
        name="exchange",
    )(tile_rows, tile_cols, counts, tiles, hidden, cotangent)

    layer_out, hidden_grad = pl.pallas_call(
        functools.partial(project_kernel, n, maxb),
        out_shape=(
            jax.ShapeDtypeStruct(cotangent.shape, BF16),
            jax.ShapeDtypeStruct(hidden.shape, BF16),
        ),
        in_specs=[smem, hbm, hbm, hbm],
        out_specs=(hbm, hbm),
        scratch_shapes=[
            pltpu.VMEM((n, maxb, edge, edge), BF16),
            pltpu.VMEM(cotangent.shape, BF16),
            pltpu.VMEM((n, maxb, tokens, edge), BF16),
            pltpu.VMEM((blocks_ff, tokens, edge), F32),
            pltpu.VMEM((blocks_ff, tokens, edge), BF16),
            pltpu.VMEM((blocks_model, tokens, edge), F32),
            pltpu.VMEM((blocks_model, tokens, edge), BF16),
            pltpu.VMEM((tokens, edge), BF16),
            pltpu.VMEM((maxb, tokens, edge), F32),
            pltpu.SMEM((blocks_ff,), jnp.int32),
            pltpu.SMEM((blocks_ff,), jnp.int32),
            pltpu.SMEM((blocks_model,), jnp.int32),
            pltpu.SMEM((blocks_model,), jnp.int32),
            dma((2,)), dma, dma, dma,
        ],
        compiler_params=pltpu.CompilerParams(vmem_limit_bytes=62 * 2 ** 20),
        name="project",
    )(meta, gathered, hidden, cotangent)
    return layer_out, hidden_grad, weight_grad


def solution(mesh):
    placed = (
        P(("fsdp", "dp"), None),
        P(("fsdp", "dp"), None),
        P("fsdp", None, None),
        P("fsdp"),
        P("fsdp"),
        P("fsdp"),
    )
    return jax.shard_map(
        functools.partial(shards, mesh.shape["fsdp"], mesh.shape["dp"]),
        mesh=mesh,
        in_specs=placed,
        out_specs=(P(("fsdp", "dp"), None), P(("fsdp", "dp"), None), P("fsdp", None, None)),
        check_vma=False,
    )
```

```python
import functools
import math

import jax
import jax.numpy as jnp
from jax import lax
from jax.experimental import pallas as pl
from jax.experimental.pallas import tpu as pltpu
from jax.sharding import PartitionSpec as P

MESH = pl.DeviceIdType.MESH
F32 = jnp.float32
BF16 = jnp.bfloat16


def exchange_kernel(
    n, dp, root,
    rows_s, cols_s, cnt_s, tiles_hbm, hid_hbm, cot_hbm,
    meta_out, tiles_out, wg_out,
    hid_v, cot_v, tiles_v, meta_v, meta_s, acc, sbuf, rbuf, fin, zs, zr, za, sqz, sqf,
    in_sem, out_sem, meta_ss, meta_rs, ag_ss, ag_rs, rs_ss, rs_rs,
    zs_ss, zs_rs, za_ss, za_rs, qz_ss, qz_rs, qf_ss, qf_rs,
):
    me = lax.axis_index("fsdp")
    z = lax.axis_index("dp")
    maxb, edge = tiles_hbm.shape[0], tiles_hbm.shape[1]
    half = maxb // 2
    per = maxb // dp
    stages = n.bit_length() - 1
    chip_bits = stages - 1
    orders = [list(range(1, stages)), list(range(stages - 1, 0, -1))]
    core = lax.rem(me, 2)

    def bit_of(b):
        return lax.rem(me // (2 ** b), 2)

    def flip(value_me, b):
        return value_me + (1 - 2 * bit_of(b)) * (2 ** b)

    def fetch(source, target, sem):
        def step(i, carry):
            at = pl.ds(pl.multiple_of(i * edge, edge), edge)
            pltpu.make_async_copy(source.at[:, at], target.at[i], sem).start()
            return carry
        lax.fori_loop(0, target.shape[0], step, 0)

    own_copy = pltpu.make_async_copy(tiles_hbm, tiles_v.at[me], in_sem.at[2])
    own_copy.start()
    fetch(cot_hbm, cot_v, in_sem.at[1])
    fetch(hid_hbm, hid_v, in_sem.at[0])

    barrier = pltpu.get_barrier_semaphore()
    for k in range(1, n):
        pl.semaphore_signal(
            barrier, inc=1, device_id={"fsdp": lax.rem(me + k, n)}, device_id_type=MESH
        )
    for k in range(1, dp):
        pl.semaphore_signal(
            barrier, inc=1, device_id={"dp": lax.rem(z + k, dp)}, device_id_type=MESH
        )
    lane = lax.broadcasted_iota(jnp.int32, (8, 128), 1)
    sub = lax.broadcasted_iota(jnp.int32, (8, 128), 0)
    meta = jnp.where(sub == 2, cnt_s[0], 0)
    for j in range(maxb):
        meta = jnp.where((sub == 0) & (lane == j), rows_s[j], meta)
        meta = jnp.where((sub == 1) & (lane == j), cols_s[j], meta)
    meta_v[me] = meta
    own_copy.wait()
    pl.semaphore_wait(barrier, n - 1 + dp - 1)

    meta_copies = []
    for k in range(1, n):
        copy = pltpu.make_async_remote_copy(
            meta_v.at[me], meta_v.at[me], meta_ss.at[k - 1], meta_rs.at[k - 1],
            device_id={"fsdp": lax.rem(me + k, n)}, device_id_type=MESH,
        )
        copy.start()
        meta_copies.append(copy)

    ag_copies = {}

    def ag_send(p, i, e):
        bits = orders[p] + [0]
        owner = me
        for t in range(len(bits)):
            if (e >> t) & 1:
                owner = flip(owner, bits[t])
        piece = tiles_v.at[owner, pl.ds(p * half, half)]
        where = 2 ** i - 1 + e
        copy = pltpu.make_async_remote_copy(
            piece, piece, ag_ss.at[p, where], ag_rs.at[p, where],
            device_id={"fsdp": flip(me, bits[i])}, device_id_type=MESH,
        )
        copy.start()
        ag_copies[p, i, e] = copy

    for i in range(stages):
        for p in range(2):
            ag_send(p, i, 0)

    for copy in meta_copies:
        copy.wait_recv()
    to_smem = pltpu.make_async_copy(meta_v, meta_s, in_sem.at[3])
    to_smem.start()
    to_smem.wait()
    meta_back = pltpu.make_async_copy(meta_v, meta_out, out_sem.at[0])
    meta_back.start()
    pltpu.make_async_copy(cot_v, cot_v, in_sem.at[1]).wait()
    pltpu.make_async_copy(hid_v, hid_v, in_sem.at[0]).wait()

    def owner_at(p, e, core_bit):
        owner = core_bit
        for t, b in enumerate(orders[p]):
            ebit = lax.rem(e // (2 ** (chip_bits - 1 - t)), 2)
            owner = owner + lax.rem(bit_of(b) + 1 + ebit, 2) * (2 ** b)
        return owner

    def term(owner, j):
        return lax.dot_general(
            hid_v[meta_s[owner, 0, j]], cot_v[meta_s[owner, 1, j]],
            (((0,), (0,)), ((), ())), preferred_element_type=F32,
        )

    chips = n // 2
    offsets = [0]
    for t in range(stages):
        offsets.append(offsets[-1] + (n >> (t + 1)))

    def rs_copy(p, t, e):
        where = offsets[t] + e
        bit = 0 if t == 0 else orders[p][t - 1]
        return pltpu.make_async_remote_copy(
            sbuf.at[p, where], rbuf.at[p, where], rs_ss.at[p, where], rs_rs.at[p, where],
            device_id={"fsdp": flip(me, bit)}, device_id_type=MESH,
        )

    def foreign(e, carry):
        for p in range(2):
            owner = owner_at(p, e, 1 - core)
            for j in range(half):
                sbuf[p, e, j] = term(owner, p * half + j).astype(BF16)
            rs_copy(p, 0, e).start()
        return carry

    lax.fori_loop(0, chips, foreign, 0)

    for i in range(chip_bits):
        for p in range(2):
            for e in range(2 ** i):
                ag_copies[p, i, e].wait_recv()
                for i2 in range(i + 1, stages):
                    ag_send(p, i2, e + 2 ** i)

    def own(e, carry):
        for p in range(2):
            owner = owner_at(p, e, core)
            for j in range(half):
                acc[p, e, j] = term(owner, p * half + j)
        return carry

    lax.fori_loop(0, chips, own, 0)

    start = 0
    for t in range(stages):
        m = n >> (t + 1)
        sent = m // 2
        for e in range(m):
            for p in range(2):
                rs_copy(p, t, e).wait_recv()
                total = acc[p, start + e] + rbuf[p, offsets[t] + e].astype(F32)
                if e < sent:
                    sbuf[p, offsets[t + 1] + e] = total.astype(BF16)
                    rs_copy(p, t + 1, e).start()
                elif m > 1:
                    acc[p, start + e] = total
                else:
                    fin[pl.ds(p * half, half)] = total
                    for q in range(half // per):
                        zs[p * (half // per) + q] = total[q * per:(q + 1) * per].astype(BF16)
        start += sent

    def z_peer(r):
        return lax.rem(z + r, dp)

    z_copies = []
    for r in range(1, dp):
        copy = pltpu.make_async_remote_copy(
            zs.at[z_peer(r)], zr.at[r - 1], zs_ss.at[r - 1], zs_rs.at[r - 1],
            device_id={"dp": z_peer(r)}, device_id_type=MESH,
        )
        copy.start()
        z_copies.append(copy)

    for p in range(2):
        for e in range(2 ** chip_bits):
            ag_copies[p, chip_bits, e].wait_recv()
    tiles_back = pltpu.make_async_copy(tiles_v, tiles_out, out_sem.at[1])
    tiles_back.start()

    piece = fin[pl.ds(z * per, per)]
    for r in range(1, dp):
        z_copies[r - 1].wait_recv()
        piece = piece + zr[r - 1].astype(F32)
    slot = z * per + lax.broadcasted_iota(jnp.int32, piece.shape, 0)
    piece = piece * jnp.clip(cnt_s[0] - slot, 0, 1).astype(F32)
    za[z] = piece.astype(BF16)
    sqz[z] = jnp.sum((piece * piece).reshape(-1, 8, 128), axis=0)
    a_copies, q_copies = [], []
    for r in range(1, dp):
        copy = pltpu.make_async_remote_copy(
            sqz.at[z], sqz.at[z], qz_ss.at[r - 1], qz_rs.at[r - 1],
            device_id={"dp": z_peer(r)}, device_id_type=MESH,
        )
        copy.start()
        q_copies.append(copy)
    for r in range(1, dp):
        copy = pltpu.make_async_remote_copy(
            za.at[z], za.at[z], za_ss.at[r - 1], za_rs.at[r - 1],
            device_id={"dp": z_peer(r)}, device_id_type=MESH,
        )
        copy.start()
        a_copies.append(copy)
    for copy in q_copies:
        copy.wait_recv()
    sqf[me] = jnp.sum(sqz[...], axis=0)
    f_copies = []
    for k in range(1, n):
        copy = pltpu.make_async_remote_copy(
            sqf.at[me], sqf.at[me], qf_ss.at[k - 1], qf_rs.at[k - 1],
            device_id={"fsdp": lax.rem(me + k, n)}, device_id_type=MESH,
        )
        copy.start()
        f_copies.append(copy)
    entries = meta_s[0, 2, 0]
    for k in range(1, n):
        entries = entries + meta_s[k, 2, 0]
    for copy in a_copies + f_copies:
        copy.wait_recv()
    squares = jnp.sum(jnp.sum(sqf[...], axis=0), axis=(0, 1), keepdims=True)
    live = jnp.full((1, 1), entries, jnp.int32).astype(F32) * edge * edge
    spread = jnp.sqrt(squares / live)
    factor = jnp.minimum(1.0, 0.5 * root / spread) / root
    for q in range(dp):
        for i in range(per):
            wg_out[q * per + i] = za[q, i].astype(F32) * factor

    for copy in meta_copies + list(ag_copies.values()) + z_copies + q_copies + a_copies + f_copies:
        copy.wait_send()
    for t in range(stages):
        for e in range(n >> (t + 1)):
            for p in range(2):
                rs_copy(p, t, e).wait_send()
    meta_back.wait()
    tiles_back.wait()


def project_kernel(
    n, maxb,
    meta_s, tiles_hbm, hid_hbm, cot_hbm,
    layer_hbm, grad_hbm,
    tiles_v, cot_v, hid_v, gacc, gout, lacc, lout, zero_v, values,
    row_left, row_seen, col_left, col_seen,
    in_sem, hid_sem, g_sem, l_sem,
):
    edge = zero_v.shape[1]
    tile_copy = pltpu.make_async_copy(tiles_hbm, tiles_v, in_sem.at[0])
    cot_copy = pltpu.make_async_copy(cot_hbm, cot_v, in_sem.at[1])
    tile_copy.start()
    cot_copy.start()
    zero_v[...] = jnp.zeros_like(zero_v)

    def clear(left, seen):
        def step(i, carry):
            left[i] = 0
            seen[i] = 0
            return carry
        lax.fori_loop(0, left.shape[0], step, 0)

    clear(row_left, row_seen)
    clear(col_left, col_seen)

    def columns(i):
        return pl.ds(pl.multiple_of(i * edge, edge), edge)

    def each_live(visit):
        def owner(o, carry):
            def slot(j, inner):
                visit(o, j, meta_s[o, 0, j], meta_s[o, 1, j])
                return inner
            return lax.fori_loop(0, meta_s[o, 2, 0], slot, carry)
        lax.fori_loop(0, n, owner, 0)

    def fetch(o, j, row, col):
        pltpu.make_async_copy(hid_hbm.at[:, columns(row)], hid_v.at[o, j], hid_sem).start()
        row_left[row] = row_left[row] + 1
        col_left[col] = col_left[col] + 1

    each_live(fetch)

    def blank(left, target, sem):
        def step(i, carry):
            @pl.when(left[i] == 0)
            def _():
                pltpu.make_async_copy(zero_v, target.at[:, columns(i)], sem).start()
            return carry
        lax.fori_loop(0, left.shape[0], step, 0)

    blank(row_left, grad_hbm, g_sem)
    blank(col_left, layer_hbm, l_sem)
    tile_copy.wait()
    cot_copy.wait()

    def add_block(at, value, left, seen, total, out, target, sem):
        remaining = left[at] - 1
        first = seen[at] == 0
        left[at] = remaining
        seen[at] = 1

        @pl.when(first & (remaining == 0))
        def _():
            out[at] = value[...].astype(BF16)

        @pl.when(first & (remaining > 0))
        def _():
            total[at] = value[...]

        @pl.when(jnp.logical_not(first))
        def _():
            summed = total[at] + value[...]
            total[at] = summed
            out[at] = summed.astype(BF16)

        @pl.when(remaining == 0)
        def _():
            pltpu.make_async_copy(out.at[at], target.at[:, columns(at)], sem).start()

    def backward(o, carry):
        for j in range(maxb):
            values[j] = lax.dot_general(
                cot_v[:, columns(meta_s[o, 1, j])], tiles_v[o, j], (((1,), (1,)), ((), ())),
                preferred_element_type=F32,
            )

        def slot(j, inner):
            add_block(
                meta_s[o, 0, j], values.at[j], row_left, row_seen, gacc, gout, grad_hbm, g_sem
            )
            return inner

        return lax.fori_loop(0, meta_s[o, 2, 0], slot, carry)

    lax.fori_loop(0, n, backward, 0)

    def arrived(o, j, row, col):
        pltpu.make_async_copy(hid_hbm.at[:, columns(row)], hid_v.at[o, j], hid_sem).wait()

    each_live(arrived)

    def forward(o, carry):
        for j in range(maxb):
            values[j] = jnp.dot(hid_v[o, j], tiles_v[o, j], preferred_element_type=F32)

        def slot(j, inner):
            add_block(
                meta_s[o, 1, j], values.at[j], col_left, col_seen, lacc, lout, layer_hbm, l_sem
            )
            return inner

        return lax.fori_loop(0, meta_s[o, 2, 0], slot, carry)

    lax.fori_loop(0, n, forward, 0)
    pltpu.make_async_copy(grad_hbm, grad_hbm, g_sem).wait()
    pltpu.make_async_copy(layer_hbm, layer_hbm, l_sem).wait()


def fused_kernel(
    n, dp, root,
    rows_hbm, cols_hbm, cnt_s, tiles_hbm, hid_hbm, cot_hbm,
    grad_out, layer_out, wg_out, table_s,
    rows_s, cols_s, hid_v, cot_v, tiles_v, meta_v, full_v, full_s, table_v,
    acc, sbuf, rbuf, fin, zs, zr, za, sqf, grad_q, layer_q,
    in_sem, send_sem, meta_rs, ag_rs, pair_rs, rs_rs, z_rs, za_rs, sq_rs,
):
    me = lax.axis_index("fsdp")
    z = lax.axis_index("dp")
    maxb, edge = tiles_hbm.shape[0], tiles_hbm.shape[1]
    slots = n * maxb
    half = maxb // 2
    rows_z = 2 * edge // dp
    stages = n.bit_length() - 1
    chip_bits = stages - 1
    chips = n // 2
    orders = [list(range(1, stages)), list(range(stages - 1, 0, -1))]

    def bit_of(b):
        return lax.rem(me // (2 ** b), 2)

    def relative(x):
        other = me
        for b in range(stages):
            if (x >> b) & 1:
                other = other + (1 - 2 * bit_of(b)) * (2 ** b)
        return other

    def z_peer(r):
        return lax.rem(z + r, dp)

    near = [x for x in range(n) if bin(x >> 1).count("1") < 2]
    far = [x for x in range(n) if x not in near]
    queue = [0, 1] + [x for x in near if x > 1 and x % 2 == 0]
    queue += [x for x in near if x > 1 and x % 2 == 1] + far
    place = [queue.index(x) for x in range(n)]

    def fetch(source, target, sem, first, last):
        def step(i, carry):
            at = pl.ds(pl.multiple_of(i * edge, edge), edge)
            pltpu.make_async_copy(source.at[:, at], target.at[i], sem).start()
            return carry
        lax.fori_loop(first, last, step, 0)

    def blocks_wait(count, sem):
        if count <= maxb:
            blocks = tiles_v.at[0, pl.ds(0, count)]
        else:
            blocks = tiles_v.at[pl.ds(0, count // maxb)]
        pltpu.make_async_copy(blocks, blocks, sem).wait()

    barrier = pltpu.get_barrier_semaphore()
    for r in range(1, dp):
        pl.semaphore_signal(
            barrier, inc=1, device_id={"dp": z_peer(r)}, device_id_type=MESH
        )
    for x in range(n - 1, 0, -1):
        pl.semaphore_signal(
            barrier, inc=1, device_id={"fsdp": relative(x)}, device_id_type=MESH
        )
    rows_copy = pltpu.make_async_copy(rows_hbm, rows_s, in_sem.at[2])
    rows_copy.start()
    cols_copy = pltpu.make_async_copy(cols_hbm, cols_s, in_sem.at[3])
    cols_copy.start()
    own_copy = pltpu.make_async_copy(tiles_hbm, tiles_v.at[0], in_sem.at[7])
    own_copy.start()

    early = hid_v.shape[0] * 3 // 8
    fetch(cot_hbm, cot_v, in_sem.at[1], 0, cot_v.shape[0])
    fetch(hid_hbm, hid_v, in_sem.at[0], 0, early)

    lane = lax.broadcasted_iota(jnp.int32, (8, 128), 1)
    sub = lax.broadcasted_iota(jnp.int32, (8, 128), 0)
    meta = jnp.where(sub == 2, cnt_s[0], 0)
    rows_copy.wait()
    cols_copy.wait()
    for j in range(maxb):
        here = lax.rem(lane, maxb) == j
        meta = jnp.where((sub == 0) & here, rows_s[j], meta)
        meta = jnp.where((sub == 1) & here, cols_s[j], meta)
    meta_v[0] = meta
    pl.semaphore_wait(barrier, n - 1 + dp - 1)

    for x in range(n - 1, 0, -1):
        pltpu.make_async_remote_copy(
            meta_v.at[0], meta_v.at[place[x]], send_sem.at[0], meta_rs.at[int(x in far)],
            device_id={"fsdp": relative(x)}, device_id_type=MESH,
        ).start()
    own_copy.wait()

    ag_done = set()

    def ag_index(i, e, h):
        split = 0 < i < chip_bits and e == 0
        keys = [(i, e, h) for i in range(stages) for e in range(2 ** i) for h in range(2)
                if h == 0 or (0 < i < chip_bits and e == 0)]
        return keys.index((i, e, h if split else 0)), maxb // 2 if split else maxb

    def ag_send(p, i, e, h):
        bits = orders[p] + [0]
        owner = 0
        for t in range(len(bits)):
            if (e >> t) & 1:
                owner |= 1 << bits[t]
        part = pl.ds(p * half + h * (half // 2), half // 2)
        pltpu.make_async_remote_copy(
            tiles_v.at[place[owner], part], tiles_v.at[place[owner | (1 << bits[i])], part],
            send_sem.at[1], ag_rs.at[ag_index(i, e, h)[0]],
            device_id={"fsdp": relative(1 << bits[i])}, device_id_type=MESH,
        ).start()

    def ag_wait(i, e, h):
        index, count = ag_index(i, e, h)
        if index not in ag_done:
            ag_done.add(index)
            blocks_wait(count, ag_rs.at[index])

    for i in range(stages):
        for p in range(2):
            for h in range(2):
                if h == 0 or i == 0 or i == chip_bits:
                    ag_send(p, i, 0, h)

    grad_q[slots] = jnp.zeros(grad_q.shape[1:], F32)
    layer_q[slots] = jnp.zeros(layer_q.shape[1:], F32)
    grad_out[slots] = jnp.zeros(grad_out.shape[1:], BF16)
    layer_out[slots] = jnp.zeros(layer_out.shape[1:], BF16)

    fetch(hid_hbm, hid_v, in_sem.at[0], early, hid_v.shape[0])

    def collect(xs, full):
        arrive = [x for x in xs if x]
        first = min(place[x] for x in arrive)
        metas = meta_v.at[pl.ds(first, len(arrive))]
        pltpu.make_async_copy(metas, metas, meta_rs.at[int(xs is far)]).wait()
        for x in xs:
            full = jnp.where(lane // maxb == place[x], meta_v[place[x]], full)
        return full

    def to_smem(k):
        return pltpu.make_async_copy(full_v.at[k], full_s.at[k], in_sem.at[4 + k])

    known = collect(near, jnp.zeros((8, 128), jnp.int32))
    full_v[0] = known
    to_smem(0).start()

    def term(x, j):
        k = 0 if x in near else 1
        q = place[x] * maxb + j
        return lax.dot_general(
            hid_v[full_s[k, 0, q]], cot_v[full_s[k, 1, q]],
            (((0,), (0,)), ((), ())), preferred_element_type=F32,
        )

    def owner_at(p, e):
        owner = 0
        for t, b in enumerate(orders[p]):
            if not (e >> (chip_bits - 1 - t)) & 1:
                owner |= 1 << b
        return owner

    offsets = [0]
    for t in range(stages):
        offsets.append(offsets[-1] + (n >> (t + 1)))

    def pair_copy(p, e):
        return pltpu.make_async_remote_copy(
            sbuf.at[p, e], rbuf.at[p, e], send_sem.at[2], pair_rs.at[e],
            device_id={"fsdp": relative(1)}, device_id_type=MESH,
        )

    def rs_copy(p, t, e, c):
        where = offsets[t] + e
        return pltpu.make_async_remote_copy(
            sbuf.at[p, where, c], rbuf.at[p, where, c],
            send_sem.at[2], rs_rs.at[t - 1, c],
            device_id={"fsdp": relative(1 << orders[p][t - 1])}, device_id_type=MESH,
        )

    def foreign(e):
        for p in range(2):
            for c in range(half):
                sbuf[p, e, c] = term(owner_at(p, e) | 1, p * half + c).astype(BF16)
        for p in range(2):
            pair_copy(p, e).start()

    def own(e):
        for p in range(2):
            for c in range(half):
                acc[p, e, c] = term(owner_at(p, e), p * half + c)

    starts = [0]
    for t in range(stages):
        starts.append(starts[-1] + (n >> (t + 1)) // 2)

    paired = set()

    def pair_wait(e):
        if e not in paired:
            paired.add(e)
            blocks_wait(maxb, pair_rs.at[e])

    def pass_on(e, cs):
        for p in range(2):
            pair_wait(e)
            for c in cs:
                total = acc[p, e, c] + rbuf[p, e, c].astype(F32)
                sbuf[p, offsets[1] + e, c] = total.astype(BF16)
            for c in cs:
                rs_copy(p, 1, e, c).start()

    def reduce_step(t, c):
        m = n >> (t + 1)
        blocks_wait(2 * m, rs_rs.at[t - 1, c])
        for e in range(m):
            for p in range(2):
                at_e = starts[t] + e
                total = acc[p, at_e, c] + rbuf[p, offsets[t] + e, c].astype(F32)
                if t == 1:
                    total = total + rbuf[p, at_e, c].astype(F32)
                if e < m // 2:
                    sbuf[p, offsets[t + 1] + e, c] = total.astype(BF16)
                    rs_copy(p, t + 1, e, c).start()
                elif m > 1:
                    acc[p, at_e, c] = total
                else:
                    at = pl.ds(p * edge, edge)
                    fin[c, at] = total
                    zs[c, at] = total.astype(BF16)
        if m == 1:
            for r in range(1, dp):
                z_copy(c, r).start()

    def z_rows(index):
        return pl.ds(pl.multiple_of(index * rows_z, rows_z), rows_z)

    def z_copy(c, r):
        return pltpu.make_async_remote_copy(
            zs.at[c, z_rows(z_peer(r))], zr.at[c, r - 1], send_sem.at[3], z_rs.at[c],
            device_id={"dp": z_peer(r)}, device_id_type=MESH,
        )

    def a_copy(c, r):
        return pltpu.make_async_remote_copy(
            za.at[c, z_rows(z)], za.at[c, z_rows(z)], send_sem.at[4], za_rs,
            device_id={"dp": z_peer(r)}, device_id_type=MESH,
        )

    def z_step(c, squares):
        piece = fin[c, z_rows(z)]
        pltpu.make_async_copy(zr.at[c], zr.at[c], z_rs.at[c]).wait()
        for r in range(1, dp):
            piece = piece + zr[c, r - 1].astype(F32)
        row = z * rows_z + lax.broadcasted_iota(jnp.int32, piece.shape, 0)
        slot = (row // edge) * half + c
        piece = piece * jnp.clip(cnt_s[0] - slot, 0, 1).astype(F32)
        za[c, z_rows(z)] = piece.astype(BF16)
        for r in range(1, dp):
            a_copy(c, r).start()
        return squares + jnp.sum((piece * piece).reshape(-1, 8, 128), axis=0)

    def project(at):
        def load(j):
            q = at * maxb + j
            backward = lax.dot_general(
                cot_v[full_s[1, 1, q]], tiles_v[at, j], (((1,), (1,)), ((), ())),
                preferred_element_type=F32,
            )
            forward = jnp.dot(hid_v[full_s[1, 0, q]], tiles_v[at, j], preferred_element_type=F32)
            return q, backward, forward
        for j in range(maxb):
            q, backward, forward = load(j)
            backward = backward + grad_q[table_s[0, q]]
            grad_q[q] = backward
            grad_out[q] = backward.astype(BF16)
            forward = forward + layer_q[table_s[1, q]]
            layer_q[q] = forward
            layer_out[q] = forward.astype(BF16)

    def arrived(x):
        for p in range(2):
            bits = orders[p] + [0]
            index = [t for t in range(stages) if (x >> bits[t]) & 1]
            if index:
                e = sum(1 << t for t in index[:-1])
                for h in range(2):
                    ag_wait(index[-1], e, h)

    sent = sorted(range(chips // 2), key=lambda e: bin(owner_at(0, e)).count("1"))
    kept = list(range(chips // 2, chips))
    to_smem(0).wait()
    pltpu.make_async_copy(cot_v, cot_v, in_sem.at[1]).wait()
    pltpu.make_async_copy(hid_v, hid_v, in_sem.at[0]).wait()
    foreign(sent[0])
    full = collect(far, known)
    full_v[1] = full
    to_smem(1).start()
    own(sent[0])
    to_smem(1).wait()
    for k in range(1, len(sent)):
        foreign(sent[k])
        pass_on(sent[k - 1], [0])
        own(sent[k])
    foreign(kept[0])
    pass_on(sent[-1], [0])
    for c in range(1, half - 1):
        for e in sent:
            pass_on(e, [c])
    for e in kept[1:]:
        foreign(e)

    wide = lax.broadcasted_iota(jnp.int32, (slots, 128), 1)
    tall = lax.broadcasted_iota(jnp.int32, (slots, 128), 0)
    alive = lax.rem(lane[0:1], maxb) < full[2:3]
    table = jnp.full((8, 128), slots, jnp.int32)
    for k in range(2):
        named = jnp.broadcast_to(jnp.where(alive, full[k:k + 1], -1), (slots, 128))
        named_t = jnp.sum(jnp.where(wide == tall, named, 0), axis=1, keepdims=True)
        before = jnp.max(
            jnp.where((named_t == named) & (tall < wide), tall, -1), axis=0, keepdims=True
        )
        last = jnp.max(jnp.where(named_t == wide, tall, -1), axis=0, keepdims=True)
        table = jnp.where(sub == k, jnp.where(before < 0, slots, before), table)
        table = jnp.where(sub == 2 + k, jnp.where(last < 0, slots, last), table)
    table_v[...] = table
    table_copy = pltpu.make_async_copy(table_v, table_s, in_sem.at[6])
    table_copy.start()
    for e in kept:
        own(e)
    table_copy.wait()

    def project_all(xs):
        for x in xs:
            arrived(x)
        first = place[xs[0]]

        def one(at, carry):
            project(at)
            return carry

        lax.fori_loop(first, first + len(xs), one, 0)

    def ag_pass(i, e, h):
        ag_wait(i, e, h)
        for p in range(2):
            ag_send(p, chip_bits, e + 2 ** i, h)

    project_all([0, 1])
    for h in range(2):
        for i in range(chip_bits if h == 0 else 1):
            ag_pass(i, 0, h)
    for e in kept:
        pair_wait(e)
    reduce_step(1, 0)
    for e in sent:
        pass_on(e, [half - 1])

    def second(c, carry):
        reduce_step(1, c)
        return carry

    lax.fori_loop(1, half - 1, second, 0)
    for t in range(2, stages):
        reduce_step(t, 0)
    reduce_step(1, half - 1)
    for t in range(2, stages):
        def third(c, carry):
            reduce_step(t, c)
            return carry

        lax.fori_loop(1, half, third, 0)

    for i in range(1, chip_bits):
        for p in range(2):
            ag_send(p, i, 0, 1)
    for i in range(1, chip_bits):
        for e in range(1, 2 ** i):
            for p in range(2):
                for h in range(2):
                    ag_wait(i - 1, e - 2 ** (i - 1), h)
                    ag_send(p, i, e, h)

    squares = lax.fori_loop(0, half // 2, z_step, jnp.zeros((8, 128), F32))
    for i in range(1, chip_bits):
        ag_pass(i, 0, 1)
    project_all([x for x in near if x > 1 and x % 2 == 0])
    squares = lax.fori_loop(half // 2, half, z_step, squares)
    device = me * dp + z
    sqf[device] = jnp.sum(squares, axis=0, keepdims=True)
    for x in range(n):
        for r in range(dp):
            if x or r:
                pltpu.make_async_remote_copy(
                    sqf.at[device], sqf.at[device], send_sem.at[5], sq_rs,
                    device_id={"fsdp": relative(x), "dp": z_peer(r)}, device_id_type=MESH,
                ).start()

    project_all([x for x in near if x > 1 and x % 2 == 1])
    for i in range(1, chip_bits):
        for e in range(1, 2 ** i):
            for h in range(2):
                ag_pass(i, e, h)
    project_all(far)

    entries = full_s[1, 2, 0]
    for x in range(1, n):
        entries = entries + full_s[1, 2, x * maxb]
    others = sqf.at[pl.ds(0, n * dp - 1)]
    pltpu.make_async_copy(others, others, sq_rs).wait()
    squares = jnp.sum(jnp.sum(sqf[...], axis=0), axis=1, keepdims=True)
    live = jnp.full((1, 1), entries, jnp.int32).astype(F32) * edge * edge
    spread = jnp.sqrt(squares / live)
    factor = jnp.minimum(1.0, 0.5 * root / spread) / root

    pltpu.make_async_copy(zr, zr, za_rs).wait()

    def finish(c, carry):
        for p in range(2):
            wg_out[p * half + c] = za[c, pl.ds(p * edge, edge)].astype(F32) * factor
        return carry

    lax.fori_loop(0, half, finish, 0)

    metas = meta_v.at[pl.ds(1, n - 1)]
    gathered = tiles_v.at[pl.ds(1, n - 1)]
    for k, sent in enumerate((metas, gathered, sbuf, zr, zr, others)):
        pltpu.make_async_copy(sent, sent, send_sem.at[k]).wait()


def write_kernel(
    grad_v, layer_v, wg_v, table_s,
    layer_hbm, grad_hbm, wg_hbm,
    w_sem, g_sem, l_sem,
):
    edge = grad_v.shape[2]

    def write(row, source, target, sem):
        def step(i, carry):
            at = pl.ds(pl.multiple_of(i * edge, edge), edge)
            pltpu.make_async_copy(source.at[table_s[row, i]], target.at[:, at], sem).start()
            return carry
        lax.fori_loop(0, target.shape[1] // edge, step, 0)

    write(2, grad_v, grad_hbm, g_sem)
    write(3, layer_v, layer_hbm, l_sem)
    wg_copy = pltpu.make_async_copy(wg_v, wg_hbm, w_sem)
    wg_copy.start()
    pltpu.make_async_copy(grad_hbm, grad_hbm, g_sem).wait()
    pltpu.make_async_copy(layer_hbm, layer_hbm, l_sem).wait()
    wg_copy.wait()


def fused(n, dp, hidden, cotangent, tiles, tile_rows, tile_cols, counts):
    tokens, width_ff = hidden.shape
    maxb, edge, _ = tiles.shape
    root = math.sqrt(tokens * n * dp)
    slots, half, stages = n * maxb, maxb // 2, n.bit_length() - 1
    in_hbm = functools.partial(pltpu.with_memory_space_constraint, memory_space=pltpu.HBM)
    rows_z = 2 * edge // dp
    hbm = pl.BlockSpec(memory_space=pltpu.HBM)
    smem = pl.BlockSpec(memory_space=pltpu.SMEM)
    vmem = pl.BlockSpec(memory_space=pltpu.VMEM)
    dma = pltpu.SemaphoreType.DMA
    grad, layer, weight, table = pl.pallas_call(
        functools.partial(fused_kernel, n, dp, root),
        out_shape=(
            pltpu.VMEM((slots + 1, tokens, edge), BF16),
            pltpu.VMEM((slots + 1, tokens, edge), BF16),
            pltpu.VMEM((maxb, edge, edge), F32),
            pltpu.SMEM((8, 128), jnp.int32),
        ),
        in_specs=[hbm, hbm, smem, hbm, hbm, hbm],
        out_specs=(vmem, vmem, vmem, smem),
        scratch_shapes=[
            pltpu.SMEM(tile_rows.shape, jnp.int32),
            pltpu.SMEM(tile_cols.shape, jnp.int32),
            pltpu.VMEM((hidden.shape[1] // edge, tokens, edge), BF16),
            pltpu.VMEM((cotangent.shape[1] // edge, tokens, edge), BF16),
            pltpu.VMEM((n, maxb, edge, edge), BF16),
            pltpu.VMEM((n, 8, 128), jnp.int32),
            pltpu.VMEM((2, 8, 128), jnp.int32),
            pltpu.SMEM((2, 8, 128), jnp.int32),
            pltpu.VMEM((8, 128), jnp.int32),
            pltpu.VMEM((2, n // 2, half, edge, edge), F32),
            pltpu.VMEM((2, n - 1, half, edge, edge), BF16),
            pltpu.VMEM((2, n - 1, half, edge, edge), BF16),
            pltpu.VMEM((half, 2 * edge, edge), F32),
            pltpu.VMEM((half, 2 * edge, edge), BF16),
            pltpu.VMEM((half, dp - 1, rows_z, edge), BF16),
            pltpu.VMEM((half, 2 * edge, edge), BF16),
            pltpu.VMEM((n * dp, 1, 128), F32),
            pltpu.VMEM((slots + 1, tokens, edge), F32),
            pltpu.VMEM((slots + 1, tokens, edge), F32),
            dma((8,)), dma((6,)), dma((2,)),
            dma((n - 1 + max(stages - 2, 0),)),
            dma((n // 2,)), dma((stages - 1, half)), dma((half,)), dma, dma,
        ],
        compiler_params=pltpu.CompilerParams(
            collective_id=0, has_side_effects=True, vmem_limit_bytes=44 * 2 ** 20
        ),
        name="fused",
    )(in_hbm(tile_rows), in_hbm(tile_cols), counts, in_hbm(tiles), in_hbm(hidden), in_hbm(cotangent))
    return pl.pallas_call(
        write_kernel,
        out_shape=(
            jax.ShapeDtypeStruct(cotangent.shape, BF16),
            jax.ShapeDtypeStruct(hidden.shape, BF16),
            jax.ShapeDtypeStruct(tiles.shape, F32),
        ),
        in_specs=[vmem, vmem, vmem, smem],
        out_specs=(hbm, hbm, hbm),
        scratch_shapes=[dma, dma, dma],
        compiler_params=pltpu.CompilerParams(vmem_limit_bytes=16 * 2 ** 20),
        name="write",
    )(grad, layer, weight, table)


def shards(n, dp, hidden, cotangent, tiles, tile_rows, tile_cols, counts):
    tokens, width_ff = hidden.shape
    width_model = cotangent.shape[1]
    maxb, edge, _ = tiles.shape
    blocks_ff, blocks_model = width_ff // edge, width_model // edge
    root = math.sqrt(tokens * n * dp)
    half, per = maxb // 2, maxb // dp
    sums = n * maxb * tokens * edge * 12
    if n == 8 and dp % 2 == 0 and max(n * maxb, blocks_ff, blocks_model) <= 128 and sums <= 28 * 2 ** 20:
        return fused(n, dp, hidden, cotangent, tiles, tile_rows, tile_cols, counts)
    hbm = pl.BlockSpec(memory_space=pl.ANY)
    smem = pl.BlockSpec(memory_space=pltpu.SMEM)
    vmem = pl.BlockSpec(memory_space=pltpu.VMEM)
    dma = pltpu.SemaphoreType.DMA
    meta, gathered, weight_grad = pl.pallas_call(
        functools.partial(exchange_kernel, n, dp, root),
        out_shape=(
            jax.ShapeDtypeStruct((n, 8, 128), jnp.int32),
            jax.ShapeDtypeStruct((n, maxb, edge, edge), BF16),
            jax.ShapeDtypeStruct((maxb, edge, edge), F32),
        ),
        in_specs=[smem, smem, smem, hbm, hbm, hbm],
        out_specs=(hbm, hbm, vmem),
        scratch_shapes=[
            pltpu.VMEM((blocks_ff, tokens, edge), BF16),
            pltpu.VMEM((blocks_model, tokens, edge), BF16),
            pltpu.VMEM((n, maxb, edge, edge), BF16),
            pltpu.VMEM((n, 8, 128), jnp.int32),
            pltpu.SMEM((n, 8, 128), jnp.int32),
            pltpu.VMEM((2, n // 2, half, edge, edge), F32),
            pltpu.VMEM((2, n - 1, half, edge, edge), BF16),
            pltpu.VMEM((2, n - 1, half, edge, edge), BF16),
            pltpu.VMEM((maxb, edge, edge), F32),
            pltpu.VMEM((dp, per, edge, edge), BF16),
            pltpu.VMEM((dp - 1, per, edge, edge), BF16),
            pltpu.VMEM((dp, per, edge, edge), BF16),
            pltpu.VMEM((dp, 8, 128), F32),
            pltpu.VMEM((n, 8, 128), F32),
            dma((4,)), dma((2,)),
            dma((n - 1,)), dma((n - 1,)),
            dma((2, n - 1)), dma((2, n - 1)),
            dma((2, n - 1)), dma((2, n - 1)),
            dma((dp - 1,)), dma((dp - 1,)),
            dma((dp - 1,)), dma((dp - 1,)),
            dma((dp - 1,)), dma((dp - 1,)),
            dma((n - 1,)), dma((n - 1,)),
        ],
        compiler_params=pltpu.CompilerParams(
            collective_id=0, has_side_effects=True, vmem_limit_bytes=60 * 2 ** 20
        ),
        name="exchange",
    )(tile_rows, tile_cols, counts, tiles, hidden, cotangent)

    layer_out, hidden_grad = pl.pallas_call(
        functools.partial(project_kernel, n, maxb),
        out_shape=(
            jax.ShapeDtypeStruct(cotangent.shape, BF16),
            jax.ShapeDtypeStruct(hidden.shape, BF16),
        ),
        in_specs=[smem, hbm, hbm, hbm],
        out_specs=(hbm, hbm),
        scratch_shapes=[
            pltpu.VMEM((n, maxb, edge, edge), BF16),
            pltpu.VMEM(cotangent.shape, BF16),
            pltpu.VMEM((n, maxb, tokens, edge), BF16),
            pltpu.VMEM((blocks_ff, tokens, edge), F32),
            pltpu.VMEM((blocks_ff, tokens, edge), BF16),
            pltpu.VMEM((blocks_model, tokens, edge), F32),
            pltpu.VMEM((blocks_model, tokens, edge), BF16),
            pltpu.VMEM((tokens, edge), BF16),
            pltpu.VMEM((maxb, tokens, edge), F32),
            pltpu.SMEM((blocks_ff,), jnp.int32),
            pltpu.SMEM((blocks_ff,), jnp.int32),
            pltpu.SMEM((blocks_model,), jnp.int32),
            pltpu.SMEM((blocks_model,), jnp.int32),
            dma((2,)), dma, dma, dma,
        ],
        compiler_params=pltpu.CompilerParams(vmem_limit_bytes=62 * 2 ** 20),
        name="project",
    )(meta, gathered, hidden, cotangent)
    return layer_out, hidden_grad, weight_grad


def solution(mesh):
    placed = (
        P(("fsdp", "dp"), None),
        P(("fsdp", "dp"), None),
        P("fsdp", None, None),
        P("fsdp"),
        P("fsdp"),
        P("fsdp"),
    )
    return jax.shard_map(
        functools.partial(shards, mesh.shape["fsdp"], mesh.shape["dp"]),
        mesh=mesh,
        in_specs=placed,
        out_specs=(P(("fsdp", "dp"), None), P(("fsdp", "dp"), None), P("fsdp", None, None)),
        check_vma=False,
    )
```

```python
import functools
import math

import jax
import jax.numpy as jnp
from jax import lax
from jax.experimental import pallas as pl
from jax.experimental.pallas import tpu as pltpu
from jax.sharding import PartitionSpec as P

MESH = pl.DeviceIdType.MESH
F32 = jnp.float32
BF16 = jnp.bfloat16


def exchange_kernel(
    n, dp, root,
    rows_s, cols_s, cnt_s, tiles_hbm, hid_hbm, cot_hbm,
    meta_out, tiles_out, wg_out,
    hid_v, cot_v, tiles_v, meta_v, meta_s, acc, sbuf, rbuf, fin, zs, zr, za, sqz, sqf,
    in_sem, out_sem, meta_ss, meta_rs, ag_ss, ag_rs, rs_ss, rs_rs,
    zs_ss, zs_rs, za_ss, za_rs, qz_ss, qz_rs, qf_ss, qf_rs,
):
    me = lax.axis_index("fsdp")
    z = lax.axis_index("dp")
    maxb, edge = tiles_hbm.shape[0], tiles_hbm.shape[1]
    half = maxb // 2
    per = maxb // dp
    stages = n.bit_length() - 1
    chip_bits = stages - 1
    orders = [list(range(1, stages)), list(range(stages - 1, 0, -1))]
    core = lax.rem(me, 2)

    def bit_of(b):
        return lax.rem(me // (2 ** b), 2)

    def flip(value_me, b):
        return value_me + (1 - 2 * bit_of(b)) * (2 ** b)

    def fetch(source, target, sem):
        def step(i, carry):
            at = pl.ds(pl.multiple_of(i * edge, edge), edge)
            pltpu.make_async_copy(source.at[:, at], target.at[i], sem).start()
            return carry
        lax.fori_loop(0, target.shape[0], step, 0)

    own_copy = pltpu.make_async_copy(tiles_hbm, tiles_v.at[me], in_sem.at[2])
    own_copy.start()
    fetch(cot_hbm, cot_v, in_sem.at[1])
    fetch(hid_hbm, hid_v, in_sem.at[0])

    barrier = pltpu.get_barrier_semaphore()
    for k in range(1, n):
        pl.semaphore_signal(
            barrier, inc=1, device_id={"fsdp": lax.rem(me + k, n)}, device_id_type=MESH
        )
    for k in range(1, dp):
        pl.semaphore_signal(
            barrier, inc=1, device_id={"dp": lax.rem(z + k, dp)}, device_id_type=MESH
        )
    lane = lax.broadcasted_iota(jnp.int32, (8, 128), 1)
    sub = lax.broadcasted_iota(jnp.int32, (8, 128), 0)
    meta = jnp.where(sub == 2, cnt_s[0], 0)
    for j in range(maxb):
        meta = jnp.where((sub == 0) & (lane == j), rows_s[j], meta)
        meta = jnp.where((sub == 1) & (lane == j), cols_s[j], meta)
    meta_v[me] = meta
    own_copy.wait()
    pl.semaphore_wait(barrier, n - 1 + dp - 1)

    meta_copies = []
    for k in range(1, n):
        copy = pltpu.make_async_remote_copy(
            meta_v.at[me], meta_v.at[me], meta_ss.at[k - 1], meta_rs.at[k - 1],
            device_id={"fsdp": lax.rem(me + k, n)}, device_id_type=MESH,
        )
        copy.start()
        meta_copies.append(copy)

    ag_copies = {}

    def ag_send(p, i, e):
        bits = orders[p] + [0]
        owner = me
        for t in range(len(bits)):
            if (e >> t) & 1:
                owner = flip(owner, bits[t])
        piece = tiles_v.at[owner, pl.ds(p * half, half)]
        where = 2 ** i - 1 + e
        copy = pltpu.make_async_remote_copy(
            piece, piece, ag_ss.at[p, where], ag_rs.at[p, where],
            device_id={"fsdp": flip(me, bits[i])}, device_id_type=MESH,
        )
        copy.start()
        ag_copies[p, i, e] = copy

    for i in range(stages):
        for p in range(2):
            ag_send(p, i, 0)

    for copy in meta_copies:
        copy.wait_recv()
    to_smem = pltpu.make_async_copy(meta_v, meta_s, in_sem.at[3])
    to_smem.start()
    to_smem.wait()
    meta_back = pltpu.make_async_copy(meta_v, meta_out, out_sem.at[0])
    meta_back.start()
    pltpu.make_async_copy(cot_v, cot_v, in_sem.at[1]).wait()
    pltpu.make_async_copy(hid_v, hid_v, in_sem.at[0]).wait()

    def owner_at(p, e, core_bit):
        owner = core_bit
        for t, b in enumerate(orders[p]):
            ebit = lax.rem(e // (2 ** (chip_bits - 1 - t)), 2)
            owner = owner + lax.rem(bit_of(b) + 1 + ebit, 2) * (2 ** b)
        return owner

    def term(owner, j):
        return lax.dot_general(
            hid_v[meta_s[owner, 0, j]], cot_v[meta_s[owner, 1, j]],
            (((0,), (0,)), ((), ())), preferred_element_type=F32,
        )

    chips = n // 2
    offsets = [0]
    for t in range(stages):
        offsets.append(offsets[-1] + (n >> (t + 1)))

    def rs_copy(p, t, e):
        where = offsets[t] + e
        bit = 0 if t == 0 else orders[p][t - 1]
        return pltpu.make_async_remote_copy(
            sbuf.at[p, where], rbuf.at[p, where], rs_ss.at[p, where], rs_rs.at[p, where],
            device_id={"fsdp": flip(me, bit)}, device_id_type=MESH,
        )

    def foreign(e, carry):
        for p in range(2):
            owner = owner_at(p, e, 1 - core)
            for j in range(half):
                sbuf[p, e, j] = term(owner, p * half + j).astype(BF16)
            rs_copy(p, 0, e).start()
        return carry

    lax.fori_loop(0, chips, foreign, 0)

    for i in range(chip_bits):
        for p in range(2):
            for e in range(2 ** i):
                ag_copies[p, i, e].wait_recv()
                for i2 in range(i + 1, stages):
                    ag_send(p, i2, e + 2 ** i)

    def own(e, carry):
        for p in range(2):
            owner = owner_at(p, e, core)
            for j in range(half):
                acc[p, e, j] = term(owner, p * half + j)
        return carry

    lax.fori_loop(0, chips, own, 0)

    start = 0
    for t in range(stages):
        m = n >> (t + 1)
        sent = m // 2
        for e in range(m):
            for p in range(2):
                rs_copy(p, t, e).wait_recv()
                total = acc[p, start + e] + rbuf[p, offsets[t] + e].astype(F32)
                if e < sent:
                    sbuf[p, offsets[t + 1] + e] = total.astype(BF16)
                    rs_copy(p, t + 1, e).start()
                elif m > 1:
                    acc[p, start + e] = total
                else:
                    fin[pl.ds(p * half, half)] = total
                    for q in range(half // per):
                        zs[p * (half // per) + q] = total[q * per:(q + 1) * per].astype(BF16)
        start += sent

    def z_peer(r):
        return lax.rem(z + r, dp)

    z_copies = []
    for r in range(1, dp):
        copy = pltpu.make_async_remote_copy(
            zs.at[z_peer(r)], zr.at[r - 1], zs_ss.at[r - 1], zs_rs.at[r - 1],
            device_id={"dp": z_peer(r)}, device_id_type=MESH,
        )
        copy.start()
        z_copies.append(copy)

    for p in range(2):
        for e in range(2 ** chip_bits):
            ag_copies[p, chip_bits, e].wait_recv()
    tiles_back = pltpu.make_async_copy(tiles_v, tiles_out, out_sem.at[1])
    tiles_back.start()

    piece = fin[pl.ds(z * per, per)]
    for r in range(1, dp):
        z_copies[r - 1].wait_recv()
        piece = piece + zr[r - 1].astype(F32)
    slot = z * per + lax.broadcasted_iota(jnp.int32, piece.shape, 0)
    piece = piece * jnp.clip(cnt_s[0] - slot, 0, 1).astype(F32)
    za[z] = piece.astype(BF16)
    sqz[z] = jnp.sum((piece * piece).reshape(-1, 8, 128), axis=0)
    a_copies, q_copies = [], []
    for r in range(1, dp):
        copy = pltpu.make_async_remote_copy(
            sqz.at[z], sqz.at[z], qz_ss.at[r - 1], qz_rs.at[r - 1],
            device_id={"dp": z_peer(r)}, device_id_type=MESH,
        )
        copy.start()
        q_copies.append(copy)
    for r in range(1, dp):
        copy = pltpu.make_async_remote_copy(
            za.at[z], za.at[z], za_ss.at[r - 1], za_rs.at[r - 1],
            device_id={"dp": z_peer(r)}, device_id_type=MESH,
        )
        copy.start()
        a_copies.append(copy)
    for copy in q_copies:
        copy.wait_recv()
    sqf[me] = jnp.sum(sqz[...], axis=0)
    f_copies = []
    for k in range(1, n):
        copy = pltpu.make_async_remote_copy(
            sqf.at[me], sqf.at[me], qf_ss.at[k - 1], qf_rs.at[k - 1],
            device_id={"fsdp": lax.rem(me + k, n)}, device_id_type=MESH,
        )
        copy.start()
        f_copies.append(copy)
    entries = meta_s[0, 2, 0]
    for k in range(1, n):
        entries = entries + meta_s[k, 2, 0]
    for copy in a_copies + f_copies:
        copy.wait_recv()
    squares = jnp.sum(jnp.sum(sqf[...], axis=0), axis=(0, 1), keepdims=True)
    live = jnp.full((1, 1), entries, jnp.int32).astype(F32) * edge * edge
    spread = jnp.sqrt(squares / live)
    factor = jnp.minimum(1.0, 0.5 * root / spread) / root
    for q in range(dp):
        for i in range(per):
            wg_out[q * per + i] = za[q, i].astype(F32) * factor

    for copy in meta_copies + list(ag_copies.values()) + z_copies + q_copies + a_copies + f_copies:
        copy.wait_send()
    for t in range(stages):
        for e in range(n >> (t + 1)):
            for p in range(2):
                rs_copy(p, t, e).wait_send()
    meta_back.wait()
    tiles_back.wait()


def project_kernel(
    n, maxb,
    meta_s, tiles_hbm, hid_hbm, cot_hbm,
    layer_hbm, grad_hbm,
    tiles_v, cot_v, hid_v, gacc, gout, lacc, lout, zero_v, values,
    row_left, row_seen, col_left, col_seen,
    in_sem, hid_sem, g_sem, l_sem,
):
    edge = zero_v.shape[1]
    tile_copy = pltpu.make_async_copy(tiles_hbm, tiles_v, in_sem.at[0])
    cot_copy = pltpu.make_async_copy(cot_hbm, cot_v, in_sem.at[1])
    tile_copy.start()
    cot_copy.start()
    zero_v[...] = jnp.zeros_like(zero_v)

    def clear(left, seen):
        def step(i, carry):
            left[i] = 0
            seen[i] = 0
            return carry
        lax.fori_loop(0, left.shape[0], step, 0)

    clear(row_left, row_seen)
    clear(col_left, col_seen)

    def columns(i):
        return pl.ds(pl.multiple_of(i * edge, edge), edge)

    def each_live(visit):
        def owner(o, carry):
            def slot(j, inner):
                visit(o, j, meta_s[o, 0, j], meta_s[o, 1, j])
                return inner
            return lax.fori_loop(0, meta_s[o, 2, 0], slot, carry)
        lax.fori_loop(0, n, owner, 0)

    def fetch(o, j, row, col):
        pltpu.make_async_copy(hid_hbm.at[:, columns(row)], hid_v.at[o, j], hid_sem).start()
        row_left[row] = row_left[row] + 1
        col_left[col] = col_left[col] + 1

    each_live(fetch)

    def blank(left, target, sem):
        def step(i, carry):
            @pl.when(left[i] == 0)
            def _():
                pltpu.make_async_copy(zero_v, target.at[:, columns(i)], sem).start()
            return carry
        lax.fori_loop(0, left.shape[0], step, 0)

    blank(row_left, grad_hbm, g_sem)
    blank(col_left, layer_hbm, l_sem)
    tile_copy.wait()
    cot_copy.wait()

    def add_block(at, value, left, seen, total, out, target, sem):
        remaining = left[at] - 1
        first = seen[at] == 0
        left[at] = remaining
        seen[at] = 1

        @pl.when(first & (remaining == 0))
        def _():
            out[at] = value[...].astype(BF16)

        @pl.when(first & (remaining > 0))
        def _():
            total[at] = value[...]

        @pl.when(jnp.logical_not(first))
        def _():
            summed = total[at] + value[...]
            total[at] = summed
            out[at] = summed.astype(BF16)

        @pl.when(remaining == 0)
        def _():
            pltpu.make_async_copy(out.at[at], target.at[:, columns(at)], sem).start()

    def backward(o, carry):
        for j in range(maxb):
            values[j] = lax.dot_general(
                cot_v[:, columns(meta_s[o, 1, j])], tiles_v[o, j], (((1,), (1,)), ((), ())),
                preferred_element_type=F32,
            )

        def slot(j, inner):
            add_block(
                meta_s[o, 0, j], values.at[j], row_left, row_seen, gacc, gout, grad_hbm, g_sem
            )
            return inner

        return lax.fori_loop(0, meta_s[o, 2, 0], slot, carry)

    lax.fori_loop(0, n, backward, 0)

    def arrived(o, j, row, col):
        pltpu.make_async_copy(hid_hbm.at[:, columns(row)], hid_v.at[o, j], hid_sem).wait()

    each_live(arrived)

    def forward(o, carry):
        for j in range(maxb):
            values[j] = jnp.dot(hid_v[o, j], tiles_v[o, j], preferred_element_type=F32)

        def slot(j, inner):
            add_block(
                meta_s[o, 1, j], values.at[j], col_left, col_seen, lacc, lout, layer_hbm, l_sem
            )
            return inner

        return lax.fori_loop(0, meta_s[o, 2, 0], slot, carry)

    lax.fori_loop(0, n, forward, 0)
    pltpu.make_async_copy(grad_hbm, grad_hbm, g_sem).wait()
    pltpu.make_async_copy(layer_hbm, layer_hbm, l_sem).wait()


def fused_kernel(
    n, dp, root,
    rows_hbm, cols_hbm, cnt_s, tiles_hbm, hid_hbm, cot_hbm,
    grad_out, layer_out, wg_out, table_s,
    rows_s, cols_s, hid_v, cot_v, tiles_v, meta_v, full_v, full_s, table_v,
    acc, sbuf, rbuf, fin, zs, zr, za, sqf, grad_q, layer_q,
    in_sem, send_sem, meta_rs, ag_rs, pair_rs, rs_rs, z_rs, za_rs, sq_rs,
):
    me = lax.axis_index("fsdp")
    z = lax.axis_index("dp")
    maxb, edge = tiles_hbm.shape[0], tiles_hbm.shape[1]
    slots = n * maxb
    half = maxb // 2
    rows_z = 2 * edge // dp
    stages = n.bit_length() - 1
    chip_bits = stages - 1
    chips = n // 2
    orders = [list(range(1, stages)), list(range(stages - 1, 0, -1))]

    def bit_of(b):
        return lax.rem(me // (2 ** b), 2)

    def relative(x):
        other = me
        for b in range(stages):
            if (x >> b) & 1:
                other = other + (1 - 2 * bit_of(b)) * (2 ** b)
        return other

    def z_peer(r):
        return lax.rem(z + r, dp)

    near = [x for x in range(n) if bin(x >> 1).count("1") < 2]
    far = [x for x in range(n) if x not in near]
    queue = [0, 1] + [x for x in near if x > 1 and x % 2 == 0]
    queue += [x for x in near if x > 1 and x % 2 == 1] + far
    place = [queue.index(x) for x in range(n)]

    def fetch(source, target, sem, first, last):
        def step(i, carry):
            at = pl.ds(pl.multiple_of(i * edge, edge), edge)
            pltpu.make_async_copy(source.at[:, at], target.at[i], sem).start()
            return carry
        lax.fori_loop(first, last, step, 0)

    def blocks_wait(count, sem):
        if count <= maxb:
            blocks = tiles_v.at[0, pl.ds(0, count)]
        else:
            blocks = tiles_v.at[pl.ds(0, count // maxb)]
        pltpu.make_async_copy(blocks, blocks, sem).wait()

    barrier = pltpu.get_barrier_semaphore()
    for r in range(1, dp):
        pl.semaphore_signal(
            barrier, inc=1, device_id={"dp": z_peer(r)}, device_id_type=MESH
        )
    for x in range(n - 1, 0, -1):
        pl.semaphore_signal(
            barrier, inc=1, device_id={"fsdp": relative(x)}, device_id_type=MESH
        )
    rows_copy = pltpu.make_async_copy(rows_hbm, rows_s, in_sem.at[2])
    rows_copy.start()
    cols_copy = pltpu.make_async_copy(cols_hbm, cols_s, in_sem.at[3])
    cols_copy.start()
    own_copy = pltpu.make_async_copy(tiles_hbm, tiles_v.at[0], in_sem.at[7])
    own_copy.start()

    early = hid_v.shape[0] * 3 // 8
    fetch(cot_hbm, cot_v, in_sem.at[1], 0, cot_v.shape[0])
    fetch(hid_hbm, hid_v, in_sem.at[0], 0, early)

    lane = lax.broadcasted_iota(jnp.int32, (8, 128), 1)
    sub = lax.broadcasted_iota(jnp.int32, (8, 128), 0)
    meta = jnp.where(sub == 2, cnt_s[0], 0)
    rows_copy.wait()
    cols_copy.wait()
    for j in range(maxb):
        here = lax.rem(lane, maxb) == j
        meta = jnp.where((sub == 0) & here, rows_s[j], meta)
        meta = jnp.where((sub == 1) & here, cols_s[j], meta)
    meta_v[0] = meta
    pl.semaphore_wait(barrier, n - 1 + dp - 1)

    for x in range(n - 1, 0, -1):
        pltpu.make_async_remote_copy(
            meta_v.at[0], meta_v.at[place[x]], send_sem.at[0], meta_rs.at[int(x in far)],
            device_id={"fsdp": relative(x)}, device_id_type=MESH,
        ).start()
    own_copy.wait()

    ag_done = set()

    def ag_index(i, e, h):
        split = 0 < i < chip_bits and e == 0
        keys = [(i, e, h) for i in range(stages) for e in range(2 ** i) for h in range(2)
                if h == 0 or (0 < i < chip_bits and e == 0)]
        return keys.index((i, e, h if split else 0)), maxb // 2 if split else maxb

    def ag_send(p, i, e, h):
        bits = orders[p] + [0]
        owner = 0
        for t in range(len(bits)):
            if (e >> t) & 1:
                owner |= 1 << bits[t]
        part = pl.ds(p * half + h * (half // 2), half // 2)
        pltpu.make_async_remote_copy(
            tiles_v.at[place[owner], part], tiles_v.at[place[owner | (1 << bits[i])], part],
            send_sem.at[1], ag_rs.at[ag_index(i, e, h)[0]],
            device_id={"fsdp": relative(1 << bits[i])}, device_id_type=MESH,
        ).start()

    def ag_wait(i, e, h):
        index, count = ag_index(i, e, h)
        if index not in ag_done:
            ag_done.add(index)
            blocks_wait(count, ag_rs.at[index])

    for i in range(stages):
        for p in range(2):
            for h in range(2):
                if h == 0 or i == 0 or i == chip_bits:
                    ag_send(p, i, 0, h)

    grad_q[slots] = jnp.zeros(grad_q.shape[1:], F32)
    layer_q[slots] = jnp.zeros(layer_q.shape[1:], F32)
    grad_out[slots] = jnp.zeros(grad_out.shape[1:], BF16)
    layer_out[slots] = jnp.zeros(layer_out.shape[1:], BF16)

    fetch(hid_hbm, hid_v, in_sem.at[0], early, hid_v.shape[0])

    def collect(xs, full):
        arrive = [x for x in xs if x]
        first = min(place[x] for x in arrive)
        metas = meta_v.at[pl.ds(first, len(arrive))]
        pltpu.make_async_copy(metas, metas, meta_rs.at[int(xs is far)]).wait()
        for x in xs:
            full = jnp.where(lane // maxb == place[x], meta_v[place[x]], full)
        return full

    def to_smem(k):
        return pltpu.make_async_copy(full_v.at[k], full_s.at[k], in_sem.at[4 + k])

    known = collect(near, jnp.zeros((8, 128), jnp.int32))
    full_v[0] = known
    to_smem(0).start()

    def term(x, j, named=None):
        q = place[x] * maxb + j
        k = 0 if x in near else 1
        row = full_s[k, 0, q] if named is None else named[0, q]
        col = full_s[k, 1, q] if named is None else named[1, q]
        return lax.dot_general(
            hid_v[row], cot_v[col],
            (((0,), (0,)), ((), ())), preferred_element_type=F32,
        )

    def owner_at(p, e):
        owner = 0
        for t, b in enumerate(orders[p]):
            if not (e >> (chip_bits - 1 - t)) & 1:
                owner |= 1 << b
        return owner

    offsets = [0]
    for t in range(stages):
        offsets.append(offsets[-1] + (n >> (t + 1)))

    def pair_copy(p, e):
        return pltpu.make_async_remote_copy(
            sbuf.at[p, e], rbuf.at[p, e], send_sem.at[2], pair_rs.at[e],
            device_id={"fsdp": relative(1)}, device_id_type=MESH,
        )

    def rs_copy(p, t, e, c):
        where = offsets[t] + e
        return pltpu.make_async_remote_copy(
            sbuf.at[p, where, c], rbuf.at[p, where, c],
            send_sem.at[2], rs_rs.at[t - 1, c],
            device_id={"fsdp": relative(1 << orders[p][t - 1])}, device_id_type=MESH,
        )

    def foreign(e, named=None):
        for p in range(2):
            for c in range(half):
                sbuf[p, e, c] = term(owner_at(p, e) | 1, p * half + c, named).astype(BF16)
        for p in range(2):
            pair_copy(p, e).start()

    def own(e):
        for p in range(2):
            for c in range(half):
                acc[p, e, c] = term(owner_at(p, e), p * half + c)

    starts = [0]
    for t in range(stages):
        starts.append(starts[-1] + (n >> (t + 1)) // 2)

    paired = set()

    def pair_wait(e):
        if e not in paired:
            paired.add(e)
            blocks_wait(maxb, pair_rs.at[e])

    def pass_on(e, cs):
        for p in range(2):
            pair_wait(e)
            for c in cs:
                total = acc[p, e, c] + rbuf[p, e, c].astype(F32)
                sbuf[p, offsets[1] + e, c] = total.astype(BF16)
            for c in cs:
                rs_copy(p, 1, e, c).start()

    def reduce_step(t, c):
        m = n >> (t + 1)
        blocks_wait(2 * m, rs_rs.at[t - 1, c])
        for e in range(m):
            for p in range(2):
                at_e = starts[t] + e
                total = acc[p, at_e, c] + rbuf[p, offsets[t] + e, c].astype(F32)
                if t == 1:
                    total = total + rbuf[p, at_e, c].astype(F32)
                if e < m // 2:
                    sbuf[p, offsets[t + 1] + e, c] = total.astype(BF16)
                    rs_copy(p, t + 1, e, c).start()
                elif m > 1:
                    acc[p, at_e, c] = total
                else:
                    at = pl.ds(p * edge, edge)
                    fin[c, at] = total
                    zs[c, at] = total.astype(BF16)
        if m == 1:
            for r in range(1, dp):
                z_copy(c, r).start()

    def z_rows(index):
        return pl.ds(pl.multiple_of(index * rows_z, rows_z), rows_z)

    def z_copy(c, r):
        return pltpu.make_async_remote_copy(
            zs.at[c, z_rows(z_peer(r))], zr.at[c, r - 1], send_sem.at[3], z_rs.at[c],
            device_id={"dp": z_peer(r)}, device_id_type=MESH,
        )

    def a_copy(c, r):
        return pltpu.make_async_remote_copy(
            za.at[c, z_rows(z)], za.at[c, z_rows(z)], send_sem.at[4], za_rs,
            device_id={"dp": z_peer(r)}, device_id_type=MESH,
        )

    def z_sum(c, squares):
        piece = fin[c, z_rows(z)]
        pltpu.make_async_copy(zr.at[c], zr.at[c], z_rs.at[c]).wait()
        for r in range(1, dp):
            piece = piece + zr[c, r - 1].astype(F32)
        row = z * rows_z + lax.broadcasted_iota(jnp.int32, piece.shape, 0)
        slot = (row // edge) * half + c
        piece = piece * jnp.clip(cnt_s[0] - slot, 0, 1).astype(F32)
        za[c, z_rows(z)] = piece.astype(BF16)
        return squares + jnp.sum((piece * piece).reshape(-1, 8, 128), axis=0)

    def a_send(c):
        for r in range(1, dp):
            a_copy(c, r).start()

    def z_step(c, squares):
        squares = z_sum(c, squares)
        a_send(c)
        return squares

    def project(at):
        def load(j):
            q = at * maxb + j
            backward = lax.dot_general(
                cot_v[full_s[1, 1, q]], tiles_v[at, j], (((1,), (1,)), ((), ())),
                preferred_element_type=F32,
            )
            forward = jnp.dot(hid_v[full_s[1, 0, q]], tiles_v[at, j], preferred_element_type=F32)
            return q, backward, forward
        for j in range(maxb):
            q, backward, forward = load(j)
            backward = backward + grad_q[table_s[0, q]]
            grad_q[q] = backward
            grad_out[q] = backward.astype(BF16)
            forward = forward + layer_q[table_s[1, q]]
            layer_q[q] = forward
            layer_out[q] = forward.astype(BF16)

    def arrived(x):
        for p in range(2):
            bits = orders[p] + [0]
            index = [t for t in range(stages) if (x >> bits[t]) & 1]
            if index:
                e = sum(1 << t for t in index[:-1])
                for h in range(2):
                    ag_wait(index[-1], e, h)

    sent = sorted(range(chips // 2), key=lambda e: bin(owner_at(0, e)).count("1"))
    kept = list(range(chips // 2, chips))
    pltpu.make_async_copy(cot_v, cot_v, in_sem.at[1]).wait()
    pltpu.make_async_copy(hid_v, hid_v, in_sem.at[0]).wait()
    foreign(sent[0], known)
    to_smem(0).wait()
    full = collect(far, known)
    full_v[1] = full
    to_smem(1).start()
    own(sent[0])
    to_smem(1).wait()
    for k in range(1, len(sent)):
        foreign(sent[k])
        pass_on(sent[k - 1], [0])
        own(sent[k])
    foreign(kept[0])
    pass_on(sent[-1], [0])
    for c in range(1, half - 1):
        for e in sent:
            pass_on(e, [c])
    for e in kept[1:]:
        foreign(e)

    wide = lax.broadcasted_iota(jnp.int32, (slots, 128), 1)
    tall = lax.broadcasted_iota(jnp.int32, (slots, 128), 0)
    alive = lax.rem(lane[0:1], maxb) < full[2:3]
    table = jnp.full((8, 128), slots, jnp.int32)
    for k in range(2):
        named = jnp.broadcast_to(jnp.where(alive, full[k:k + 1], -1), (slots, 128))
        named_t = jnp.sum(jnp.where(wide == tall, named, 0), axis=1, keepdims=True)
        before = jnp.max(
            jnp.where((named_t == named) & (tall < wide), tall, -1), axis=0, keepdims=True
        )
        last = jnp.max(jnp.where(named_t == wide, tall, -1), axis=0, keepdims=True)
        table = jnp.where(sub == k, jnp.where(before < 0, slots, before), table)
        table = jnp.where(sub == 2 + k, jnp.where(last < 0, slots, last), table)
    table_v[...] = table
    table_copy = pltpu.make_async_copy(table_v, table_s, in_sem.at[6])
    table_copy.start()
    for e in kept:
        own(e)
    table_copy.wait()

    def project_all(xs):
        for x in xs:
            arrived(x)
        first = place[xs[0]]

        def one(at, carry):
            project(at)
            return carry

        lax.fori_loop(first, first + len(xs), one, 0)

    def ag_pass(i, e, h):
        ag_wait(i, e, h)
        for p in range(2):
            ag_send(p, chip_bits, e + 2 ** i, h)

    project_all([0, 1])
    for h in range(2):
        for i in range(chip_bits if h == 0 else 1):
            ag_pass(i, 0, h)
    for e in kept:
        pair_wait(e)
    reduce_step(1, 0)
    for e in sent:
        pass_on(e, [half - 1])

    def second(c, carry):
        reduce_step(1, c)
        return carry

    lax.fori_loop(1, half - 1, second, 0)
    for t in range(2, stages):
        reduce_step(t, 0)
    reduce_step(1, half - 1)
    for t in range(2, stages):
        def third(c, carry):
            reduce_step(t, c)
            return carry

        lax.fori_loop(1, half, third, 0)

    for i in range(1, chip_bits):
        for p in range(2):
            ag_send(p, i, 0, 1)
    for i in range(1, chip_bits):
        for e in range(1, 2 ** i):
            for p in range(2):
                for h in range(2):
                    ag_wait(i - 1, e - 2 ** (i - 1), h)
                    ag_send(p, i, e, h)

    squares = lax.fori_loop(0, half // 2, z_step, jnp.zeros((8, 128), F32))
    for i in range(1, chip_bits):
        ag_pass(i, 0, 1)
    project_all([x for x in near if x > 1 and x % 2 == 0])
    squares = lax.fori_loop(half // 2, half - 1, z_step, squares)
    squares = z_sum(half - 1, squares)
    device = me * dp + z
    sqf[device] = jnp.sum(squares, axis=0, keepdims=True)
    for x in reversed(queue):
        for r in range(dp):
            if x or r:
                pltpu.make_async_remote_copy(
                    sqf.at[device], sqf.at[device], send_sem.at[5], sq_rs,
                    device_id={"fsdp": relative(x), "dp": z_peer(r)}, device_id_type=MESH,
                ).start()
    a_send(half - 1)
    project_all([x for x in near if x > 1 and x % 2 == 1])
    for i in range(1, chip_bits):
        for e in range(1, 2 ** i):
            for h in range(2):
                ag_pass(i, e, h)
    project_all(far)

    entries = full_s[1, 2, 0]
    for x in range(1, n):
        entries = entries + full_s[1, 2, x * maxb]
    others = sqf.at[pl.ds(0, n * dp - 1)]
    pltpu.make_async_copy(others, others, sq_rs).wait()
    squares = jnp.sum(jnp.sum(sqf[...], axis=0), axis=1, keepdims=True)
    live = jnp.full((1, 1), entries, jnp.int32).astype(F32) * edge * edge
    spread = jnp.sqrt(squares / live)
    factor = jnp.minimum(1.0, 0.5 * root / spread) / root

    pltpu.make_async_copy(zr, zr, za_rs).wait()

    def finish(c, carry):
        for p in range(2):
            wg_out[p * half + c] = za[c, pl.ds(p * edge, edge)].astype(F32) * factor
        return carry

    lax.fori_loop(0, half, finish, 0)

    metas = meta_v.at[pl.ds(1, n - 1)]
    gathered = tiles_v.at[pl.ds(1, n - 1)]
    for k, sent in enumerate((metas, gathered, sbuf, zr, zr, others)):
        pltpu.make_async_copy(sent, sent, send_sem.at[k]).wait()


def write_kernel(
    grad_v, layer_v, wg_v, table_s,
    layer_hbm, grad_hbm, wg_hbm,
    w_sem, g_sem, l_sem,
):
    edge = grad_v.shape[2]

    def write(row, source, target, sem):
        def step(i, carry):
            at = pl.ds(pl.multiple_of(i * edge, edge), edge)
            pltpu.make_async_copy(source.at[table_s[row, i]], target.at[:, at], sem).start()
            return carry
        lax.fori_loop(0, target.shape[1] // edge, step, 0)

    write(2, grad_v, grad_hbm, g_sem)
    write(3, layer_v, layer_hbm, l_sem)
    wg_copy = pltpu.make_async_copy(wg_v, wg_hbm, w_sem)
    wg_copy.start()
    pltpu.make_async_copy(grad_hbm, grad_hbm, g_sem).wait()
    pltpu.make_async_copy(layer_hbm, layer_hbm, l_sem).wait()
    wg_copy.wait()


def fused(n, dp, hidden, cotangent, tiles, tile_rows, tile_cols, counts):
    tokens, width_ff = hidden.shape
    maxb, edge, _ = tiles.shape
    root = math.sqrt(tokens * n * dp)
    slots, half, stages = n * maxb, maxb // 2, n.bit_length() - 1
    in_hbm = functools.partial(pltpu.with_memory_space_constraint, memory_space=pltpu.HBM)
    rows_z = 2 * edge // dp
    hbm = pl.BlockSpec(memory_space=pltpu.HBM)
    smem = pl.BlockSpec(memory_space=pltpu.SMEM)
    vmem = pl.BlockSpec(memory_space=pltpu.VMEM)
    dma = pltpu.SemaphoreType.DMA
    grad, layer, weight, table = pl.pallas_call(
        functools.partial(fused_kernel, n, dp, root),
        out_shape=(
            pltpu.VMEM((slots + 1, tokens, edge), BF16),
            pltpu.VMEM((slots + 1, tokens, edge), BF16),
            pltpu.VMEM((maxb, edge, edge), F32),
            pltpu.SMEM((8, 128), jnp.int32),
        ),
        in_specs=[hbm, hbm, smem, hbm, hbm, hbm],
        out_specs=(vmem, vmem, vmem, smem),
        scratch_shapes=[
            pltpu.SMEM(tile_rows.shape, jnp.int32),
            pltpu.SMEM(tile_cols.shape, jnp.int32),
            pltpu.VMEM((hidden.shape[1] // edge, tokens, edge), BF16),
            pltpu.VMEM((cotangent.shape[1] // edge, tokens, edge), BF16),
            pltpu.VMEM((n, maxb, edge, edge), BF16),
            pltpu.VMEM((n, 8, 128), jnp.int32),
            pltpu.VMEM((2, 8, 128), jnp.int32),
            pltpu.SMEM((2, 8, 128), jnp.int32),
            pltpu.VMEM((8, 128), jnp.int32),
            pltpu.VMEM((2, n // 2, half, edge, edge), F32),
            pltpu.VMEM((2, n - 1, half, edge, edge), BF16),
            pltpu.VMEM((2, n - 1, half, edge, edge), BF16),
            pltpu.VMEM((half, 2 * edge, edge), F32),
            pltpu.VMEM((half, 2 * edge, edge), BF16),
            pltpu.VMEM((half, dp - 1, rows_z, edge), BF16),
            pltpu.VMEM((half, 2 * edge, edge), BF16),
            pltpu.VMEM((n * dp, 1, 128), F32),
            pltpu.VMEM((slots + 1, tokens, edge), F32),
            pltpu.VMEM((slots + 1, tokens, edge), F32),
            dma((8,)), dma((6,)), dma((2,)),
            dma((n - 1 + max(stages - 2, 0),)),
            dma((n // 2,)), dma((stages - 1, half)), dma((half,)), dma, dma,
        ],
        compiler_params=pltpu.CompilerParams(
            collective_id=0, has_side_effects=True, vmem_limit_bytes=44 * 2 ** 20
        ),
        name="fused",
    )(in_hbm(tile_rows), in_hbm(tile_cols), counts, in_hbm(tiles), in_hbm(hidden), in_hbm(cotangent))
    return pl.pallas_call(
        write_kernel,
        out_shape=(
            jax.ShapeDtypeStruct(cotangent.shape, BF16),
            jax.ShapeDtypeStruct(hidden.shape, BF16),
            jax.ShapeDtypeStruct(tiles.shape, F32),
        ),
        in_specs=[vmem, vmem, vmem, smem],
        out_specs=(hbm, hbm, hbm),
        scratch_shapes=[dma, dma, dma],
        compiler_params=pltpu.CompilerParams(vmem_limit_bytes=16 * 2 ** 20),
        name="write",
    )(grad, layer, weight, table)


def shards(n, dp, hidden, cotangent, tiles, tile_rows, tile_cols, counts):
    tokens, width_ff = hidden.shape
    width_model = cotangent.shape[1]
    maxb, edge, _ = tiles.shape
    blocks_ff, blocks_model = width_ff // edge, width_model // edge
    root = math.sqrt(tokens * n * dp)
    half, per = maxb // 2, maxb // dp
    sums = n * maxb * tokens * edge * 12
    if n == 8 and dp % 2 == 0 and max(n * maxb, blocks_ff, blocks_model) <= 128 and sums <= 28 * 2 ** 20:
        return fused(n, dp, hidden, cotangent, tiles, tile_rows, tile_cols, counts)
    hbm = pl.BlockSpec(memory_space=pl.ANY)
    smem = pl.BlockSpec(memory_space=pltpu.SMEM)
    vmem = pl.BlockSpec(memory_space=pltpu.VMEM)
    dma = pltpu.SemaphoreType.DMA
    meta, gathered, weight_grad = pl.pallas_call(
        functools.partial(exchange_kernel, n, dp, root),
        out_shape=(
            jax.ShapeDtypeStruct((n, 8, 128), jnp.int32),
            jax.ShapeDtypeStruct((n, maxb, edge, edge), BF16),
            jax.ShapeDtypeStruct((maxb, edge, edge), F32),
        ),
        in_specs=[smem, smem, smem, hbm, hbm, hbm],
        out_specs=(hbm, hbm, vmem),
        scratch_shapes=[
            pltpu.VMEM((blocks_ff, tokens, edge), BF16),
            pltpu.VMEM((blocks_model, tokens, edge), BF16),
            pltpu.VMEM((n, maxb, edge, edge), BF16),
            pltpu.VMEM((n, 8, 128), jnp.int32),
            pltpu.SMEM((n, 8, 128), jnp.int32),
            pltpu.VMEM((2, n // 2, half, edge, edge), F32),
            pltpu.VMEM((2, n - 1, half, edge, edge), BF16),
            pltpu.VMEM((2, n - 1, half, edge, edge), BF16),
            pltpu.VMEM((maxb, edge, edge), F32),
            pltpu.VMEM((dp, per, edge, edge), BF16),
            pltpu.VMEM((dp - 1, per, edge, edge), BF16),
            pltpu.VMEM((dp, per, edge, edge), BF16),
            pltpu.VMEM((dp, 8, 128), F32),
            pltpu.VMEM((n, 8, 128), F32),
            dma((4,)), dma((2,)),
            dma((n - 1,)), dma((n - 1,)),
            dma((2, n - 1)), dma((2, n - 1)),
            dma((2, n - 1)), dma((2, n - 1)),
            dma((dp - 1,)), dma((dp - 1,)),
            dma((dp - 1,)), dma((dp - 1,)),
            dma((dp - 1,)), dma((dp - 1,)),
            dma((n - 1,)), dma((n - 1,)),
        ],
        compiler_params=pltpu.CompilerParams(
            collective_id=0, has_side_effects=True, vmem_limit_bytes=60 * 2 ** 20
        ),
        name="exchange",
    )(tile_rows, tile_cols, counts, tiles, hidden, cotangent)

    layer_out, hidden_grad = pl.pallas_call(
        functools.partial(project_kernel, n, maxb),
        out_shape=(
            jax.ShapeDtypeStruct(cotangent.shape, BF16),
            jax.ShapeDtypeStruct(hidden.shape, BF16),
        ),
        in_specs=[smem, hbm, hbm, hbm],
        out_specs=(hbm, hbm),
        scratch_shapes=[
            pltpu.VMEM((n, maxb, edge, edge), BF16),
            pltpu.VMEM(cotangent.shape, BF16),
            pltpu.VMEM((n, maxb, tokens, edge), BF16),
            pltpu.VMEM((blocks_ff, tokens, edge), F32),
            pltpu.VMEM((blocks_ff, tokens, edge), BF16),
            pltpu.VMEM((blocks_model, tokens, edge), F32),
            pltpu.VMEM((blocks_model, tokens, edge), BF16),
            pltpu.VMEM((tokens, edge), BF16),
            pltpu.VMEM((maxb, tokens, edge), F32),
            pltpu.SMEM((blocks_ff,), jnp.int32),
            pltpu.SMEM((blocks_ff,), jnp.int32),
            pltpu.SMEM((blocks_model,), jnp.int32),
            pltpu.SMEM((blocks_model,), jnp.int32),
            dma((2,)), dma, dma, dma,
        ],
        compiler_params=pltpu.CompilerParams(vmem_limit_bytes=62 * 2 ** 20),
        name="project",
    )(meta, gathered, hidden, cotangent)
    return layer_out, hidden_grad, weight_grad


def solution(mesh):
    placed = (
        P(("fsdp", "dp"), None),
        P(("fsdp", "dp"), None),
        P("fsdp", None, None),
        P("fsdp"),
        P("fsdp"),
        P("fsdp"),
    )
    return jax.shard_map(
        functools.partial(shards, mesh.shape["fsdp"], mesh.shape["dp"]),
        mesh=mesh,
        in_specs=placed,
        out_specs=(P(("fsdp", "dp"), None), P(("fsdp", "dp"), None), P("fsdp", None, None)),
        check_vma=False,
    )
```

```python
import functools
import math

import jax
import jax.numpy as jnp
from jax import lax
from jax.experimental import pallas as pl
from jax.experimental.pallas import tpu as pltpu
from jax.sharding import PartitionSpec as P

MESH = pl.DeviceIdType.MESH
F32 = jnp.float32
BF16 = jnp.bfloat16


def exchange_kernel(
    n, dp, root,
    rows_s, cols_s, cnt_s, tiles_hbm, hid_hbm, cot_hbm,
    meta_out, tiles_out, wg_out,
    hid_v, cot_v, tiles_v, meta_v, meta_s, acc, sbuf, rbuf, fin, zs, zr, za, sqz, sqf,
    in_sem, out_sem, meta_ss, meta_rs, ag_ss, ag_rs, rs_ss, rs_rs,
    zs_ss, zs_rs, za_ss, za_rs, qz_ss, qz_rs, qf_ss, qf_rs,
):
    me = lax.axis_index("fsdp")
    z = lax.axis_index("dp")
    maxb, edge = tiles_hbm.shape[0], tiles_hbm.shape[1]
    half = maxb // 2
    per = maxb // dp
    stages = n.bit_length() - 1
    chip_bits = stages - 1
    orders = [list(range(1, stages)), list(range(stages - 1, 0, -1))]
    core = lax.rem(me, 2)

    def bit_of(b):
        return lax.rem(me // (2 ** b), 2)

    def flip(value_me, b):
        return value_me + (1 - 2 * bit_of(b)) * (2 ** b)

    def fetch(source, target, sem):
        def step(i, carry):
            at = pl.ds(pl.multiple_of(i * edge, edge), edge)
            pltpu.make_async_copy(source.at[:, at], target.at[i], sem).start()
            return carry
        lax.fori_loop(0, target.shape[0], step, 0)

    own_copy = pltpu.make_async_copy(tiles_hbm, tiles_v.at[me], in_sem.at[2])
    own_copy.start()
    fetch(cot_hbm, cot_v, in_sem.at[1])
    fetch(hid_hbm, hid_v, in_sem.at[0])

    barrier = pltpu.get_barrier_semaphore()
    for k in range(1, n):
        pl.semaphore_signal(
            barrier, inc=1, device_id={"fsdp": lax.rem(me + k, n)}, device_id_type=MESH
        )
    for k in range(1, dp):
        pl.semaphore_signal(
            barrier, inc=1, device_id={"dp": lax.rem(z + k, dp)}, device_id_type=MESH
        )
    lane = lax.broadcasted_iota(jnp.int32, (8, 128), 1)
    sub = lax.broadcasted_iota(jnp.int32, (8, 128), 0)
    meta = jnp.where(sub == 2, cnt_s[0], 0)
    for j in range(maxb):
        meta = jnp.where((sub == 0) & (lane == j), rows_s[j], meta)
        meta = jnp.where((sub == 1) & (lane == j), cols_s[j], meta)
    meta_v[me] = meta
    own_copy.wait()
    pl.semaphore_wait(barrier, n - 1 + dp - 1)

    meta_copies = []
    for k in range(1, n):
        copy = pltpu.make_async_remote_copy(
            meta_v.at[me], meta_v.at[me], meta_ss.at[k - 1], meta_rs.at[k - 1],
            device_id={"fsdp": lax.rem(me + k, n)}, device_id_type=MESH,
        )
        copy.start()
        meta_copies.append(copy)

    ag_copies = {}

    def ag_send(p, i, e):
        bits = orders[p] + [0]
        owner = me
        for t in range(len(bits)):
            if (e >> t) & 1:
                owner = flip(owner, bits[t])
        piece = tiles_v.at[owner, pl.ds(p * half, half)]
        where = 2 ** i - 1 + e
        copy = pltpu.make_async_remote_copy(
            piece, piece, ag_ss.at[p, where], ag_rs.at[p, where],
            device_id={"fsdp": flip(me, bits[i])}, device_id_type=MESH,
        )
        copy.start()
        ag_copies[p, i, e] = copy

    for i in range(stages):
        for p in range(2):
            ag_send(p, i, 0)

    for copy in meta_copies:
        copy.wait_recv()
    to_smem = pltpu.make_async_copy(meta_v, meta_s, in_sem.at[3])
    to_smem.start()
    to_smem.wait()
    meta_back = pltpu.make_async_copy(meta_v, meta_out, out_sem.at[0])
    meta_back.start()
    pltpu.make_async_copy(cot_v, cot_v, in_sem.at[1]).wait()
    pltpu.make_async_copy(hid_v, hid_v, in_sem.at[0]).wait()

    def owner_at(p, e, core_bit):
        owner = core_bit
        for t, b in enumerate(orders[p]):
            ebit = lax.rem(e // (2 ** (chip_bits - 1 - t)), 2)
            owner = owner + lax.rem(bit_of(b) + 1 + ebit, 2) * (2 ** b)
        return owner

    def term(owner, j):
        return lax.dot_general(
            hid_v[meta_s[owner, 0, j]], cot_v[meta_s[owner, 1, j]],
            (((0,), (0,)), ((), ())), preferred_element_type=F32,
        )

    chips = n // 2
    offsets = [0]
    for t in range(stages):
        offsets.append(offsets[-1] + (n >> (t + 1)))

    def rs_copy(p, t, e):
        where = offsets[t] + e
        bit = 0 if t == 0 else orders[p][t - 1]
        return pltpu.make_async_remote_copy(
            sbuf.at[p, where], rbuf.at[p, where], rs_ss.at[p, where], rs_rs.at[p, where],
            device_id={"fsdp": flip(me, bit)}, device_id_type=MESH,
        )

    def foreign(e, carry):
        for p in range(2):
            owner = owner_at(p, e, 1 - core)
            for j in range(half):
                sbuf[p, e, j] = term(owner, p * half + j).astype(BF16)
            rs_copy(p, 0, e).start()
        return carry

    lax.fori_loop(0, chips, foreign, 0)

    for i in range(chip_bits):
        for p in range(2):
            for e in range(2 ** i):
                ag_copies[p, i, e].wait_recv()
                for i2 in range(i + 1, stages):
                    ag_send(p, i2, e + 2 ** i)

    def own(e, carry):
        for p in range(2):
            owner = owner_at(p, e, core)
            for j in range(half):
                acc[p, e, j] = term(owner, p * half + j)
        return carry

    lax.fori_loop(0, chips, own, 0)

    start = 0
    for t in range(stages):
        m = n >> (t + 1)
        sent = m // 2
        for e in range(m):
            for p in range(2):
                rs_copy(p, t, e).wait_recv()
                total = acc[p, start + e] + rbuf[p, offsets[t] + e].astype(F32)
                if e < sent:
                    sbuf[p, offsets[t + 1] + e] = total.astype(BF16)
                    rs_copy(p, t + 1, e).start()
                elif m > 1:
                    acc[p, start + e] = total
                else:
                    fin[pl.ds(p * half, half)] = total
                    for q in range(half // per):
                        zs[p * (half // per) + q] = total[q * per:(q + 1) * per].astype(BF16)
        start += sent

    def z_peer(r):
        return lax.rem(z + r, dp)

    z_copies = []
    for r in range(1, dp):
        copy = pltpu.make_async_remote_copy(
            zs.at[z_peer(r)], zr.at[r - 1], zs_ss.at[r - 1], zs_rs.at[r - 1],
            device_id={"dp": z_peer(r)}, device_id_type=MESH,
        )
        copy.start()
        z_copies.append(copy)

    for p in range(2):
        for e in range(2 ** chip_bits):
            ag_copies[p, chip_bits, e].wait_recv()
    tiles_back = pltpu.make_async_copy(tiles_v, tiles_out, out_sem.at[1])
    tiles_back.start()

    piece = fin[pl.ds(z * per, per)]
    for r in range(1, dp):
        z_copies[r - 1].wait_recv()
        piece = piece + zr[r - 1].astype(F32)
    slot = z * per + lax.broadcasted_iota(jnp.int32, piece.shape, 0)
    piece = piece * jnp.clip(cnt_s[0] - slot, 0, 1).astype(F32)
    za[z] = piece.astype(BF16)
    sqz[z] = jnp.sum((piece * piece).reshape(-1, 8, 128), axis=0)
    a_copies, q_copies = [], []
    for r in range(1, dp):
        copy = pltpu.make_async_remote_copy(
            sqz.at[z], sqz.at[z], qz_ss.at[r - 1], qz_rs.at[r - 1],
            device_id={"dp": z_peer(r)}, device_id_type=MESH,
        )
        copy.start()
        q_copies.append(copy)
    for r in range(1, dp):
        copy = pltpu.make_async_remote_copy(
            za.at[z], za.at[z], za_ss.at[r - 1], za_rs.at[r - 1],
            device_id={"dp": z_peer(r)}, device_id_type=MESH,
        )
        copy.start()
        a_copies.append(copy)
    for copy in q_copies:
        copy.wait_recv()
    sqf[me] = jnp.sum(sqz[...], axis=0)
    f_copies = []
    for k in range(1, n):
        copy = pltpu.make_async_remote_copy(
            sqf.at[me], sqf.at[me], qf_ss.at[k - 1], qf_rs.at[k - 1],
            device_id={"fsdp": lax.rem(me + k, n)}, device_id_type=MESH,
        )
        copy.start()
        f_copies.append(copy)
    entries = meta_s[0, 2, 0]
    for k in range(1, n):
        entries = entries + meta_s[k, 2, 0]
    for copy in a_copies + f_copies:
        copy.wait_recv()
    squares = jnp.sum(jnp.sum(sqf[...], axis=0), axis=(0, 1), keepdims=True)
    live = jnp.full((1, 1), entries, jnp.int32).astype(F32) * edge * edge
    spread = jnp.sqrt(squares / live)
    factor = jnp.minimum(1.0, 0.5 * root / spread) / root
    for q in range(dp):
        for i in range(per):
            wg_out[q * per + i] = za[q, i].astype(F32) * factor

    for copy in meta_copies + list(ag_copies.values()) + z_copies + q_copies + a_copies + f_copies:
        copy.wait_send()
    for t in range(stages):
        for e in range(n >> (t + 1)):
            for p in range(2):
                rs_copy(p, t, e).wait_send()
    meta_back.wait()
    tiles_back.wait()


def project_kernel(
    n, maxb,
    meta_s, tiles_hbm, hid_hbm, cot_hbm,
    layer_hbm, grad_hbm,
    tiles_v, cot_v, hid_v, gacc, gout, lacc, lout, zero_v, values,
    row_left, row_seen, col_left, col_seen,
    in_sem, hid_sem, g_sem, l_sem,
):
    edge = zero_v.shape[1]
    tile_copy = pltpu.make_async_copy(tiles_hbm, tiles_v, in_sem.at[0])
    cot_copy = pltpu.make_async_copy(cot_hbm, cot_v, in_sem.at[1])
    tile_copy.start()
    cot_copy.start()
    zero_v[...] = jnp.zeros_like(zero_v)

    def clear(left, seen):
        def step(i, carry):
            left[i] = 0
            seen[i] = 0
            return carry
        lax.fori_loop(0, left.shape[0], step, 0)

    clear(row_left, row_seen)
    clear(col_left, col_seen)

    def columns(i):
        return pl.ds(pl.multiple_of(i * edge, edge), edge)

    def each_live(visit):
        def owner(o, carry):
            def slot(j, inner):
                visit(o, j, meta_s[o, 0, j], meta_s[o, 1, j])
                return inner
            return lax.fori_loop(0, meta_s[o, 2, 0], slot, carry)
        lax.fori_loop(0, n, owner, 0)

    def fetch(o, j, row, col):
        pltpu.make_async_copy(hid_hbm.at[:, columns(row)], hid_v.at[o, j], hid_sem).start()
        row_left[row] = row_left[row] + 1
        col_left[col] = col_left[col] + 1

    each_live(fetch)

    def blank(left, target, sem):
        def step(i, carry):
            @pl.when(left[i] == 0)
            def _():
                pltpu.make_async_copy(zero_v, target.at[:, columns(i)], sem).start()
            return carry
        lax.fori_loop(0, left.shape[0], step, 0)

    blank(row_left, grad_hbm, g_sem)
    blank(col_left, layer_hbm, l_sem)
    tile_copy.wait()
    cot_copy.wait()

    def add_block(at, value, left, seen, total, out, target, sem):
        remaining = left[at] - 1
        first = seen[at] == 0
        left[at] = remaining
        seen[at] = 1

        @pl.when(first & (remaining == 0))
        def _():
            out[at] = value[...].astype(BF16)

        @pl.when(first & (remaining > 0))
        def _():
            total[at] = value[...]

        @pl.when(jnp.logical_not(first))
        def _():
            summed = total[at] + value[...]
            total[at] = summed
            out[at] = summed.astype(BF16)

        @pl.when(remaining == 0)
        def _():
            pltpu.make_async_copy(out.at[at], target.at[:, columns(at)], sem).start()

    def backward(o, carry):
        for j in range(maxb):
            values[j] = lax.dot_general(
                cot_v[:, columns(meta_s[o, 1, j])], tiles_v[o, j], (((1,), (1,)), ((), ())),
                preferred_element_type=F32,
            )

        def slot(j, inner):
            add_block(
                meta_s[o, 0, j], values.at[j], row_left, row_seen, gacc, gout, grad_hbm, g_sem
            )
            return inner

        return lax.fori_loop(0, meta_s[o, 2, 0], slot, carry)

    lax.fori_loop(0, n, backward, 0)

    def arrived(o, j, row, col):
        pltpu.make_async_copy(hid_hbm.at[:, columns(row)], hid_v.at[o, j], hid_sem).wait()

    each_live(arrived)

    def forward(o, carry):
        for j in range(maxb):
            values[j] = jnp.dot(hid_v[o, j], tiles_v[o, j], preferred_element_type=F32)

        def slot(j, inner):
            add_block(
                meta_s[o, 1, j], values.at[j], col_left, col_seen, lacc, lout, layer_hbm, l_sem
            )
            return inner

        return lax.fori_loop(0, meta_s[o, 2, 0], slot, carry)

    lax.fori_loop(0, n, forward, 0)
    pltpu.make_async_copy(grad_hbm, grad_hbm, g_sem).wait()
    pltpu.make_async_copy(layer_hbm, layer_hbm, l_sem).wait()


def fused_kernel(
    n, dp, root,
    rows_hbm, cols_hbm, cnt_s, tiles_hbm, hid_hbm, cot_hbm,
    grad_out, layer_out, wg_out, table_s,
    rows_s, cols_s, hid_v, cot_v, tiles_v, meta_v, full_v, full_s, table_v,
    acc, sbuf, rbuf, fin, zs, zr, za, sqf, grad_q, layer_q,
    in_sem, send_sem, meta_rs, ag_rs, pair_rs, rs_rs, z_rs, za_rs, zb_rs, zf_rs, sq_rs,
):
    me = lax.axis_index("fsdp")
    z = lax.axis_index("dp")
    maxb, edge = tiles_hbm.shape[0], tiles_hbm.shape[1]
    slots = n * maxb
    half = maxb // 2
    rows_z = 2 * edge // dp
    stages = n.bit_length() - 1
    chip_bits = stages - 1
    chips = n // 2
    orders = [list(range(1, stages)), list(range(stages - 1, 0, -1))]

    def bit_of(b):
        return lax.rem(me // (2 ** b), 2)

    def relative(x):
        other = me
        for b in range(stages):
            if (x >> b) & 1:
                other = other + (1 - 2 * bit_of(b)) * (2 ** b)
        return other

    def z_peer(r):
        return lax.rem(z + r, dp)

    near = [x for x in range(n) if bin(x >> 1).count("1") < 2]
    far = [x for x in range(n) if x not in near]
    queue = [0, 1] + [x for x in near if x > 1 and x % 2 == 0]
    queue += [x for x in near if x > 1 and x % 2 == 1] + far
    place = [queue.index(x) for x in range(n)]

    def fetch(source, target, sem, first, last):
        def step(i, carry):
            at = pl.ds(pl.multiple_of(i * edge, edge), edge)
            pltpu.make_async_copy(source.at[:, at], target.at[i], sem).start()
            return carry
        lax.fori_loop(first, last, step, 0)

    def blocks_wait(count, sem):
        if count <= maxb:
            blocks = tiles_v.at[0, pl.ds(0, count)]
        else:
            blocks = tiles_v.at[pl.ds(0, count // maxb)]
        pltpu.make_async_copy(blocks, blocks, sem).wait()

    barrier = pltpu.get_barrier_semaphore()
    for r in range(1, dp):
        pl.semaphore_signal(
            barrier, inc=1, device_id={"dp": z_peer(r)}, device_id_type=MESH
        )
    for x in range(n - 1, 0, -1):
        pl.semaphore_signal(
            barrier, inc=1, device_id={"fsdp": relative(x)}, device_id_type=MESH
        )
    rows_copy = pltpu.make_async_copy(rows_hbm, rows_s, in_sem.at[2])
    rows_copy.start()
    cols_copy = pltpu.make_async_copy(cols_hbm, cols_s, in_sem.at[3])
    cols_copy.start()
    own_copy = pltpu.make_async_copy(tiles_hbm, tiles_v.at[0], in_sem.at[7])
    own_copy.start()

    early = hid_v.shape[0] * 3 // 8
    fetch(cot_hbm, cot_v, in_sem.at[1], 0, cot_v.shape[0])
    fetch(hid_hbm, hid_v, in_sem.at[0], 0, early)

    lane = lax.broadcasted_iota(jnp.int32, (8, 128), 1)
    sub = lax.broadcasted_iota(jnp.int32, (8, 128), 0)
    meta = jnp.where(sub == 2, cnt_s[0], 0)
    rows_copy.wait()
    cols_copy.wait()
    for j in range(maxb):
        here = lax.rem(lane, maxb) == j
        meta = jnp.where((sub == 0) & here, rows_s[j], meta)
        meta = jnp.where((sub == 1) & here, cols_s[j], meta)
    meta_v[0] = meta
    pl.semaphore_wait(barrier, n - 1 + dp - 1)

    for x in range(n - 1, 0, -1):
        pltpu.make_async_remote_copy(
            meta_v.at[0], meta_v.at[place[x]], send_sem.at[0], meta_rs.at[int(x in far)],
            device_id={"fsdp": relative(x)}, device_id_type=MESH,
        ).start()
    own_copy.wait()

    ag_done = set()

    def ag_index(i, e, h):
        split = 0 < i < chip_bits and e == 0
        keys = [(i, e, h) for i in range(stages) for e in range(2 ** i) for h in range(2)
                if h == 0 or (0 < i < chip_bits and e == 0)]
        return keys.index((i, e, h if split else 0)), maxb // 2 if split else maxb

    def ag_send(p, i, e, h):
        bits = orders[p] + [0]
        owner = 0
        for t in range(len(bits)):
            if (e >> t) & 1:
                owner |= 1 << bits[t]
        part = pl.ds(p * half + h * (half // 2), half // 2)
        pltpu.make_async_remote_copy(
            tiles_v.at[place[owner], part], tiles_v.at[place[owner | (1 << bits[i])], part],
            send_sem.at[1], ag_rs.at[ag_index(i, e, h)[0]],
            device_id={"fsdp": relative(1 << bits[i])}, device_id_type=MESH,
        ).start()

    def ag_wait(i, e, h):
        index, count = ag_index(i, e, h)
        if index not in ag_done:
            ag_done.add(index)
            blocks_wait(count, ag_rs.at[index])

    for i in range(stages):
        for p in range(2):
            for h in range(2):
                if h == 0 or i == 0 or i == chip_bits:
                    ag_send(p, i, 0, h)

    grad_q[slots] = jnp.zeros(grad_q.shape[1:], F32)
    layer_q[slots] = jnp.zeros(layer_q.shape[1:], F32)
    grad_out[slots] = jnp.zeros(grad_out.shape[1:], BF16)
    layer_out[slots] = jnp.zeros(layer_out.shape[1:], BF16)

    fetch(hid_hbm, hid_v, in_sem.at[0], early, hid_v.shape[0])

    def collect(xs, full):
        arrive = [x for x in xs if x]
        first = min(place[x] for x in arrive)
        metas = meta_v.at[pl.ds(first, len(arrive))]
        pltpu.make_async_copy(metas, metas, meta_rs.at[int(xs is far)]).wait()
        for x in xs:
            full = jnp.where(lane // maxb == place[x], meta_v[place[x]], full)
        return full

    def to_smem(k):
        return pltpu.make_async_copy(full_v.at[k], full_s.at[k], in_sem.at[4 + k])

    known = collect(near, jnp.zeros((8, 128), jnp.int32))
    full_v[0] = known
    to_smem(0).start()

    def term(x, j, named=None):
        q = place[x] * maxb + j
        k = 0 if x in near else 1
        row = full_s[k, 0, q] if named is None else named[0, q]
        col = full_s[k, 1, q] if named is None else named[1, q]
        return lax.dot_general(
            hid_v[row], cot_v[col],
            (((0,), (0,)), ((), ())), preferred_element_type=F32,
        )

    def owner_at(p, e):
        owner = 0
        for t, b in enumerate(orders[p]):
            if not (e >> (chip_bits - 1 - t)) & 1:
                owner |= 1 << b
        return owner

    offsets = [0]
    for t in range(stages):
        offsets.append(offsets[-1] + (n >> (t + 1)))

    def pair_copy(p, e):
        return pltpu.make_async_remote_copy(
            sbuf.at[p, e], rbuf.at[p, e], send_sem.at[2], pair_rs.at[e],
            device_id={"fsdp": relative(1)}, device_id_type=MESH,
        )

    def rs_copy(p, t, e, c):
        where = offsets[t] + e
        return pltpu.make_async_remote_copy(
            sbuf.at[p, where, c], rbuf.at[p, where, c],
            send_sem.at[2], rs_rs.at[t - 1, c],
            device_id={"fsdp": relative(1 << orders[p][t - 1])}, device_id_type=MESH,
        )

    def foreign(e, named=None):
        for p in range(2):
            for c in range(half):
                sbuf[p, e, c] = term(owner_at(p, e) | 1, p * half + c, named).astype(BF16)
        for p in range(2):
            pair_copy(p, e).start()

    def own(e):
        for p in range(2):
            for c in range(half):
                acc[p, e, c] = term(owner_at(p, e), p * half + c)

    starts = [0]
    for t in range(stages):
        starts.append(starts[-1] + (n >> (t + 1)) // 2)

    paired = set()

    def pair_wait(e):
        if e not in paired:
            paired.add(e)
            blocks_wait(maxb, pair_rs.at[e])

    def pass_on(e, cs):
        for p in range(2):
            pair_wait(e)
            for c in cs:
                total = acc[p, e, c] + rbuf[p, e, c].astype(F32)
                sbuf[p, offsets[1] + e, c] = total.astype(BF16)
            for c in cs:
                rs_copy(p, 1, e, c).start()

    def reduce_step(t, c):
        m = n >> (t + 1)
        blocks_wait(2 * m, rs_rs.at[t - 1, c])
        for e in range(m):
            for p in range(2):
                at_e = starts[t] + e
                total = acc[p, at_e, c] + rbuf[p, offsets[t] + e, c].astype(F32)
                if t == 1:
                    total = total + rbuf[p, at_e, c].astype(F32)
                if e < m // 2:
                    sbuf[p, offsets[t + 1] + e, c] = total.astype(BF16)
                    rs_copy(p, t + 1, e, c).start()
                elif m > 1:
                    acc[p, at_e, c] = total
                else:
                    at = pl.ds(p * edge, edge)
                    fin[c, at] = total
                    zs[c, at] = total.astype(BF16)
        if m == 1:
            for r in range(1, dp):
                z_copy(c, r).start()

    def z_rows(index):
        return pl.ds(pl.multiple_of(index * rows_z, rows_z), rows_z)

    def z_copy(c, r):
        return pltpu.make_async_remote_copy(
            zs.at[c, z_rows(z_peer(r))], zr.at[c, r - 1], send_sem.at[3], z_rs.at[c],
            device_id={"dp": z_peer(r)}, device_id_type=MESH,
        )

    def a_copy(c, piece, peer, sem):
        return pltpu.make_async_remote_copy(
            za.at[c, z_rows(piece)], za.at[c, z_rows(piece)], send_sem.at[4], sem,
            device_id={"dp": peer}, device_id_type=MESH,
        )

    handed = half // 2 if dp == 4 else 0
    z_near = z + 1 - 2 * lax.rem(z, 2)
    z_far = z + 2 - 4 * lax.rem(z // 2, 2)

    def z_sum(c, squares):
        piece = fin[c, z_rows(z)]
        pltpu.make_async_copy(zr.at[c], zr.at[c], z_rs.at[c]).wait()
        for r in range(1, dp):
            piece = piece + zr[c, r - 1].astype(F32)
        row = z * rows_z + lax.broadcasted_iota(jnp.int32, piece.shape, 0)
        slot = (row // edge) * half + c
        piece = piece * jnp.clip(cnt_s[0] - slot, 0, 1).astype(F32)
        za[c, z_rows(z)] = piece.astype(BF16)
        return squares + jnp.sum((piece * piece).reshape(-1, 8, 128), axis=0)

    def a_send(c):
        for r in range(1, dp):
            a_copy(c, z, z_peer(r), za_rs).start()

    def a_cross(c):
        a_copy(c, z, z_far, zf_rs.at[c]).start()
        a_copy(c, z, z_near, zb_rs).start()

    def a_hand(c):
        a_copy(c, z, z_far, zf_rs.at[c]).wait_recv()
        a_copy(c, z_far, z_near, zb_rs).start()

    def z_cross(c, squares):
        squares = z_sum(c, squares)
        a_cross(c)
        return squares

    def z_step(c, squares):
        squares = z_sum(c, squares)
        a_send(c)
        return squares

    def project(at):
        def load(j):
            q = at * maxb + j
            backward = lax.dot_general(
                cot_v[full_s[1, 1, q]], tiles_v[at, j], (((1,), (1,)), ((), ())),
                preferred_element_type=F32,
            )
            forward = jnp.dot(hid_v[full_s[1, 0, q]], tiles_v[at, j], preferred_element_type=F32)
            return q, backward, forward
        for j in range(maxb):
            q, backward, forward = load(j)
            backward = backward + grad_q[table_s[0, q]]
            grad_q[q] = backward
            grad_out[q] = backward.astype(BF16)
            forward = forward + layer_q[table_s[1, q]]
            layer_q[q] = forward
            layer_out[q] = forward.astype(BF16)

    def arrived(x):
        for p in range(2):
            bits = orders[p] + [0]
            index = [t for t in range(stages) if (x >> bits[t]) & 1]
            if index:
                e = sum(1 << t for t in index[:-1])
                for h in range(2):
                    ag_wait(index[-1], e, h)

    sent = sorted(range(chips // 2), key=lambda e: bin(owner_at(0, e)).count("1"))
    kept = list(range(chips // 2, chips))
    pltpu.make_async_copy(cot_v, cot_v, in_sem.at[1]).wait()
    pltpu.make_async_copy(hid_v, hid_v, in_sem.at[0]).wait()
    foreign(sent[0], known)
    to_smem(0).wait()
    full = collect(far, known)
    full_v[1] = full
    to_smem(1).start()
    own(sent[0])
    to_smem(1).wait()
    for k in range(1, len(sent)):
        foreign(sent[k])
        pass_on(sent[k - 1], [0])
        own(sent[k])
    foreign(kept[0])
    pass_on(sent[-1], [0])
    for c in range(1, half - 1):
        for e in sent:
            pass_on(e, [c])
    for e in kept[1:]:
        foreign(e)

    wide = lax.broadcasted_iota(jnp.int32, (slots, 128), 1)
    tall = lax.broadcasted_iota(jnp.int32, (slots, 128), 0)
    alive = lax.rem(lane[0:1], maxb) < full[2:3]
    table = jnp.full((8, 128), slots, jnp.int32)
    for k in range(2):
        named = jnp.broadcast_to(jnp.where(alive, full[k:k + 1], -1), (slots, 128))
        named_t = jnp.sum(jnp.where(wide == tall, named, 0), axis=1, keepdims=True)
        before = jnp.max(
            jnp.where((named_t == named) & (tall < wide), tall, -1), axis=0, keepdims=True
        )
        last = jnp.max(jnp.where(named_t == wide, tall, -1), axis=0, keepdims=True)
        table = jnp.where(sub == k, jnp.where(before < 0, slots, before), table)
        table = jnp.where(sub == 2 + k, jnp.where(last < 0, slots, last), table)
    table_v[...] = table
    table_copy = pltpu.make_async_copy(table_v, table_s, in_sem.at[6])
    table_copy.start()
    for e in kept:
        own(e)
    table_copy.wait()

    def project_all(xs):
        for x in xs:
            arrived(x)
        first = place[xs[0]]

        def one(at, carry):
            project(at)
            return carry

        lax.fori_loop(first, first + len(xs), one, 0)

    def ag_pass(i, e, h):
        ag_wait(i, e, h)
        for p in range(2):
            ag_send(p, chip_bits, e + 2 ** i, h)

    project_all([0, 1])
    for h in range(2):
        for i in range(chip_bits if h == 0 else 1):
            ag_pass(i, 0, h)
    for e in kept:
        pair_wait(e)
    reduce_step(1, 0)
    for e in sent:
        pass_on(e, [half - 1])

    def second(c, carry):
        reduce_step(1, c)
        return carry

    lax.fori_loop(1, half - 1, second, 0)
    for t in range(2, stages):
        reduce_step(t, 0)
    reduce_step(1, half - 1)
    for t in range(2, stages):
        def third(c, carry):
            reduce_step(t, c)
            return carry

        lax.fori_loop(1, half, third, 0)

    for i in range(1, chip_bits):
        for p in range(2):
            ag_send(p, i, 0, 1)
    for i in range(1, chip_bits):
        for e in range(1, 2 ** i):
            for p in range(2):
                for h in range(2):
                    ag_wait(i - 1, e - 2 ** (i - 1), h)
                    ag_send(p, i, e, h)

    squares = lax.fori_loop(0, handed, z_cross, jnp.zeros((8, 128), F32))
    squares = lax.fori_loop(handed, half // 2, z_step, squares)
    for i in range(1, chip_bits):
        ag_pass(i, 0, 1)
    project_all([x for x in near if x > 1 and x % 2 == 0])
    squares = lax.fori_loop(half // 2, half - 1, z_step, squares)
    squares = z_sum(half - 1, squares)
    device = me * dp + z
    sqf[device] = jnp.sum(squares, axis=0, keepdims=True)
    for x in reversed(queue):
        for r in range(dp):
            if x or r:
                pltpu.make_async_remote_copy(
                    sqf.at[device], sqf.at[device], send_sem.at[5], sq_rs,
                    device_id={"fsdp": relative(x), "dp": z_peer(r)}, device_id_type=MESH,
                ).start()
    a_send(half - 1)
    for i in range(1, chip_bits):
        for e in range(1, 2 ** i):
            for h in range(2):
                ag_pass(i, e, h)
    crossed = [x for x in near if x > 1 and x % 2 == 1]
    for c in range(handed):
        a_hand(c)
    project_all(crossed)
    project_all(far)

    entries = full_s[1, 2, 0]
    for x in range(1, n):
        entries = entries + full_s[1, 2, x * maxb]
    others = sqf.at[pl.ds(0, n * dp - 1)]
    pltpu.make_async_copy(others, others, sq_rs).wait()
    squares = jnp.sum(jnp.sum(sqf[...], axis=0), axis=1, keepdims=True)
    live = jnp.full((1, 1), entries, jnp.int32).astype(F32) * edge * edge
    spread = jnp.sqrt(squares / live)
    factor = jnp.minimum(1.0, 0.5 * root / spread) / root

    if handed:
        twice = za.at[pl.ds(0, handed)]
        pltpu.make_async_copy(twice.at[:, pl.ds(0, 2 * rows_z)], twice.at[:, pl.ds(0, 2 * rows_z)], zb_rs).wait()
    direct = zr.at[pl.ds(handed, half - handed)]
    pltpu.make_async_copy(direct, direct, za_rs).wait()

    def finish(c, carry):
        for p in range(2):
            wg_out[p * half + c] = za[c, pl.ds(p * edge, edge)].astype(F32) * factor
        return carry

    lax.fori_loop(0, half, finish, 0)

    metas = meta_v.at[pl.ds(1, n - 1)]
    gathered = tiles_v.at[pl.ds(1, n - 1)]
    for k, sent in enumerate((metas, gathered, sbuf, zr, zr, others)):
        pltpu.make_async_copy(sent, sent, send_sem.at[k]).wait()


def write_kernel(
    grad_v, layer_v, wg_v, table_s,
    layer_hbm, grad_hbm, wg_hbm,
    w_sem, g_sem, l_sem,
):
    edge = grad_v.shape[2]

    def write(row, source, target, sem):
        def step(i, carry):
            at = pl.ds(pl.multiple_of(i * edge, edge), edge)
            pltpu.make_async_copy(source.at[table_s[row, i]], target.at[:, at], sem).start()
            return carry
        lax.fori_loop(0, target.shape[1] // edge, step, 0)

    write(2, grad_v, grad_hbm, g_sem)
    write(3, layer_v, layer_hbm, l_sem)
    wg_copy = pltpu.make_async_copy(wg_v, wg_hbm, w_sem)
    wg_copy.start()
    pltpu.make_async_copy(grad_hbm, grad_hbm, g_sem).wait()
    pltpu.make_async_copy(layer_hbm, layer_hbm, l_sem).wait()
    wg_copy.wait()


def fused(n, dp, hidden, cotangent, tiles, tile_rows, tile_cols, counts):
    tokens, width_ff = hidden.shape
    maxb, edge, _ = tiles.shape
    root = math.sqrt(tokens * n * dp)
    slots, half, stages = n * maxb, maxb // 2, n.bit_length() - 1
    in_hbm = functools.partial(pltpu.with_memory_space_constraint, memory_space=pltpu.HBM)
    rows_z = 2 * edge // dp
    hbm = pl.BlockSpec(memory_space=pltpu.HBM)
    smem = pl.BlockSpec(memory_space=pltpu.SMEM)
    vmem = pl.BlockSpec(memory_space=pltpu.VMEM)
    dma = pltpu.SemaphoreType.DMA
    grad, layer, weight, table = pl.pallas_call(
        functools.partial(fused_kernel, n, dp, root),
        out_shape=(
            pltpu.VMEM((slots + 1, tokens, edge), BF16),
            pltpu.VMEM((slots + 1, tokens, edge), BF16),
            pltpu.VMEM((maxb, edge, edge), F32),
            pltpu.SMEM((8, 128), jnp.int32),
        ),
        in_specs=[hbm, hbm, smem, hbm, hbm, hbm],
        out_specs=(vmem, vmem, vmem, smem),
        scratch_shapes=[
            pltpu.SMEM(tile_rows.shape, jnp.int32),
            pltpu.SMEM(tile_cols.shape, jnp.int32),
            pltpu.VMEM((hidden.shape[1] // edge, tokens, edge), BF16),
            pltpu.VMEM((cotangent.shape[1] // edge, tokens, edge), BF16),
            pltpu.VMEM((n, maxb, edge, edge), BF16),
            pltpu.VMEM((n, 8, 128), jnp.int32),
            pltpu.VMEM((2, 8, 128), jnp.int32),
            pltpu.SMEM((2, 8, 128), jnp.int32),
            pltpu.VMEM((8, 128), jnp.int32),
            pltpu.VMEM((2, n // 2, half, edge, edge), F32),
            pltpu.VMEM((2, n - 1, half, edge, edge), BF16),
            pltpu.VMEM((2, n - 1, half, edge, edge), BF16),
            pltpu.VMEM((half, 2 * edge, edge), F32),
            pltpu.VMEM((half, 2 * edge, edge), BF16),
            pltpu.VMEM((half, dp - 1, rows_z, edge), BF16),
            pltpu.VMEM((half, 2 * edge, edge), BF16),
            pltpu.VMEM((n * dp, 1, 128), F32),
            pltpu.VMEM((slots + 1, tokens, edge), F32),
            pltpu.VMEM((slots + 1, tokens, edge), F32),
            dma((8,)), dma((6,)), dma((2,)),
            dma((n - 1 + max(stages - 2, 0),)),
            dma((n // 2,)), dma((stages - 1, half)), dma((half,)), dma, dma, dma((half,)), dma,
        ],
        compiler_params=pltpu.CompilerParams(
            collective_id=0, has_side_effects=True, vmem_limit_bytes=44 * 2 ** 20
        ),
        name="fused",
    )(in_hbm(tile_rows), in_hbm(tile_cols), counts, in_hbm(tiles), in_hbm(hidden), in_hbm(cotangent))
    return pl.pallas_call(
        write_kernel,
        out_shape=(
            jax.ShapeDtypeStruct(cotangent.shape, BF16),
            jax.ShapeDtypeStruct(hidden.shape, BF16),
            jax.ShapeDtypeStruct(tiles.shape, F32),
        ),
        in_specs=[vmem, vmem, vmem, smem],
        out_specs=(hbm, hbm, hbm),
        scratch_shapes=[dma, dma, dma],
        compiler_params=pltpu.CompilerParams(vmem_limit_bytes=16 * 2 ** 20),
        name="write",
    )(grad, layer, weight, table)


def shards(n, dp, hidden, cotangent, tiles, tile_rows, tile_cols, counts):
    tokens, width_ff = hidden.shape
    width_model = cotangent.shape[1]
    maxb, edge, _ = tiles.shape
    blocks_ff, blocks_model = width_ff // edge, width_model // edge
    root = math.sqrt(tokens * n * dp)
    half, per = maxb // 2, maxb // dp
    sums = n * maxb * tokens * edge * 12
    if n == 8 and dp % 2 == 0 and max(n * maxb, blocks_ff, blocks_model) <= 128 and sums <= 28 * 2 ** 20:
        return fused(n, dp, hidden, cotangent, tiles, tile_rows, tile_cols, counts)
    hbm = pl.BlockSpec(memory_space=pl.ANY)
    smem = pl.BlockSpec(memory_space=pltpu.SMEM)
    vmem = pl.BlockSpec(memory_space=pltpu.VMEM)
    dma = pltpu.SemaphoreType.DMA
    meta, gathered, weight_grad = pl.pallas_call(
        functools.partial(exchange_kernel, n, dp, root),
        out_shape=(
            jax.ShapeDtypeStruct((n, 8, 128), jnp.int32),
            jax.ShapeDtypeStruct((n, maxb, edge, edge), BF16),
            jax.ShapeDtypeStruct((maxb, edge, edge), F32),
        ),
        in_specs=[smem, smem, smem, hbm, hbm, hbm],
        out_specs=(hbm, hbm, vmem),
        scratch_shapes=[
            pltpu.VMEM((blocks_ff, tokens, edge), BF16),
            pltpu.VMEM((blocks_model, tokens, edge), BF16),
            pltpu.VMEM((n, maxb, edge, edge), BF16),
            pltpu.VMEM((n, 8, 128), jnp.int32),
            pltpu.SMEM((n, 8, 128), jnp.int32),
            pltpu.VMEM((2, n // 2, half, edge, edge), F32),
            pltpu.VMEM((2, n - 1, half, edge, edge), BF16),
            pltpu.VMEM((2, n - 1, half, edge, edge), BF16),
            pltpu.VMEM((maxb, edge, edge), F32),
            pltpu.VMEM((dp, per, edge, edge), BF16),
            pltpu.VMEM((dp - 1, per, edge, edge), BF16),
            pltpu.VMEM((dp, per, edge, edge), BF16),
            pltpu.VMEM((dp, 8, 128), F32),
            pltpu.VMEM((n, 8, 128), F32),
            dma((4,)), dma((2,)),
            dma((n - 1,)), dma((n - 1,)),
            dma((2, n - 1)), dma((2, n - 1)),
            dma((2, n - 1)), dma((2, n - 1)),
            dma((dp - 1,)), dma((dp - 1,)),
            dma((dp - 1,)), dma((dp - 1,)),
            dma((dp - 1,)), dma((dp - 1,)),
            dma((n - 1,)), dma((n - 1,)),
        ],
        compiler_params=pltpu.CompilerParams(
            collective_id=0, has_side_effects=True, vmem_limit_bytes=60 * 2 ** 20
        ),
        name="exchange",
    )(tile_rows, tile_cols, counts, tiles, hidden, cotangent)

    layer_out, hidden_grad = pl.pallas_call(
        functools.partial(project_kernel, n, maxb),
        out_shape=(
            jax.ShapeDtypeStruct(cotangent.shape, BF16),
            jax.ShapeDtypeStruct(hidden.shape, BF16),
        ),
        in_specs=[smem, hbm, hbm, hbm],
        out_specs=(hbm, hbm),
        scratch_shapes=[
            pltpu.VMEM((n, maxb, edge, edge), BF16),
            pltpu.VMEM(cotangent.shape, BF16),
            pltpu.VMEM((n, maxb, tokens, edge), BF16),
            pltpu.VMEM((blocks_ff, tokens, edge), F32),
            pltpu.VMEM((blocks_ff, tokens, edge), BF16),
            pltpu.VMEM((blocks_model, tokens, edge), F32),
            pltpu.VMEM((blocks_model, tokens, edge), BF16),
            pltpu.VMEM((tokens, edge), BF16),
            pltpu.VMEM((maxb, tokens, edge), F32),
            pltpu.SMEM((blocks_ff,), jnp.int32),
            pltpu.SMEM((blocks_ff,), jnp.int32),
            pltpu.SMEM((blocks_model,), jnp.int32),
            pltpu.SMEM((blocks_model,), jnp.int32),
            dma((2,)), dma, dma, dma,
        ],
        compiler_params=pltpu.CompilerParams(vmem_limit_bytes=62 * 2 ** 20),
        name="project",
    )(meta, gathered, hidden, cotangent)
    return layer_out, hidden_grad, weight_grad


def solution(mesh):
    placed = (
        P(("fsdp", "dp"), None),
        P(("fsdp", "dp"), None),
        P("fsdp", None, None),
        P("fsdp"),
        P("fsdp"),
        P("fsdp"),
    )
    return jax.shard_map(
        functools.partial(shards, mesh.shape["fsdp"], mesh.shape["dp"]),
        mesh=mesh,
        in_specs=placed,
        out_specs=(P(("fsdp", "dp"), None), P(("fsdp", "dp"), None), P("fsdp", None, None)),
        check_vma=False,
    )
```

```python
import functools
import math

import jax
import jax.numpy as jnp
from jax import lax
from jax.experimental import pallas as pl
from jax.experimental.pallas import tpu as pltpu
from jax.sharding import PartitionSpec as P

MESH = pl.DeviceIdType.MESH
F32 = jnp.float32
BF16 = jnp.bfloat16


def exchange_kernel(
    n, dp, root,
    rows_s, cols_s, cnt_s, tiles_hbm, hid_hbm, cot_hbm,
    meta_out, tiles_out, wg_out,
    hid_v, cot_v, tiles_v, meta_v, meta_s, acc, sbuf, rbuf, fin, zs, zr, za, sqz, sqf,
    in_sem, out_sem, meta_ss, meta_rs, ag_ss, ag_rs, rs_ss, rs_rs,
    zs_ss, zs_rs, za_ss, za_rs, qz_ss, qz_rs, qf_ss, qf_rs,
):
    me = lax.axis_index("fsdp")
    z = lax.axis_index("dp")
    maxb, edge = tiles_hbm.shape[0], tiles_hbm.shape[1]
    half = maxb // 2
    per = maxb // dp
    stages = n.bit_length() - 1
    chip_bits = stages - 1
    orders = [list(range(1, stages)), list(range(stages - 1, 0, -1))]
    core = lax.rem(me, 2)

    def bit_of(b):
        return lax.rem(me // (2 ** b), 2)

    def flip(value_me, b):
        return value_me + (1 - 2 * bit_of(b)) * (2 ** b)

    def fetch(source, target, sem):
        def step(i, carry):
            at = pl.ds(pl.multiple_of(i * edge, edge), edge)
            pltpu.make_async_copy(source.at[:, at], target.at[i], sem).start()
            return carry
        lax.fori_loop(0, target.shape[0], step, 0)

    own_copy = pltpu.make_async_copy(tiles_hbm, tiles_v.at[me], in_sem.at[2])
    own_copy.start()
    fetch(cot_hbm, cot_v, in_sem.at[1])
    fetch(hid_hbm, hid_v, in_sem.at[0])

    barrier = pltpu.get_barrier_semaphore()
    for k in range(1, n):
        pl.semaphore_signal(
            barrier, inc=1, device_id={"fsdp": lax.rem(me + k, n)}, device_id_type=MESH
        )
    for k in range(1, dp):
        pl.semaphore_signal(
            barrier, inc=1, device_id={"dp": lax.rem(z + k, dp)}, device_id_type=MESH
        )
    lane = lax.broadcasted_iota(jnp.int32, (8, 128), 1)
    sub = lax.broadcasted_iota(jnp.int32, (8, 128), 0)
    meta = jnp.where(sub == 2, cnt_s[0], 0)
    for j in range(maxb):
        meta = jnp.where((sub == 0) & (lane == j), rows_s[j], meta)
        meta = jnp.where((sub == 1) & (lane == j), cols_s[j], meta)
    meta_v[me] = meta
    own_copy.wait()
    pl.semaphore_wait(barrier, n - 1 + dp - 1)

    meta_copies = []
    for k in range(1, n):
        copy = pltpu.make_async_remote_copy(
            meta_v.at[me], meta_v.at[me], meta_ss.at[k - 1], meta_rs.at[k - 1],
            device_id={"fsdp": lax.rem(me + k, n)}, device_id_type=MESH,
        )
        copy.start()
        meta_copies.append(copy)

    ag_copies = {}

    def ag_send(p, i, e):
        bits = orders[p] + [0]
        owner = me
        for t in range(len(bits)):
            if (e >> t) & 1:
                owner = flip(owner, bits[t])
        piece = tiles_v.at[owner, pl.ds(p * half, half)]
        where = 2 ** i - 1 + e
        copy = pltpu.make_async_remote_copy(
            piece, piece, ag_ss.at[p, where], ag_rs.at[p, where],
            device_id={"fsdp": flip(me, bits[i])}, device_id_type=MESH,
        )
        copy.start()
        ag_copies[p, i, e] = copy

    for i in range(stages):
        for p in range(2):
            ag_send(p, i, 0)

    for copy in meta_copies:
        copy.wait_recv()
    to_smem = pltpu.make_async_copy(meta_v, meta_s, in_sem.at[3])
    to_smem.start()
    to_smem.wait()
    meta_back = pltpu.make_async_copy(meta_v, meta_out, out_sem.at[0])
    meta_back.start()
    pltpu.make_async_copy(cot_v, cot_v, in_sem.at[1]).wait()
    pltpu.make_async_copy(hid_v, hid_v, in_sem.at[0]).wait()

    def owner_at(p, e, core_bit):
        owner = core_bit
        for t, b in enumerate(orders[p]):
            ebit = lax.rem(e // (2 ** (chip_bits - 1 - t)), 2)
            owner = owner + lax.rem(bit_of(b) + 1 + ebit, 2) * (2 ** b)
        return owner

    def term(owner, j):
        return lax.dot_general(
            hid_v[meta_s[owner, 0, j]], cot_v[meta_s[owner, 1, j]],
            (((0,), (0,)), ((), ())), preferred_element_type=F32,
        )

    chips = n // 2
    offsets = [0]
    for t in range(stages):
        offsets.append(offsets[-1] + (n >> (t + 1)))

    def rs_copy(p, t, e):
        where = offsets[t] + e
        bit = 0 if t == 0 else orders[p][t - 1]
        return pltpu.make_async_remote_copy(
            sbuf.at[p, where], rbuf.at[p, where], rs_ss.at[p, where], rs_rs.at[p, where],
            device_id={"fsdp": flip(me, bit)}, device_id_type=MESH,
        )

    def foreign(e, carry):
        for p in range(2):
            owner = owner_at(p, e, 1 - core)
            for j in range(half):
                sbuf[p, e, j] = term(owner, p * half + j).astype(BF16)
            rs_copy(p, 0, e).start()
        return carry

    lax.fori_loop(0, chips, foreign, 0)

    for i in range(chip_bits):
        for p in range(2):
            for e in range(2 ** i):
                ag_copies[p, i, e].wait_recv()
                for i2 in range(i + 1, stages):
                    ag_send(p, i2, e + 2 ** i)

    def own(e, carry):
        for p in range(2):
            owner = owner_at(p, e, core)
            for j in range(half):
                acc[p, e, j] = term(owner, p * half + j)
        return carry

    lax.fori_loop(0, chips, own, 0)

    start = 0
    for t in range(stages):
        m = n >> (t + 1)
        sent = m // 2
        for e in range(m):
            for p in range(2):
                rs_copy(p, t, e).wait_recv()
                total = acc[p, start + e] + rbuf[p, offsets[t] + e].astype(F32)
                if e < sent:
                    sbuf[p, offsets[t + 1] + e] = total.astype(BF16)
                    rs_copy(p, t + 1, e).start()
                elif m > 1:
                    acc[p, start + e] = total
                else:
                    fin[pl.ds(p * half, half)] = total
                    for q in range(half // per):
                        zs[p * (half // per) + q] = total[q * per:(q + 1) * per].astype(BF16)
        start += sent

    def z_peer(r):
        return lax.rem(z + r, dp)

    z_copies = []
    for r in range(1, dp):
        copy = pltpu.make_async_remote_copy(
            zs.at[z_peer(r)], zr.at[r - 1], zs_ss.at[r - 1], zs_rs.at[r - 1],
            device_id={"dp": z_peer(r)}, device_id_type=MESH,
        )
        copy.start()
        z_copies.append(copy)

    for p in range(2):
        for e in range(2 ** chip_bits):
            ag_copies[p, chip_bits, e].wait_recv()
    tiles_back = pltpu.make_async_copy(tiles_v, tiles_out, out_sem.at[1])
    tiles_back.start()

    piece = fin[pl.ds(z * per, per)]
    for r in range(1, dp):
        z_copies[r - 1].wait_recv()
        piece = piece + zr[r - 1].astype(F32)
    slot = z * per + lax.broadcasted_iota(jnp.int32, piece.shape, 0)
    piece = piece * jnp.clip(cnt_s[0] - slot, 0, 1).astype(F32)
    za[z] = piece.astype(BF16)
    sqz[z] = jnp.sum((piece * piece).reshape(-1, 8, 128), axis=0)
    a_copies, q_copies = [], []
    for r in range(1, dp):
        copy = pltpu.make_async_remote_copy(
            sqz.at[z], sqz.at[z], qz_ss.at[r - 1], qz_rs.at[r - 1],
            device_id={"dp": z_peer(r)}, device_id_type=MESH,
        )
        copy.start()
        q_copies.append(copy)
    for r in range(1, dp):
        copy = pltpu.make_async_remote_copy(
            za.at[z], za.at[z], za_ss.at[r - 1], za_rs.at[r - 1],
            device_id={"dp": z_peer(r)}, device_id_type=MESH,
        )
        copy.start()
        a_copies.append(copy)
    for copy in q_copies:
        copy.wait_recv()
    sqf[me] = jnp.sum(sqz[...], axis=0)
    f_copies = []
    for k in range(1, n):
        copy = pltpu.make_async_remote_copy(
            sqf.at[me], sqf.at[me], qf_ss.at[k - 1], qf_rs.at[k - 1],
            device_id={"fsdp": lax.rem(me + k, n)}, device_id_type=MESH,
        )
        copy.start()
        f_copies.append(copy)
    entries = meta_s[0, 2, 0]
    for k in range(1, n):
        entries = entries + meta_s[k, 2, 0]
    for copy in a_copies + f_copies:
        copy.wait_recv()
    squares = jnp.sum(jnp.sum(sqf[...], axis=0), axis=(0, 1), keepdims=True)
    live = jnp.full((1, 1), entries, jnp.int32).astype(F32) * edge * edge
    spread = jnp.sqrt(squares / live)
    factor = jnp.minimum(1.0, 0.5 * root / spread) / root
    for q in range(dp):
        for i in range(per):
            wg_out[q * per + i] = za[q, i].astype(F32) * factor

    for copy in meta_copies + list(ag_copies.values()) + z_copies + q_copies + a_copies + f_copies:
        copy.wait_send()
    for t in range(stages):
        for e in range(n >> (t + 1)):
            for p in range(2):
                rs_copy(p, t, e).wait_send()
    meta_back.wait()
    tiles_back.wait()


def project_kernel(
    n, maxb,
    meta_s, tiles_hbm, hid_hbm, cot_hbm,
    layer_hbm, grad_hbm,
    tiles_v, cot_v, hid_v, gacc, gout, lacc, lout, zero_v, values,
    row_left, row_seen, col_left, col_seen,
    in_sem, hid_sem, g_sem, l_sem,
):
    edge = zero_v.shape[1]
    tile_copy = pltpu.make_async_copy(tiles_hbm, tiles_v, in_sem.at[0])
    cot_copy = pltpu.make_async_copy(cot_hbm, cot_v, in_sem.at[1])
    tile_copy.start()
    cot_copy.start()
    zero_v[...] = jnp.zeros_like(zero_v)

    def clear(left, seen):
        def step(i, carry):
            left[i] = 0
            seen[i] = 0
            return carry
        lax.fori_loop(0, left.shape[0], step, 0)

    clear(row_left, row_seen)
    clear(col_left, col_seen)

    def columns(i):
        return pl.ds(pl.multiple_of(i * edge, edge), edge)

    def each_live(visit):
        def owner(o, carry):
            def slot(j, inner):
                visit(o, j, meta_s[o, 0, j], meta_s[o, 1, j])
                return inner
            return lax.fori_loop(0, meta_s[o, 2, 0], slot, carry)
        lax.fori_loop(0, n, owner, 0)

    def fetch(o, j, row, col):
        pltpu.make_async_copy(hid_hbm.at[:, columns(row)], hid_v.at[o, j], hid_sem).start()
        row_left[row] = row_left[row] + 1
        col_left[col] = col_left[col] + 1

    each_live(fetch)

    def blank(left, target, sem):
        def step(i, carry):
            @pl.when(left[i] == 0)
            def _():
                pltpu.make_async_copy(zero_v, target.at[:, columns(i)], sem).start()
            return carry
        lax.fori_loop(0, left.shape[0], step, 0)

    blank(row_left, grad_hbm, g_sem)
    blank(col_left, layer_hbm, l_sem)
    tile_copy.wait()
    cot_copy.wait()

    def add_block(at, value, left, seen, total, out, target, sem):
        remaining = left[at] - 1
        first = seen[at] == 0
        left[at] = remaining
        seen[at] = 1

        @pl.when(first & (remaining == 0))
        def _():
            out[at] = value[...].astype(BF16)

        @pl.when(first & (remaining > 0))
        def _():
            total[at] = value[...]

        @pl.when(jnp.logical_not(first))
        def _():
            summed = total[at] + value[...]
            total[at] = summed
            out[at] = summed.astype(BF16)

        @pl.when(remaining == 0)
        def _():
            pltpu.make_async_copy(out.at[at], target.at[:, columns(at)], sem).start()

    def backward(o, carry):
        for j in range(maxb):
            values[j] = lax.dot_general(
                cot_v[:, columns(meta_s[o, 1, j])], tiles_v[o, j], (((1,), (1,)), ((), ())),
                preferred_element_type=F32,
            )

        def slot(j, inner):
            add_block(
                meta_s[o, 0, j], values.at[j], row_left, row_seen, gacc, gout, grad_hbm, g_sem
            )
            return inner

        return lax.fori_loop(0, meta_s[o, 2, 0], slot, carry)

    lax.fori_loop(0, n, backward, 0)

    def arrived(o, j, row, col):
        pltpu.make_async_copy(hid_hbm.at[:, columns(row)], hid_v.at[o, j], hid_sem).wait()

    each_live(arrived)

    def forward(o, carry):
        for j in range(maxb):
            values[j] = jnp.dot(hid_v[o, j], tiles_v[o, j], preferred_element_type=F32)

        def slot(j, inner):
            add_block(
                meta_s[o, 1, j], values.at[j], col_left, col_seen, lacc, lout, layer_hbm, l_sem
            )
            return inner

        return lax.fori_loop(0, meta_s[o, 2, 0], slot, carry)

    lax.fori_loop(0, n, forward, 0)
    pltpu.make_async_copy(grad_hbm, grad_hbm, g_sem).wait()
    pltpu.make_async_copy(layer_hbm, layer_hbm, l_sem).wait()


def fused_kernel(
    n, dp, root,
    rows_hbm, cols_hbm, cnt_s, tiles_hbm, hid_hbm, cot_hbm,
    grad_out, layer_out, wg_out, table_s,
    rows_s, cols_s, hid_v, cot_v, tiles_v, meta_v, full_v, full_s, table_v,
    acc, sbuf, rbuf, fin, zs, zr, za, sqf, grad_q, layer_q,
    in_sem, send_sem, meta_rs, ag_rs, pair_rs, rs_rs, z_rs, za_rs, zb_rs, zf_rs, sq_rs, ready,
):
    me = lax.axis_index("fsdp")
    z = lax.axis_index("dp")
    maxb, edge = tiles_hbm.shape[0], tiles_hbm.shape[1]
    slots = n * maxb
    half = maxb // 2
    rows_z = 2 * edge // dp
    stages = n.bit_length() - 1
    chip_bits = stages - 1
    chips = n // 2
    orders = [list(range(1, stages)), list(range(stages - 1, 0, -1))]

    def bit_of(b):
        return lax.rem(me // (2 ** b), 2)

    def relative(x):
        other = me
        for b in range(stages):
            if (x >> b) & 1:
                other = other + (1 - 2 * bit_of(b)) * (2 ** b)
        return other

    def z_peer(r):
        return lax.rem(z + r, dp)

    z_near = z + 1 - 2 * lax.rem(z, 2)
    z_far = z + 2 - 4 * lax.rem(z // 2, 2)
    greeted = [z_near, z_far] if dp == 4 else [z_peer(r) for r in range(1, dp)]

    near = [x for x in range(n) if bin(x >> 1).count("1") < 2]
    far = [x for x in range(n) if x not in near]
    queue = [0, 1] + [x for x in near if x > 1 and x % 2 == 0]
    queue += [x for x in near if x > 1 and x % 2 == 1] + far
    place = [queue.index(x) for x in range(n)]

    def fetch(source, target, sem, first, last):
        def step(i, carry):
            at = pl.ds(pl.multiple_of(i * edge, edge), edge)
            pltpu.make_async_copy(source.at[:, at], target.at[i], sem).start()
            return carry
        lax.fori_loop(first, last, step, 0)

    def blocks_wait(count, sem):
        if count <= maxb:
            blocks = tiles_v.at[0, pl.ds(0, count)]
        else:
            blocks = tiles_v.at[pl.ds(0, count // maxb)]
        pltpu.make_async_copy(blocks, blocks, sem).wait()

    barrier = pltpu.get_barrier_semaphore()
    for peer in greeted:
        pl.semaphore_signal(barrier, inc=1, device_id={"dp": peer}, device_id_type=MESH)
    for x in range(n - 1, 0, -1):
        pl.semaphore_signal(
            barrier, inc=1, device_id={"fsdp": relative(x)}, device_id_type=MESH
        )
    rows_copy = pltpu.make_async_copy(rows_hbm, rows_s, in_sem.at[2])
    rows_copy.start()
    cols_copy = pltpu.make_async_copy(cols_hbm, cols_s, in_sem.at[3])
    cols_copy.start()
    own_copy = pltpu.make_async_copy(tiles_hbm, tiles_v.at[0], in_sem.at[7])
    own_copy.start()

    early = hid_v.shape[0] * 3 // 8
    fetch(cot_hbm, cot_v, in_sem.at[1], 0, cot_v.shape[0])
    fetch(hid_hbm, hid_v, in_sem.at[0], 0, early)

    lane = lax.broadcasted_iota(jnp.int32, (8, 128), 1)
    sub = lax.broadcasted_iota(jnp.int32, (8, 128), 0)
    meta = jnp.where(sub == 2, cnt_s[0], 0)
    rows_copy.wait()
    cols_copy.wait()
    for j in range(maxb):
        here = lax.rem(lane, maxb) == j
        meta = jnp.where((sub == 0) & here, rows_s[j], meta)
        meta = jnp.where((sub == 1) & here, cols_s[j], meta)
    meta_v[0] = meta
    pl.semaphore_wait(barrier, n - 1 + len(greeted))
    if dp == 4:
        pl.semaphore_signal(ready, inc=1, device_id={"dp": z_near}, device_id_type=MESH)

    for x in range(n - 1, 0, -1):
        pltpu.make_async_remote_copy(
            meta_v.at[0], meta_v.at[place[x]], send_sem.at[0], meta_rs.at[int(x in far)],
            device_id={"fsdp": relative(x)}, device_id_type=MESH,
        ).start()
    own_copy.wait()

    ag_done = set()

    def ag_index(i, e, h):
        split = 0 < i < chip_bits and e == 0
        keys = [(i, e, h) for i in range(stages) for e in range(2 ** i) for h in range(2)
                if h == 0 or (0 < i < chip_bits and e == 0)]
        return keys.index((i, e, h if split else 0)), maxb // 2 if split else maxb

    def ag_send(p, i, e, h):
        bits = orders[p] + [0]
        owner = 0
        for t in range(len(bits)):
            if (e >> t) & 1:
                owner |= 1 << bits[t]
        part = pl.ds(p * half + h * (half // 2), half // 2)
        pltpu.make_async_remote_copy(
            tiles_v.at[place[owner], part], tiles_v.at[place[owner | (1 << bits[i])], part],
            send_sem.at[1], ag_rs.at[ag_index(i, e, h)[0]],
            device_id={"fsdp": relative(1 << bits[i])}, device_id_type=MESH,
        ).start()

    def ag_wait(i, e, h):
        index, count = ag_index(i, e, h)
        if index not in ag_done:
            ag_done.add(index)
            blocks_wait(count, ag_rs.at[index])

    for i in range(stages):
        for p in range(2):
            for h in range(2):
                if h == 0 or i == 0 or i == chip_bits:
                    ag_send(p, i, 0, h)

    grad_q[slots] = jnp.zeros(grad_q.shape[1:], F32)
    layer_q[slots] = jnp.zeros(layer_q.shape[1:], F32)
    grad_out[slots] = jnp.zeros(grad_out.shape[1:], BF16)
    layer_out[slots] = jnp.zeros(layer_out.shape[1:], BF16)

    fetch(hid_hbm, hid_v, in_sem.at[0], early, hid_v.shape[0])

    def collect(xs, full):
        arrive = [x for x in xs if x]
        first = min(place[x] for x in arrive)
        metas = meta_v.at[pl.ds(first, len(arrive))]
        pltpu.make_async_copy(metas, metas, meta_rs.at[int(xs is far)]).wait()
        for x in xs:
            full = jnp.where(lane // maxb == place[x], meta_v[place[x]], full)
        return full

    def to_smem(k):
        return pltpu.make_async_copy(full_v.at[k], full_s.at[k], in_sem.at[4 + k])

    known = collect(near, jnp.zeros((8, 128), jnp.int32))
    full_v[0] = known
    to_smem(0).start()

    def term(x, j, named=None):
        q = place[x] * maxb + j
        k = 0 if x in near else 1
        row = full_s[k, 0, q] if named is None else named[0, q]
        col = full_s[k, 1, q] if named is None else named[1, q]
        return lax.dot_general(
            hid_v[row], cot_v[col],
            (((0,), (0,)), ((), ())), preferred_element_type=F32,
        )

    def owner_at(p, e):
        owner = 0
        for t, b in enumerate(orders[p]):
            if not (e >> (chip_bits - 1 - t)) & 1:
                owner |= 1 << b
        return owner

    offsets = [0]
    for t in range(stages):
        offsets.append(offsets[-1] + (n >> (t + 1)))

    def pair_copy(p, e):
        return pltpu.make_async_remote_copy(
            sbuf.at[p, e], rbuf.at[p, e], send_sem.at[2], pair_rs.at[e],
            device_id={"fsdp": relative(1)}, device_id_type=MESH,
        )

    def rs_copy(p, t, e, c):
        where = offsets[t] + e
        return pltpu.make_async_remote_copy(
            sbuf.at[p, where, c], rbuf.at[p, where, c],
            send_sem.at[2], rs_rs.at[t - 1, c],
            device_id={"fsdp": relative(1 << orders[p][t - 1])}, device_id_type=MESH,
        )

    def foreign(e, named=None):
        for p in range(2):
            for c in range(half):
                sbuf[p, e, c] = term(owner_at(p, e) | 1, p * half + c, named).astype(BF16)
        for p in range(2):
            pair_copy(p, e).start()

    def own(e):
        for p in range(2):
            for c in range(half):
                acc[p, e, c] = term(owner_at(p, e), p * half + c)

    starts = [0]
    for t in range(stages):
        starts.append(starts[-1] + (n >> (t + 1)) // 2)

    paired = set()

    def pair_wait(e):
        if e not in paired:
            paired.add(e)
            blocks_wait(maxb, pair_rs.at[e])

    def pass_on(e, cs):
        for p in range(2):
            pair_wait(e)
            for c in cs:
                total = acc[p, e, c] + rbuf[p, e, c].astype(F32)
                sbuf[p, offsets[1] + e, c] = total.astype(BF16)
            for c in cs:
                rs_copy(p, 1, e, c).start()

    def reduce_step(t, c):
        m = n >> (t + 1)
        blocks_wait(2 * m, rs_rs.at[t - 1, c])
        for e in range(m):
            for p in range(2):
                at_e = starts[t] + e
                total = acc[p, at_e, c] + rbuf[p, offsets[t] + e, c].astype(F32)
                if t == 1:
                    total = total + rbuf[p, at_e, c].astype(F32)
                if e < m // 2:
                    sbuf[p, offsets[t + 1] + e, c] = total.astype(BF16)
                    rs_copy(p, t + 1, e, c).start()
                elif m > 1:
                    acc[p, at_e, c] = total
                else:
                    at = pl.ds(p * edge, edge)
                    fin[c, at] = total
                    zs[c, at] = total.astype(BF16)
        if m == 1:
            for r in range(1, dp):
                z_copy(c, r).start()

    def z_rows(index):
        return pl.ds(pl.multiple_of(index * rows_z, rows_z), rows_z)

    def z_copy(c, r):
        return pltpu.make_async_remote_copy(
            zs.at[c, z_rows(z_peer(r))], zr.at[c, r - 1], send_sem.at[3], z_rs.at[c],
            device_id={"dp": z_peer(r)}, device_id_type=MESH,
        )

    def a_copy(c, piece, peer, sem):
        return pltpu.make_async_remote_copy(
            za.at[c, z_rows(piece)], za.at[c, z_rows(piece)], send_sem.at[4], sem,
            device_id={"dp": peer}, device_id_type=MESH,
        )

    handed = half // 2 if dp == 4 else 0

    def z_sum(c, squares):
        piece = fin[c, z_rows(z)]
        pltpu.make_async_copy(zr.at[c], zr.at[c], z_rs.at[c]).wait()
        for r in range(1, dp):
            piece = piece + zr[c, r - 1].astype(F32)
        row = z * rows_z + lax.broadcasted_iota(jnp.int32, piece.shape, 0)
        slot = (row // edge) * half + c
        piece = piece * jnp.clip(cnt_s[0] - slot, 0, 1).astype(F32)
        za[c, z_rows(z)] = piece.astype(BF16)
        return squares + jnp.sum((piece * piece).reshape(-1, 8, 128), axis=0)

    def a_send(c):
        for r in range(1, dp):
            a_copy(c, z, z_peer(r), za_rs).start()

    def a_cross(c):
        a_copy(c, z, z_far, zf_rs.at[c]).start()
        a_copy(c, z, z_near, zb_rs).start()

    def a_hand(c):
        a_copy(c, z, z_far, zf_rs.at[c]).wait_recv()
        a_copy(c, z_far, z_near, zb_rs).start()

    def z_step(c, squares):
        squares = z_sum(c, squares)
        a_send(c)
        return squares

    def project(at):
        def load(j):
            q = at * maxb + j
            backward = lax.dot_general(
                cot_v[full_s[1, 1, q]], tiles_v[at, j], (((1,), (1,)), ((), ())),
                preferred_element_type=F32,
            )
            forward = jnp.dot(hid_v[full_s[1, 0, q]], tiles_v[at, j], preferred_element_type=F32)
            return q, backward, forward
        for j in range(maxb):
            q, backward, forward = load(j)
            backward = backward + grad_q[table_s[0, q]]
            grad_q[q] = backward
            grad_out[q] = backward.astype(BF16)
            forward = forward + layer_q[table_s[1, q]]
            layer_q[q] = forward
            layer_out[q] = forward.astype(BF16)

    def arrived(x):
        for p in range(2):
            bits = orders[p] + [0]
            index = [t for t in range(stages) if (x >> bits[t]) & 1]
            if index:
                e = sum(1 << t for t in index[:-1])
                for h in range(2):
                    ag_wait(index[-1], e, h)

    sent = sorted(range(chips // 2), key=lambda e: bin(owner_at(0, e)).count("1"))
    kept = list(range(chips // 2, chips))
    pltpu.make_async_copy(cot_v, cot_v, in_sem.at[1]).wait()
    pltpu.make_async_copy(hid_v, hid_v, in_sem.at[0]).wait()
    foreign(sent[0], known)
    to_smem(0).wait()
    full = collect(far, known)
    full_v[1] = full
    to_smem(1).start()
    for e in sent[1:]:
        foreign(e, full)
    own(sent[0])
    to_smem(1).wait()
    pass_on(sent[0], [0, 1])
    for e in sent[1:]:
        own(e)
    foreign(kept[0])
    for e in sent[1:]:
        pass_on(e, [0, 1])
    for c in range(2, half - 1):
        for e in sent:
            pass_on(e, [c])
    for e in kept[1:]:
        foreign(e)

    wide = lax.broadcasted_iota(jnp.int32, (slots, 128), 1)
    tall = lax.broadcasted_iota(jnp.int32, (slots, 128), 0)
    alive = lax.rem(lane[0:1], maxb) < full[2:3]
    table = jnp.full((8, 128), slots, jnp.int32)
    for k in range(2):
        named = jnp.broadcast_to(jnp.where(alive, full[k:k + 1], -1), (slots, 128))
        named_t = jnp.sum(jnp.where(wide == tall, named, 0), axis=1, keepdims=True)
        before = jnp.max(
            jnp.where((named_t == named) & (tall < wide), tall, -1), axis=0, keepdims=True
        )
        last = jnp.max(jnp.where(named_t == wide, tall, -1), axis=0, keepdims=True)
        table = jnp.where(sub == k, jnp.where(before < 0, slots, before), table)
        table = jnp.where(sub == 2 + k, jnp.where(last < 0, slots, last), table)
    table_v[...] = table
    table_copy = pltpu.make_async_copy(table_v, table_s, in_sem.at[6])
    table_copy.start()
    for e in kept:
        own(e)
    table_copy.wait()

    def project_all(xs):
        for x in xs:
            arrived(x)
        first = place[xs[0]]

        def one(at, carry):
            project(at)
            return carry

        lax.fori_loop(first, first + len(xs), one, 0)

    def ag_pass(i, e, h):
        ag_wait(i, e, h)
        for p in range(2):
            ag_send(p, chip_bits, e + 2 ** i, h)

    project_all([0, 1])
    for h in range(2):
        for i in range(chip_bits if h == 0 else 1):
            ag_pass(i, 0, h)
    for e in kept:
        pair_wait(e)
    reduce_step(1, 0)
    for e in sent:
        pass_on(e, [half - 1])

    def second(c, carry):
        reduce_step(1, c)
        return carry

    lax.fori_loop(1, half - 1, second, 0)
    if dp == 4:
        pl.semaphore_wait(ready, 1)
    for t in range(2, stages):
        reduce_step(t, 0)
    reduce_step(1, half - 1)
    for t in range(2, stages):
        def third(c, carry):
            reduce_step(t, c)
            return carry

        lax.fori_loop(1, half, third, 0)

    for i in range(1, chip_bits):
        for p in range(2):
            ag_send(p, i, 0, 1)
    for i in range(1, chip_bits):
        for e in range(1, 2 ** i):
            for p in range(2):
                for h in range(2):
                    ag_wait(i - 1, e - 2 ** (i - 1), h)
                    ag_send(p, i, e, h)

    squares = lax.fori_loop(0, handed, z_sum, jnp.zeros((8, 128), F32))
    for c in range(handed):
        a_cross(c)
    squares = lax.fori_loop(handed, half // 2, z_step, squares)
    for i in range(1, chip_bits):
        ag_pass(i, 0, 1)
    project_all([x for x in near if x > 1 and x % 2 == 0])
    squares = lax.fori_loop(half // 2, half - 1, z_step, squares)
    squares = z_sum(half - 1, squares)
    device = me * dp + z
    sqf[device] = jnp.sum(squares, axis=0, keepdims=True)
    for x in reversed(queue):
        for r in range(dp):
            if x or r:
                pltpu.make_async_remote_copy(
                    sqf.at[device], sqf.at[device], send_sem.at[5], sq_rs,
                    device_id={"fsdp": relative(x), "dp": z_peer(r)}, device_id_type=MESH,
                ).start()
    a_send(half - 1)
    for i in range(1, chip_bits):
        for e in range(1, 2 ** i):
            for h in range(2):
                ag_pass(i, e, h)
    crossed = [x for x in near if x > 1 and x % 2 == 1]
    project_all(crossed)
    for c in range(handed):
        a_hand(c)
    project_all(far)

    entries = full_s[1, 2, 0]
    for x in range(1, n):
        entries = entries + full_s[1, 2, x * maxb]
    others = sqf.at[pl.ds(0, n * dp - 1)]
    pltpu.make_async_copy(others, others, sq_rs).wait()
    squares = jnp.sum(jnp.sum(sqf[...], axis=0), axis=1, keepdims=True)
    live = jnp.full((1, 1), entries, jnp.int32).astype(F32) * edge * edge
    spread = jnp.sqrt(squares / live)
    factor = jnp.minimum(1.0, 0.5 * root / spread) / root

    if handed:
        twice = za.at[pl.ds(0, handed)]
        pltpu.make_async_copy(twice.at[:, pl.ds(0, 2 * rows_z)], twice.at[:, pl.ds(0, 2 * rows_z)], zb_rs).wait()
    direct = zr.at[pl.ds(handed, half - handed)]
    pltpu.make_async_copy(direct, direct, za_rs).wait()

    def finish(c, carry):
        for p in range(2):
            wg_out[p * half + c] = za[c, pl.ds(p * edge, edge)].astype(F32) * factor
        return carry

    lax.fori_loop(0, half, finish, 0)

    metas = meta_v.at[pl.ds(1, n - 1)]
    gathered = tiles_v.at[pl.ds(1, n - 1)]
    for k, sent in enumerate((metas, gathered, sbuf, zr, zr, others)):
        pltpu.make_async_copy(sent, sent, send_sem.at[k]).wait()


def write_kernel(
    grad_v, layer_v, wg_v, table_s,
    layer_hbm, grad_hbm, wg_hbm,
    w_sem, g_sem, l_sem,
):
    edge = grad_v.shape[2]

    def write(row, source, target, sem):
        def step(i, carry):
            at = pl.ds(pl.multiple_of(i * edge, edge), edge)
            pltpu.make_async_copy(source.at[table_s[row, i]], target.at[:, at], sem).start()
            return carry
        lax.fori_loop(0, target.shape[1] // edge, step, 0)

    write(2, grad_v, grad_hbm, g_sem)
    write(3, layer_v, layer_hbm, l_sem)
    wg_copy = pltpu.make_async_copy(wg_v, wg_hbm, w_sem)
    wg_copy.start()
    pltpu.make_async_copy(grad_hbm, grad_hbm, g_sem).wait()
    pltpu.make_async_copy(layer_hbm, layer_hbm, l_sem).wait()
    wg_copy.wait()


def fused(n, dp, hidden, cotangent, tiles, tile_rows, tile_cols, counts):
    tokens, width_ff = hidden.shape
    maxb, edge, _ = tiles.shape
    root = math.sqrt(tokens * n * dp)
    slots, half, stages = n * maxb, maxb // 2, n.bit_length() - 1
    in_hbm = functools.partial(pltpu.with_memory_space_constraint, memory_space=pltpu.HBM)
    rows_z = 2 * edge // dp
    hbm = pl.BlockSpec(memory_space=pltpu.HBM)
    smem = pl.BlockSpec(memory_space=pltpu.SMEM)
    vmem = pl.BlockSpec(memory_space=pltpu.VMEM)
    dma = pltpu.SemaphoreType.DMA
    grad, layer, weight, table = pl.pallas_call(
        functools.partial(fused_kernel, n, dp, root),
        out_shape=(
            pltpu.VMEM((slots + 1, tokens, edge), BF16),
            pltpu.VMEM((slots + 1, tokens, edge), BF16),
            pltpu.VMEM((maxb, edge, edge), F32),
            pltpu.SMEM((8, 128), jnp.int32),
        ),
        in_specs=[hbm, hbm, smem, hbm, hbm, hbm],
        out_specs=(vmem, vmem, vmem, smem),
        scratch_shapes=[
            pltpu.SMEM(tile_rows.shape, jnp.int32),
            pltpu.SMEM(tile_cols.shape, jnp.int32),
            pltpu.VMEM((hidden.shape[1] // edge, tokens, edge), BF16),
            pltpu.VMEM((cotangent.shape[1] // edge, tokens, edge), BF16),
            pltpu.VMEM((n, maxb, edge, edge), BF16),
            pltpu.VMEM((n, 8, 128), jnp.int32),
            pltpu.VMEM((2, 8, 128), jnp.int32),
            pltpu.SMEM((2, 8, 128), jnp.int32),
            pltpu.VMEM((8, 128), jnp.int32),
            pltpu.VMEM((2, n // 2, half, edge, edge), F32),
            pltpu.VMEM((2, n - 1, half, edge, edge), BF16),
            pltpu.VMEM((2, n - 1, half, edge, edge), BF16),
            pltpu.VMEM((half, 2 * edge, edge), F32),
            pltpu.VMEM((half, 2 * edge, edge), BF16),
            pltpu.VMEM((half, dp - 1, rows_z, edge), BF16),
            pltpu.VMEM((half, 2 * edge, edge), BF16),
            pltpu.VMEM((n * dp, 1, 128), F32),
            pltpu.VMEM((slots + 1, tokens, edge), F32),
            pltpu.VMEM((slots + 1, tokens, edge), F32),
            dma((8,)), dma((6,)), dma((2,)),
            dma((n - 1 + max(stages - 2, 0),)),
            dma((n // 2,)), dma((stages - 1, half)), dma((half,)), dma, dma, dma((half,)), dma,
            pltpu.SemaphoreType.REGULAR,
        ],
        compiler_params=pltpu.CompilerParams(
            collective_id=0, has_side_effects=True, vmem_limit_bytes=44 * 2 ** 20
        ),
        name="fused",
    )(in_hbm(tile_rows), in_hbm(tile_cols), counts, in_hbm(tiles), in_hbm(hidden), in_hbm(cotangent))
    return pl.pallas_call(
        write_kernel,
        out_shape=(
            jax.ShapeDtypeStruct(cotangent.shape, BF16),
            jax.ShapeDtypeStruct(hidden.shape, BF16),
            jax.ShapeDtypeStruct(tiles.shape, F32),
        ),
        in_specs=[vmem, vmem, vmem, smem],
        out_specs=(hbm, hbm, hbm),
        scratch_shapes=[dma, dma, dma],
        compiler_params=pltpu.CompilerParams(vmem_limit_bytes=16 * 2 ** 20),
        name="write",
    )(grad, layer, weight, table)


def shards(n, dp, hidden, cotangent, tiles, tile_rows, tile_cols, counts):
    tokens, width_ff = hidden.shape
    width_model = cotangent.shape[1]
    maxb, edge, _ = tiles.shape
    blocks_ff, blocks_model = width_ff // edge, width_model // edge
    root = math.sqrt(tokens * n * dp)
    half, per = maxb // 2, maxb // dp
    sums = n * maxb * tokens * edge * 12
    if n == 8 and dp % 2 == 0 and max(n * maxb, blocks_ff, blocks_model) <= 128 and sums <= 28 * 2 ** 20:
        return fused(n, dp, hidden, cotangent, tiles, tile_rows, tile_cols, counts)
    hbm = pl.BlockSpec(memory_space=pl.ANY)
    smem = pl.BlockSpec(memory_space=pltpu.SMEM)
    vmem = pl.BlockSpec(memory_space=pltpu.VMEM)
    dma = pltpu.SemaphoreType.DMA
    meta, gathered, weight_grad = pl.pallas_call(
        functools.partial(exchange_kernel, n, dp, root),
        out_shape=(
            jax.ShapeDtypeStruct((n, 8, 128), jnp.int32),
            jax.ShapeDtypeStruct((n, maxb, edge, edge), BF16),
            jax.ShapeDtypeStruct((maxb, edge, edge), F32),
        ),
        in_specs=[smem, smem, smem, hbm, hbm, hbm],
        out_specs=(hbm, hbm, vmem),
        scratch_shapes=[
            pltpu.VMEM((blocks_ff, tokens, edge), BF16),
            pltpu.VMEM((blocks_model, tokens, edge), BF16),
            pltpu.VMEM((n, maxb, edge, edge), BF16),
            pltpu.VMEM((n, 8, 128), jnp.int32),
            pltpu.SMEM((n, 8, 128), jnp.int32),
            pltpu.VMEM((2, n // 2, half, edge, edge), F32),
            pltpu.VMEM((2, n - 1, half, edge, edge), BF16),
            pltpu.VMEM((2, n - 1, half, edge, edge), BF16),
            pltpu.VMEM((maxb, edge, edge), F32),
            pltpu.VMEM((dp, per, edge, edge), BF16),
            pltpu.VMEM((dp - 1, per, edge, edge), BF16),
            pltpu.VMEM((dp, per, edge, edge), BF16),
            pltpu.VMEM((dp, 8, 128), F32),
            pltpu.VMEM((n, 8, 128), F32),
            dma((4,)), dma((2,)),
            dma((n - 1,)), dma((n - 1,)),
            dma((2, n - 1)), dma((2, n - 1)),
            dma((2, n - 1)), dma((2, n - 1)),
            dma((dp - 1,)), dma((dp - 1,)),
            dma((dp - 1,)), dma((dp - 1,)),
            dma((dp - 1,)), dma((dp - 1,)),
            dma((n - 1,)), dma((n - 1,)),
        ],
        compiler_params=pltpu.CompilerParams(
            collective_id=0, has_side_effects=True, vmem_limit_bytes=60 * 2 ** 20
        ),
        name="exchange",
    )(tile_rows, tile_cols, counts, tiles, hidden, cotangent)

    layer_out, hidden_grad = pl.pallas_call(
        functools.partial(project_kernel, n, maxb),
        out_shape=(
            jax.ShapeDtypeStruct(cotangent.shape, BF16),
            jax.ShapeDtypeStruct(hidden.shape, BF16),
        ),
        in_specs=[smem, hbm, hbm, hbm],
        out_specs=(hbm, hbm),
        scratch_shapes=[
            pltpu.VMEM((n, maxb, edge, edge), BF16),
            pltpu.VMEM(cotangent.shape, BF16),
            pltpu.VMEM((n, maxb, tokens, edge), BF16),
            pltpu.VMEM((blocks_ff, tokens, edge), F32),
            pltpu.VMEM((blocks_ff, tokens, edge), BF16),
            pltpu.VMEM((blocks_model, tokens, edge), F32),
            pltpu.VMEM((blocks_model, tokens, edge), BF16),
            pltpu.VMEM((tokens, edge), BF16),
            pltpu.VMEM((maxb, tokens, edge), F32),
            pltpu.SMEM((blocks_ff,), jnp.int32),
            pltpu.SMEM((blocks_ff,), jnp.int32),
            pltpu.SMEM((blocks_model,), jnp.int32),
            pltpu.SMEM((blocks_model,), jnp.int32),
            dma((2,)), dma, dma, dma,
        ],
        compiler_params=pltpu.CompilerParams(vmem_limit_bytes=62 * 2 ** 20),
        name="project",
    )(meta, gathered, hidden, cotangent)
    return layer_out, hidden_grad, weight_grad


def solution(mesh):
    placed = (
        P(("fsdp", "dp"), None),
        P(("fsdp", "dp"), None),
        P("fsdp", None, None),
        P("fsdp"),
        P("fsdp"),
        P("fsdp"),
    )
    return jax.shard_map(
        functools.partial(shards, mesh.shape["fsdp"], mesh.shape["dp"]),
        mesh=mesh,
        in_specs=placed,
        out_specs=(P(("fsdp", "dp"), None), P(("fsdp", "dp"), None), P("fsdp", None, None)),
        check_vma=False,
    )
```

```python
import functools
import math

import jax
import jax.numpy as jnp
from jax import lax
from jax.experimental import pallas as pl
from jax.experimental.pallas import tpu as pltpu
from jax.sharding import PartitionSpec as P

MESH = pl.DeviceIdType.MESH
F32 = jnp.float32
BF16 = jnp.bfloat16


def exchange_kernel(
    n, dp, root,
    rows_s, cols_s, cnt_s, tiles_hbm, hid_hbm, cot_hbm,
    meta_out, tiles_out, wg_out,
    hid_v, cot_v, tiles_v, meta_v, meta_s, acc, sbuf, rbuf, fin, zs, zr, za, sqz, sqf,
    in_sem, out_sem, meta_ss, meta_rs, ag_ss, ag_rs, rs_ss, rs_rs,
    zs_ss, zs_rs, za_ss, za_rs, qz_ss, qz_rs, qf_ss, qf_rs,
):
    me = lax.axis_index("fsdp")
    z = lax.axis_index("dp")
    maxb, edge = tiles_hbm.shape[0], tiles_hbm.shape[1]
    half = maxb // 2
    per = maxb // dp
    stages = n.bit_length() - 1
    chip_bits = stages - 1
    orders = [list(range(1, stages)), list(range(stages - 1, 0, -1))]
    core = lax.rem(me, 2)

    def bit_of(b):
        return lax.rem(me // (2 ** b), 2)

    def flip(value_me, b):
        return value_me + (1 - 2 * bit_of(b)) * (2 ** b)

    def fetch(source, target, sem):
        def step(i, carry):
            at = pl.ds(pl.multiple_of(i * edge, edge), edge)
            pltpu.make_async_copy(source.at[:, at], target.at[i], sem).start()
            return carry
        lax.fori_loop(0, target.shape[0], step, 0)

    own_copy = pltpu.make_async_copy(tiles_hbm, tiles_v.at[me], in_sem.at[2])
    own_copy.start()
    fetch(cot_hbm, cot_v, in_sem.at[1])
    fetch(hid_hbm, hid_v, in_sem.at[0])

    barrier = pltpu.get_barrier_semaphore()
    for k in range(1, n):
        pl.semaphore_signal(
            barrier, inc=1, device_id={"fsdp": lax.rem(me + k, n)}, device_id_type=MESH
        )
    for k in range(1, dp):
        pl.semaphore_signal(
            barrier, inc=1, device_id={"dp": lax.rem(z + k, dp)}, device_id_type=MESH
        )
    lane = lax.broadcasted_iota(jnp.int32, (8, 128), 1)
    sub = lax.broadcasted_iota(jnp.int32, (8, 128), 0)
    meta = jnp.where(sub == 2, cnt_s[0], 0)
    for j in range(maxb):
        meta = jnp.where((sub == 0) & (lane == j), rows_s[j], meta)
        meta = jnp.where((sub == 1) & (lane == j), cols_s[j], meta)
    meta_v[me] = meta
    own_copy.wait()
    pl.semaphore_wait(barrier, n - 1 + dp - 1)

    meta_copies = []
    for k in range(1, n):
        copy = pltpu.make_async_remote_copy(
            meta_v.at[me], meta_v.at[me], meta_ss.at[k - 1], meta_rs.at[k - 1],
            device_id={"fsdp": lax.rem(me + k, n)}, device_id_type=MESH,
        )
        copy.start()
        meta_copies.append(copy)

    ag_copies = {}

    def ag_send(p, i, e):
        bits = orders[p] + [0]
        owner = me
        for t in range(len(bits)):
            if (e >> t) & 1:
                owner = flip(owner, bits[t])
        piece = tiles_v.at[owner, pl.ds(p * half, half)]
        where = 2 ** i - 1 + e
        copy = pltpu.make_async_remote_copy(
            piece, piece, ag_ss.at[p, where], ag_rs.at[p, where],
            device_id={"fsdp": flip(me, bits[i])}, device_id_type=MESH,
        )
        copy.start()
        ag_copies[p, i, e] = copy

    for i in range(stages):
        for p in range(2):
            ag_send(p, i, 0)

    for copy in meta_copies:
        copy.wait_recv()
    to_smem = pltpu.make_async_copy(meta_v, meta_s, in_sem.at[3])
    to_smem.start()
    to_smem.wait()
    meta_back = pltpu.make_async_copy(meta_v, meta_out, out_sem.at[0])
    meta_back.start()
    pltpu.make_async_copy(cot_v, cot_v, in_sem.at[1]).wait()
    pltpu.make_async_copy(hid_v, hid_v, in_sem.at[0]).wait()

    def owner_at(p, e, core_bit):
        owner = core_bit
        for t, b in enumerate(orders[p]):
            ebit = lax.rem(e // (2 ** (chip_bits - 1 - t)), 2)
            owner = owner + lax.rem(bit_of(b) + 1 + ebit, 2) * (2 ** b)
        return owner

    def term(owner, j):
        return lax.dot_general(
            hid_v[meta_s[owner, 0, j]], cot_v[meta_s[owner, 1, j]],
            (((0,), (0,)), ((), ())), preferred_element_type=F32,
        )

    chips = n // 2
    offsets = [0]
    for t in range(stages):
        offsets.append(offsets[-1] + (n >> (t + 1)))

    def rs_copy(p, t, e):
        where = offsets[t] + e
        bit = 0 if t == 0 else orders[p][t - 1]
        return pltpu.make_async_remote_copy(
            sbuf.at[p, where], rbuf.at[p, where], rs_ss.at[p, where], rs_rs.at[p, where],
            device_id={"fsdp": flip(me, bit)}, device_id_type=MESH,
        )

    def foreign(e, carry):
        for p in range(2):
            owner = owner_at(p, e, 1 - core)
            for j in range(half):
                sbuf[p, e, j] = term(owner, p * half + j).astype(BF16)
            rs_copy(p, 0, e).start()
        return carry

    lax.fori_loop(0, chips, foreign, 0)

    for i in range(chip_bits):
        for p in range(2):
            for e in range(2 ** i):
                ag_copies[p, i, e].wait_recv()
                for i2 in range(i + 1, stages):
                    ag_send(p, i2, e + 2 ** i)

    def own(e, carry):
        for p in range(2):
            owner = owner_at(p, e, core)
            for j in range(half):
                acc[p, e, j] = term(owner, p * half + j)
        return carry

    lax.fori_loop(0, chips, own, 0)

    start = 0
    for t in range(stages):
        m = n >> (t + 1)
        sent = m // 2
        for e in range(m):
            for p in range(2):
                rs_copy(p, t, e).wait_recv()
                total = acc[p, start + e] + rbuf[p, offsets[t] + e].astype(F32)
                if e < sent:
                    sbuf[p, offsets[t + 1] + e] = total.astype(BF16)
                    rs_copy(p, t + 1, e).start()
                elif m > 1:
                    acc[p, start + e] = total
                else:
                    fin[pl.ds(p * half, half)] = total
                    for q in range(half // per):
                        zs[p * (half // per) + q] = total[q * per:(q + 1) * per].astype(BF16)
        start += sent

    def z_peer(r):
        return lax.rem(z + r, dp)

    z_copies = []
    for r in range(1, dp):
        copy = pltpu.make_async_remote_copy(
            zs.at[z_peer(r)], zr.at[r - 1], zs_ss.at[r - 1], zs_rs.at[r - 1],
            device_id={"dp": z_peer(r)}, device_id_type=MESH,
        )
        copy.start()
        z_copies.append(copy)

    for p in range(2):
        for e in range(2 ** chip_bits):
            ag_copies[p, chip_bits, e].wait_recv()
    tiles_back = pltpu.make_async_copy(tiles_v, tiles_out, out_sem.at[1])
    tiles_back.start()

    piece = fin[pl.ds(z * per, per)]
    for r in range(1, dp):
        z_copies[r - 1].wait_recv()
        piece = piece + zr[r - 1].astype(F32)
    slot = z * per + lax.broadcasted_iota(jnp.int32, piece.shape, 0)
    piece = piece * jnp.clip(cnt_s[0] - slot, 0, 1).astype(F32)
    za[z] = piece.astype(BF16)
    sqz[z] = jnp.sum((piece * piece).reshape(-1, 8, 128), axis=0)
    a_copies, q_copies = [], []
    for r in range(1, dp):
        copy = pltpu.make_async_remote_copy(
            sqz.at[z], sqz.at[z], qz_ss.at[r - 1], qz_rs.at[r - 1],
            device_id={"dp": z_peer(r)}, device_id_type=MESH,
        )
        copy.start()
        q_copies.append(copy)
    for r in range(1, dp):
        copy = pltpu.make_async_remote_copy(
            za.at[z], za.at[z], za_ss.at[r - 1], za_rs.at[r - 1],
            device_id={"dp": z_peer(r)}, device_id_type=MESH,
        )
        copy.start()
        a_copies.append(copy)
    for copy in q_copies:
        copy.wait_recv()
    sqf[me] = jnp.sum(sqz[...], axis=0)
    f_copies = []
    for k in range(1, n):
        copy = pltpu.make_async_remote_copy(
            sqf.at[me], sqf.at[me], qf_ss.at[k - 1], qf_rs.at[k - 1],
            device_id={"fsdp": lax.rem(me + k, n)}, device_id_type=MESH,
        )
        copy.start()
        f_copies.append(copy)
    entries = meta_s[0, 2, 0]
    for k in range(1, n):
        entries = entries + meta_s[k, 2, 0]
    for copy in a_copies + f_copies:
        copy.wait_recv()
    squares = jnp.sum(jnp.sum(sqf[...], axis=0), axis=(0, 1), keepdims=True)
    live = jnp.full((1, 1), entries, jnp.int32).astype(F32) * edge * edge
    spread = jnp.sqrt(squares / live)
    factor = jnp.minimum(1.0, 0.5 * root / spread) / root
    for q in range(dp):
        for i in range(per):
            wg_out[q * per + i] = za[q, i].astype(F32) * factor

    for copy in meta_copies + list(ag_copies.values()) + z_copies + q_copies + a_copies + f_copies:
        copy.wait_send()
    for t in range(stages):
        for e in range(n >> (t + 1)):
            for p in range(2):
                rs_copy(p, t, e).wait_send()
    meta_back.wait()
    tiles_back.wait()


def project_kernel(
    n, maxb,
    meta_s, tiles_hbm, hid_hbm, cot_hbm,
    layer_hbm, grad_hbm,
    tiles_v, cot_v, hid_v, gacc, gout, lacc, lout, zero_v, values,
    row_left, row_seen, col_left, col_seen,
    in_sem, hid_sem, g_sem, l_sem,
):
    edge = zero_v.shape[1]
    tile_copy = pltpu.make_async_copy(tiles_hbm, tiles_v, in_sem.at[0])
    cot_copy = pltpu.make_async_copy(cot_hbm, cot_v, in_sem.at[1])
    tile_copy.start()
    cot_copy.start()
    zero_v[...] = jnp.zeros_like(zero_v)

    def clear(left, seen):
        def step(i, carry):
            left[i] = 0
            seen[i] = 0
            return carry
        lax.fori_loop(0, left.shape[0], step, 0)

    clear(row_left, row_seen)
    clear(col_left, col_seen)

    def columns(i):
        return pl.ds(pl.multiple_of(i * edge, edge), edge)

    def each_live(visit):
        def owner(o, carry):
            def slot(j, inner):
                visit(o, j, meta_s[o, 0, j], meta_s[o, 1, j])
                return inner
            return lax.fori_loop(0, meta_s[o, 2, 0], slot, carry)
        lax.fori_loop(0, n, owner, 0)

    def fetch(o, j, row, col):
        pltpu.make_async_copy(hid_hbm.at[:, columns(row)], hid_v.at[o, j], hid_sem).start()
        row_left[row] = row_left[row] + 1
        col_left[col] = col_left[col] + 1

    each_live(fetch)

    def blank(left, target, sem):
        def step(i, carry):
            @pl.when(left[i] == 0)
            def _():
                pltpu.make_async_copy(zero_v, target.at[:, columns(i)], sem).start()
            return carry
        lax.fori_loop(0, left.shape[0], step, 0)

    blank(row_left, grad_hbm, g_sem)
    blank(col_left, layer_hbm, l_sem)
    tile_copy.wait()
    cot_copy.wait()

    def add_block(at, value, left, seen, total, out, target, sem):
        remaining = left[at] - 1
        first = seen[at] == 0
        left[at] = remaining
        seen[at] = 1

        @pl.when(first & (remaining == 0))
        def _():
            out[at] = value[...].astype(BF16)

        @pl.when(first & (remaining > 0))
        def _():
            total[at] = value[...]

        @pl.when(jnp.logical_not(first))
        def _():
            summed = total[at] + value[...]
            total[at] = summed
            out[at] = summed.astype(BF16)

        @pl.when(remaining == 0)
        def _():
            pltpu.make_async_copy(out.at[at], target.at[:, columns(at)], sem).start()

    def backward(o, carry):
        for j in range(maxb):
            values[j] = lax.dot_general(
                cot_v[:, columns(meta_s[o, 1, j])], tiles_v[o, j], (((1,), (1,)), ((), ())),
                preferred_element_type=F32,
            )

        def slot(j, inner):
            add_block(
                meta_s[o, 0, j], values.at[j], row_left, row_seen, gacc, gout, grad_hbm, g_sem
            )
            return inner

        return lax.fori_loop(0, meta_s[o, 2, 0], slot, carry)

    lax.fori_loop(0, n, backward, 0)

    def arrived(o, j, row, col):
        pltpu.make_async_copy(hid_hbm.at[:, columns(row)], hid_v.at[o, j], hid_sem).wait()

    each_live(arrived)

    def forward(o, carry):
        for j in range(maxb):
            values[j] = jnp.dot(hid_v[o, j], tiles_v[o, j], preferred_element_type=F32)

        def slot(j, inner):
            add_block(
                meta_s[o, 1, j], values.at[j], col_left, col_seen, lacc, lout, layer_hbm, l_sem
            )
            return inner

        return lax.fori_loop(0, meta_s[o, 2, 0], slot, carry)

    lax.fori_loop(0, n, forward, 0)
    pltpu.make_async_copy(grad_hbm, grad_hbm, g_sem).wait()
    pltpu.make_async_copy(layer_hbm, layer_hbm, l_sem).wait()


def fused_kernel(
    n, dp, root,
    rows_hbm, cols_hbm, cnt_s, tiles_hbm, hid_hbm, cot_hbm,
    grad_out, layer_out, wg_out, table_s,
    rows_s, cols_s, hid_v, cot_v, tiles_v, meta_v, full_v, full_s, table_v,
    acc, sbuf, rbuf, fin, zs, zr, za, sqf, grad_q, layer_q,
    in_sem, send_sem, meta_rs, ag_rs, pair_rs, rs_rs, z_rs, za_rs, zb_rs, zf_rs, sq_rs, ready,
):
    me = lax.axis_index("fsdp")
    z = lax.axis_index("dp")
    maxb, edge = tiles_hbm.shape[0], tiles_hbm.shape[1]
    slots = n * maxb
    half = maxb // 2
    rows_z = 2 * edge // dp
    stages = n.bit_length() - 1
    chip_bits = stages - 1
    chips = n // 2
    orders = [list(range(1, stages)), list(range(stages - 1, 0, -1))]

    def bit_of(b):
        return lax.rem(me // (2 ** b), 2)

    def relative(x):
        other = me
        for b in range(stages):
            if (x >> b) & 1:
                other = other + (1 - 2 * bit_of(b)) * (2 ** b)
        return other

    def z_peer(r):
        return lax.rem(z + r, dp)

    z_near = z + 1 - 2 * lax.rem(z, 2)
    z_far = z + 2 - 4 * lax.rem(z // 2, 2)
    greeted = [z_near, z_far] if dp == 4 else [z_peer(r) for r in range(1, dp)]

    near = [x for x in range(n) if bin(x >> 1).count("1") < 2]
    far = [x for x in range(n) if x not in near]
    queue = [0, 1] + [x for x in near if x > 1 and x % 2 == 0]
    queue += [x for x in near if x > 1 and x % 2 == 1] + far
    place = [queue.index(x) for x in range(n)]

    def fetch(source, target, sem, first, last):
        def step(i, carry):
            at = pl.ds(pl.multiple_of(i * edge, edge), edge)
            pltpu.make_async_copy(source.at[:, at], target.at[i], sem).start()
            return carry
        lax.fori_loop(first, last, step, 0)

    def blocks_wait(count, sem):
        if count <= maxb:
            blocks = tiles_v.at[0, pl.ds(0, count)]
        else:
            blocks = tiles_v.at[pl.ds(0, count // maxb)]
        pltpu.make_async_copy(blocks, blocks, sem).wait()

    barrier = pltpu.get_barrier_semaphore()
    for peer in greeted:
        pl.semaphore_signal(barrier, inc=1, device_id={"dp": peer}, device_id_type=MESH)
    for x in range(n - 1, 0, -1):
        pl.semaphore_signal(
            barrier, inc=1, device_id={"fsdp": relative(x)}, device_id_type=MESH
        )
    rows_copy = pltpu.make_async_copy(rows_hbm, rows_s, in_sem.at[2])
    rows_copy.start()
    cols_copy = pltpu.make_async_copy(cols_hbm, cols_s, in_sem.at[3])
    cols_copy.start()
    own_copy = pltpu.make_async_copy(tiles_hbm, tiles_v.at[0], in_sem.at[7])
    own_copy.start()

    early = hid_v.shape[0] * 3 // 8
    fetch(cot_hbm, cot_v, in_sem.at[1], 0, cot_v.shape[0])
    fetch(hid_hbm, hid_v, in_sem.at[0], 0, early)

    lane = lax.broadcasted_iota(jnp.int32, (8, 128), 1)
    sub = lax.broadcasted_iota(jnp.int32, (8, 128), 0)
    meta = jnp.where(sub == 2, cnt_s[0], 0)
    rows_copy.wait()
    cols_copy.wait()
    for j in range(maxb):
        here = lax.rem(lane, maxb) == j
        meta = jnp.where((sub == 0) & here, rows_s[j], meta)
        meta = jnp.where((sub == 1) & here, cols_s[j], meta)
    meta_v[0] = meta
    pl.semaphore_wait(barrier, n - 1 + len(greeted))
    if dp == 4:
        pl.semaphore_signal(ready, inc=1, device_id={"dp": z_near}, device_id_type=MESH)

    for x in near[:0:-1] + far:
        pltpu.make_async_remote_copy(
            meta_v.at[0], meta_v.at[place[x]], send_sem.at[0], meta_rs.at[int(x in far)],
            device_id={"fsdp": relative(x)}, device_id_type=MESH,
        ).start()
    own_copy.wait()

    ag_done = set()

    def ag_index(i, e, h):
        split = 0 < i < chip_bits and e == 0
        keys = [(i, e, h) for i in range(stages) for e in range(2 ** i) for h in range(2)
                if h == 0 or (0 < i < chip_bits and e == 0)]
        return keys.index((i, e, h if split else 0)), maxb // 2 if split else maxb

    def ag_send(p, i, e, h):
        bits = orders[p] + [0]
        owner = 0
        for t in range(len(bits)):
            if (e >> t) & 1:
                owner |= 1 << bits[t]
        part = pl.ds(p * half + h * (half // 2), half // 2)
        pltpu.make_async_remote_copy(
            tiles_v.at[place[owner], part], tiles_v.at[place[owner | (1 << bits[i])], part],
            send_sem.at[1], ag_rs.at[ag_index(i, e, h)[0]],
            device_id={"fsdp": relative(1 << bits[i])}, device_id_type=MESH,
        ).start()

    def ag_wait(i, e, h):
        index, count = ag_index(i, e, h)
        if index not in ag_done:
            ag_done.add(index)
            blocks_wait(count, ag_rs.at[index])

    for i in range(stages):
        for p in range(2):
            for h in range(2):
                if h == 0 or i == 0 or i == chip_bits:
                    ag_send(p, i, 0, h)

    grad_q[slots] = jnp.zeros(grad_q.shape[1:], F32)
    layer_q[slots] = jnp.zeros(layer_q.shape[1:], F32)
    grad_out[slots] = jnp.zeros(grad_out.shape[1:], BF16)
    layer_out[slots] = jnp.zeros(layer_out.shape[1:], BF16)

    fetch(hid_hbm, hid_v, in_sem.at[0], early, hid_v.shape[0])

    def collect(xs, full):
        arrive = [x for x in xs if x]
        first = min(place[x] for x in arrive)
        metas = meta_v.at[pl.ds(first, len(arrive))]
        pltpu.make_async_copy(metas, metas, meta_rs.at[int(xs is far)]).wait()
        for x in xs:
            full = jnp.where(lane // maxb == place[x], meta_v[place[x]], full)
        return full

    def to_smem(k):
        return pltpu.make_async_copy(full_v.at[k], full_s.at[k], in_sem.at[4 + k])

    known = collect(near, jnp.zeros((8, 128), jnp.int32))
    full_v[0] = known
    to_smem(0).start()

    def term(x, j, named=None):
        q = place[x] * maxb + j
        k = 0 if x in near else 1
        row = full_s[k, 0, q] if named is None else named[0, q]
        col = full_s[k, 1, q] if named is None else named[1, q]
        return lax.dot_general(
            hid_v[row], cot_v[col],
            (((0,), (0,)), ((), ())), preferred_element_type=F32,
        )

    def owner_at(p, e):
        owner = 0
        for t, b in enumerate(orders[p]):
            if not (e >> (chip_bits - 1 - t)) & 1:
                owner |= 1 << b
        return owner

    offsets = [0]
    for t in range(stages):
        offsets.append(offsets[-1] + (n >> (t + 1)))

    def pair_copy(p, e):
        return pltpu.make_async_remote_copy(
            sbuf.at[p, e], rbuf.at[p, e], send_sem.at[2], pair_rs.at[e],
            device_id={"fsdp": relative(1)}, device_id_type=MESH,
        )

    def rs_copy(p, t, e, c):
        where = offsets[t] + e
        return pltpu.make_async_remote_copy(
            sbuf.at[p, where, c], rbuf.at[p, where, c],
            send_sem.at[2], rs_rs.at[t - 1, c],
            device_id={"fsdp": relative(1 << orders[p][t - 1])}, device_id_type=MESH,
        )

    def foreign(e, named=None):
        for p in range(2):
            for c in range(half):
                sbuf[p, e, c] = term(owner_at(p, e) | 1, p * half + c, named).astype(BF16)
        for p in range(2):
            pair_copy(p, e).start()

    def own(e):
        for p in range(2):
            for c in range(half):
                acc[p, e, c] = term(owner_at(p, e), p * half + c)

    starts = [0]
    for t in range(stages):
        starts.append(starts[-1] + (n >> (t + 1)) // 2)

    paired = set()

    def pair_wait(e):
        if e not in paired:
            paired.add(e)
            blocks_wait(maxb, pair_rs.at[e])

    def pass_on(e, cs):
        for p in range(2):
            pair_wait(e)
            for c in cs:
                total = acc[p, e, c] + rbuf[p, e, c].astype(F32)
                sbuf[p, offsets[1] + e, c] = total.astype(BF16)
            for c in cs:
                rs_copy(p, 1, e, c).start()

    def reduce_step(t, c):
        m = n >> (t + 1)
        blocks_wait(2 * m, rs_rs.at[t - 1, c])
        for e in range(m):
            for p in range(2):
                at_e = starts[t] + e
                total = acc[p, at_e, c] + rbuf[p, offsets[t] + e, c].astype(F32)
                if t == 1:
                    total = total + rbuf[p, at_e, c].astype(F32)
                if e < m // 2:
                    sbuf[p, offsets[t + 1] + e, c] = total.astype(BF16)
                    rs_copy(p, t + 1, e, c).start()
                elif m > 1:
                    acc[p, at_e, c] = total
                else:
                    at = pl.ds(p * edge, edge)
                    fin[c, at] = total
                    zs[c, at] = total.astype(BF16)
        if m == 1:
            for r in range(1, dp):
                z_copy(c, r).start()

    def z_rows(index):
        return pl.ds(pl.multiple_of(index * rows_z, rows_z), rows_z)

    def z_copy(c, r):
        return pltpu.make_async_remote_copy(
            zs.at[c, z_rows(z_peer(r))], zr.at[c, r - 1], send_sem.at[3], z_rs.at[c],
            device_id={"dp": z_peer(r)}, device_id_type=MESH,
        )

    def a_copy(c, piece, peer, sem):
        return pltpu.make_async_remote_copy(
            za.at[c, z_rows(piece)], za.at[c, z_rows(piece)], send_sem.at[4], sem,
            device_id={"dp": peer}, device_id_type=MESH,
        )

    handed = half // 2 if dp == 4 else 0

    def z_sum(c, squares):
        piece = fin[c, z_rows(z)]
        pltpu.make_async_copy(zr.at[c], zr.at[c], z_rs.at[c]).wait()
        for r in range(1, dp):
            piece = piece + zr[c, r - 1].astype(F32)
        row = z * rows_z + lax.broadcasted_iota(jnp.int32, piece.shape, 0)
        slot = (row // edge) * half + c
        piece = piece * jnp.clip(cnt_s[0] - slot, 0, 1).astype(F32)
        za[c, z_rows(z)] = piece.astype(BF16)
        return squares + jnp.sum((piece * piece).reshape(-1, 8, 128), axis=0)

    def a_send(c):
        for r in range(1, dp):
            a_copy(c, z, z_peer(r), za_rs).start()

    def a_cross(c):
        a_copy(c, z, z_far, zf_rs.at[c]).start()
        a_copy(c, z, z_near, zb_rs).start()

    def a_hand(c):
        a_copy(c, z, z_far, zf_rs.at[c]).wait_recv()
        a_copy(c, z_far, z_near, zb_rs).start()

    def z_step(c, squares):
        squares = z_sum(c, squares)
        a_send(c)
        return squares

    def project(at):
        def load(j):
            q = at * maxb + j
            backward = lax.dot_general(
                cot_v[full_s[1, 1, q]], tiles_v[at, j], (((1,), (1,)), ((), ())),
                preferred_element_type=F32,
            )
            forward = jnp.dot(hid_v[full_s[1, 0, q]], tiles_v[at, j], preferred_element_type=F32)
            return q, backward, forward
        for j in range(maxb):
            q, backward, forward = load(j)
            backward = backward + grad_q[table_s[0, q]]
            grad_q[q] = backward
            grad_out[q] = backward.astype(BF16)
            forward = forward + layer_q[table_s[1, q]]
            layer_q[q] = forward
            layer_out[q] = forward.astype(BF16)

    def arrived(x):
        for p in range(2):
            bits = orders[p] + [0]
            index = [t for t in range(stages) if (x >> bits[t]) & 1]
            if index:
                e = sum(1 << t for t in index[:-1])
                for h in range(2):
                    ag_wait(index[-1], e, h)

    sent = sorted(range(chips // 2), key=lambda e: bin(owner_at(0, e)).count("1"))
    kept = list(range(chips // 2, chips))
    pltpu.make_async_copy(cot_v, cot_v, in_sem.at[1]).wait()
    pltpu.make_async_copy(hid_v, hid_v, in_sem.at[0]).wait()
    foreign(sent[0], known)
    to_smem(0).wait()
    full = collect(far, known)
    full_v[1] = full
    to_smem(1).start()
    for e in sent[1:]:
        foreign(e, full)
    own(sent[0])
    to_smem(1).wait()
    pass_on(sent[0], [0, 1])
    for e in sent[1:]:
        own(e)
    foreign(kept[0])
    for e in sent[1:]:
        pass_on(e, [0, 1])
    for c in range(2, half - 1):
        for e in sent:
            pass_on(e, [c])
    for e in kept[1:]:
        foreign(e)

    wide = lax.broadcasted_iota(jnp.int32, (slots, 128), 1)
    tall = lax.broadcasted_iota(jnp.int32, (slots, 128), 0)
    alive = lax.rem(lane[0:1], maxb) < full[2:3]
    table = jnp.full((8, 128), slots, jnp.int32)
    for k in range(2):
        named = jnp.broadcast_to(jnp.where(alive, full[k:k + 1], -1), (slots, 128))
        named_t = jnp.sum(jnp.where(wide == tall, named, 0), axis=1, keepdims=True)
        before = jnp.max(
            jnp.where((named_t == named) & (tall < wide), tall, -1), axis=0, keepdims=True
        )
        last = jnp.max(jnp.where(named_t == wide, tall, -1), axis=0, keepdims=True)
        table = jnp.where(sub == k, jnp.where(before < 0, slots, before), table)
        table = jnp.where(sub == 2 + k, jnp.where(last < 0, slots, last), table)
    table_v[...] = table
    table_copy = pltpu.make_async_copy(table_v, table_s, in_sem.at[6])
    table_copy.start()
    for e in kept:
        own(e)
    table_copy.wait()

    def project_all(xs):
        for x in xs:
            arrived(x)
        first = place[xs[0]]

        def one(at, carry):
            project(at)
            return carry

        lax.fori_loop(first, first + len(xs), one, 0)

    def ag_pass(i, e, h):
        ag_wait(i, e, h)
        for p in range(2):
            ag_send(p, chip_bits, e + 2 ** i, h)

    project_all([0, 1])
    for h in range(2):
        for i in range(chip_bits if h == 0 else 1):
            ag_pass(i, 0, h)
    for e in kept:
        pair_wait(e)
    reduce_step(1, 0)
    for e in sent:
        pass_on(e, [half - 1])

    def second(c, carry):
        reduce_step(1, c)
        return carry

    lax.fori_loop(1, half - 1, second, 0)
    if dp == 4:
        pl.semaphore_wait(ready, 1)
    for t in range(2, stages):
        reduce_step(t, 0)
    reduce_step(1, half - 1)
    for t in range(2, stages):
        def third(c, carry):
            reduce_step(t, c)
            return carry

        lax.fori_loop(1, half, third, 0)

    for i in range(1, chip_bits):
        for p in range(2):
            ag_send(p, i, 0, 1)
    for i in range(1, chip_bits):
        for e in range(1, 2 ** i):
            for p in range(2):
                for h in range(2):
                    ag_wait(i - 1, e - 2 ** (i - 1), h)
                    ag_send(p, i, e, h)

    squares = lax.fori_loop(0, handed, z_sum, jnp.zeros((8, 128), F32))
    for c in range(handed):
        a_cross(c)
    squares = lax.fori_loop(handed, half // 2, z_step, squares)
    for i in range(1, chip_bits):
        ag_pass(i, 0, 1)
    project_all([x for x in near if x > 1 and x % 2 == 0])
    squares = lax.fori_loop(half // 2, half - 1, z_step, squares)
    squares = z_sum(half - 1, squares)
    device = me * dp + z
    sqf[device] = jnp.sum(squares, axis=0, keepdims=True)
    for x in reversed(queue):
        for r in range(dp):
            if x or r:
                pltpu.make_async_remote_copy(
                    sqf.at[device], sqf.at[device], send_sem.at[5], sq_rs,
                    device_id={"fsdp": relative(x), "dp": z_peer(r)}, device_id_type=MESH,
                ).start()
    a_send(half - 1)
    for i in range(1, chip_bits):
        for e in range(1, 2 ** i):
            for h in range(2):
                ag_pass(i, e, h)
    crossed = [x for x in near if x > 1 and x % 2 == 1]
    project_all(crossed)
    for c in range(handed):
        a_hand(c)
    project_all(far)

    entries = full_s[1, 2, 0]
    for x in range(1, n):
        entries = entries + full_s[1, 2, x * maxb]
    others = sqf.at[pl.ds(0, n * dp - 1)]
    pltpu.make_async_copy(others, others, sq_rs).wait()
    squares = jnp.sum(jnp.sum(sqf[...], axis=0), axis=1, keepdims=True)
    live = jnp.full((1, 1), entries, jnp.int32).astype(F32) * edge * edge
    spread = jnp.sqrt(squares / live)
    factor = jnp.minimum(1.0, 0.5 * root / spread) / root

    if handed:
        twice = za.at[pl.ds(0, handed)]
        pltpu.make_async_copy(twice.at[:, pl.ds(0, 2 * rows_z)], twice.at[:, pl.ds(0, 2 * rows_z)], zb_rs).wait()
    direct = zr.at[pl.ds(handed, half - handed)]
    pltpu.make_async_copy(direct, direct, za_rs).wait()

    def finish(c, carry):
        for p in range(2):
            wg_out[p * half + c] = za[c, pl.ds(p * edge, edge)].astype(F32) * factor
        return carry

    lax.fori_loop(0, half, finish, 0)

    metas = meta_v.at[pl.ds(1, n - 1)]
    gathered = tiles_v.at[pl.ds(1, n - 1)]
    for k, sent in enumerate((metas, gathered, sbuf, zr, zr, others)):
        pltpu.make_async_copy(sent, sent, send_sem.at[k]).wait()


def write_kernel(
    grad_v, layer_v, wg_v, table_s,
    layer_hbm, grad_hbm, wg_hbm,
    w_sem, g_sem, l_sem,
):
    edge = grad_v.shape[2]

    def write(row, source, target, sem):
        def step(i, carry):
            at = pl.ds(pl.multiple_of(i * edge, edge), edge)
            pltpu.make_async_copy(source.at[table_s[row, i]], target.at[:, at], sem).start()
            return carry
        lax.fori_loop(0, target.shape[1] // edge, step, 0)

    write(2, grad_v, grad_hbm, g_sem)
    write(3, layer_v, layer_hbm, l_sem)
    wg_copy = pltpu.make_async_copy(wg_v, wg_hbm, w_sem)
    wg_copy.start()
    pltpu.make_async_copy(grad_hbm, grad_hbm, g_sem).wait()
    pltpu.make_async_copy(layer_hbm, layer_hbm, l_sem).wait()
    wg_copy.wait()


def fused(n, dp, hidden, cotangent, tiles, tile_rows, tile_cols, counts):
    tokens, width_ff = hidden.shape
    maxb, edge, _ = tiles.shape
    root = math.sqrt(tokens * n * dp)
    slots, half, stages = n * maxb, maxb // 2, n.bit_length() - 1
    in_hbm = functools.partial(pltpu.with_memory_space_constraint, memory_space=pltpu.HBM)
    rows_z = 2 * edge // dp
    hbm = pl.BlockSpec(memory_space=pltpu.HBM)
    smem = pl.BlockSpec(memory_space=pltpu.SMEM)
    vmem = pl.BlockSpec(memory_space=pltpu.VMEM)
    dma = pltpu.SemaphoreType.DMA
    grad, layer, weight, table = pl.pallas_call(
        functools.partial(fused_kernel, n, dp, root),
        out_shape=(
            pltpu.VMEM((slots + 1, tokens, edge), BF16),
            pltpu.VMEM((slots + 1, tokens, edge), BF16),
            pltpu.VMEM((maxb, edge, edge), F32),
            pltpu.SMEM((8, 128), jnp.int32),
        ),
        in_specs=[hbm, hbm, smem, hbm, hbm, hbm],
        out_specs=(vmem, vmem, vmem, smem),
        scratch_shapes=[
            pltpu.SMEM(tile_rows.shape, jnp.int32),
            pltpu.SMEM(tile_cols.shape, jnp.int32),
            pltpu.VMEM((hidden.shape[1] // edge, tokens, edge), BF16),
            pltpu.VMEM((cotangent.shape[1] // edge, tokens, edge), BF16),
            pltpu.VMEM((n, maxb, edge, edge), BF16),
            pltpu.VMEM((n, 8, 128), jnp.int32),
            pltpu.VMEM((2, 8, 128), jnp.int32),
            pltpu.SMEM((2, 8, 128), jnp.int32),
            pltpu.VMEM((8, 128), jnp.int32),
            pltpu.VMEM((2, n // 2, half, edge, edge), F32),
            pltpu.VMEM((2, n - 1, half, edge, edge), BF16),
            pltpu.VMEM((2, n - 1, half, edge, edge), BF16),
            pltpu.VMEM((half, 2 * edge, edge), F32),
            pltpu.VMEM((half, 2 * edge, edge), BF16),
            pltpu.VMEM((half, dp - 1, rows_z, edge), BF16),
            pltpu.VMEM((half, 2 * edge, edge), BF16),
            pltpu.VMEM((n * dp, 1, 128), F32),
            pltpu.VMEM((slots + 1, tokens, edge), F32),
            pltpu.VMEM((slots + 1, tokens, edge), F32),
            dma((8,)), dma((6,)), dma((2,)),
            dma((n - 1 + max(stages - 2, 0),)),
            dma((n // 2,)), dma((stages - 1, half)), dma((half,)), dma, dma, dma((half,)), dma,
            pltpu.SemaphoreType.REGULAR,
        ],
        compiler_params=pltpu.CompilerParams(
            collective_id=0, has_side_effects=True, vmem_limit_bytes=44 * 2 ** 20
        ),
        name="fused",
    )(in_hbm(tile_rows), in_hbm(tile_cols), counts, in_hbm(tiles), in_hbm(hidden), in_hbm(cotangent))
    return pl.pallas_call(
        write_kernel,
        out_shape=(
            jax.ShapeDtypeStruct(cotangent.shape, BF16),
            jax.ShapeDtypeStruct(hidden.shape, BF16),
            jax.ShapeDtypeStruct(tiles.shape, F32),
        ),
        in_specs=[vmem, vmem, vmem, smem],
        out_specs=(hbm, hbm, hbm),
        scratch_shapes=[dma, dma, dma],
        compiler_params=pltpu.CompilerParams(vmem_limit_bytes=16 * 2 ** 20),
        name="write",
    )(grad, layer, weight, table)


def shards(n, dp, hidden, cotangent, tiles, tile_rows, tile_cols, counts):
    tokens, width_ff = hidden.shape
    width_model = cotangent.shape[1]
    maxb, edge, _ = tiles.shape
    blocks_ff, blocks_model = width_ff // edge, width_model // edge
    root = math.sqrt(tokens * n * dp)
    half, per = maxb // 2, maxb // dp
    sums = n * maxb * tokens * edge * 12
    if n == 8 and dp % 2 == 0 and max(n * maxb, blocks_ff, blocks_model) <= 128 and sums <= 28 * 2 ** 20:
        return fused(n, dp, hidden, cotangent, tiles, tile_rows, tile_cols, counts)
    hbm = pl.BlockSpec(memory_space=pl.ANY)
    smem = pl.BlockSpec(memory_space=pltpu.SMEM)
    vmem = pl.BlockSpec(memory_space=pltpu.VMEM)
    dma = pltpu.SemaphoreType.DMA
    meta, gathered, weight_grad = pl.pallas_call(
        functools.partial(exchange_kernel, n, dp, root),
        out_shape=(
            jax.ShapeDtypeStruct((n, 8, 128), jnp.int32),
            jax.ShapeDtypeStruct((n, maxb, edge, edge), BF16),
            jax.ShapeDtypeStruct((maxb, edge, edge), F32),
        ),
        in_specs=[smem, smem, smem, hbm, hbm, hbm],
        out_specs=(hbm, hbm, vmem),
        scratch_shapes=[
            pltpu.VMEM((blocks_ff, tokens, edge), BF16),
            pltpu.VMEM((blocks_model, tokens, edge), BF16),
            pltpu.VMEM((n, maxb, edge, edge), BF16),
            pltpu.VMEM((n, 8, 128), jnp.int32),
            pltpu.SMEM((n, 8, 128), jnp.int32),
            pltpu.VMEM((2, n // 2, half, edge, edge), F32),
            pltpu.VMEM((2, n - 1, half, edge, edge), BF16),
            pltpu.VMEM((2, n - 1, half, edge, edge), BF16),
            pltpu.VMEM((maxb, edge, edge), F32),
            pltpu.VMEM((dp, per, edge, edge), BF16),
            pltpu.VMEM((dp - 1, per, edge, edge), BF16),
            pltpu.VMEM((dp, per, edge, edge), BF16),
            pltpu.VMEM((dp, 8, 128), F32),
            pltpu.VMEM((n, 8, 128), F32),
            dma((4,)), dma((2,)),
            dma((n - 1,)), dma((n - 1,)),
            dma((2, n - 1)), dma((2, n - 1)),
            dma((2, n - 1)), dma((2, n - 1)),
            dma((dp - 1,)), dma((dp - 1,)),
            dma((dp - 1,)), dma((dp - 1,)),
            dma((dp - 1,)), dma((dp - 1,)),
            dma((n - 1,)), dma((n - 1,)),
        ],
        compiler_params=pltpu.CompilerParams(
            collective_id=0, has_side_effects=True, vmem_limit_bytes=60 * 2 ** 20
        ),
        name="exchange",
    )(tile_rows, tile_cols, counts, tiles, hidden, cotangent)

    layer_out, hidden_grad = pl.pallas_call(
        functools.partial(project_kernel, n, maxb),
        out_shape=(
            jax.ShapeDtypeStruct(cotangent.shape, BF16),
            jax.ShapeDtypeStruct(hidden.shape, BF16),
        ),
        in_specs=[smem, hbm, hbm, hbm],
        out_specs=(hbm, hbm),
        scratch_shapes=[
            pltpu.VMEM((n, maxb, edge, edge), BF16),
            pltpu.VMEM(cotangent.shape, BF16),
            pltpu.VMEM((n, maxb, tokens, edge), BF16),
            pltpu.VMEM((blocks_ff, tokens, edge), F32),
            pltpu.VMEM((blocks_ff, tokens, edge), BF16),
            pltpu.VMEM((blocks_model, tokens, edge), F32),
            pltpu.VMEM((blocks_model, tokens, edge), BF16),
            pltpu.VMEM((tokens, edge), BF16),
            pltpu.VMEM((maxb, tokens, edge), F32),
            pltpu.SMEM((blocks_ff,), jnp.int32),
            pltpu.SMEM((blocks_ff,), jnp.int32),
            pltpu.SMEM((blocks_model,), jnp.int32),
            pltpu.SMEM((blocks_model,), jnp.int32),
            dma((2,)), dma, dma, dma,
        ],
        compiler_params=pltpu.CompilerParams(vmem_limit_bytes=62 * 2 ** 20),
        name="project",
    )(meta, gathered, hidden, cotangent)
    return layer_out, hidden_grad, weight_grad


def solution(mesh):
    placed = (
        P(("fsdp", "dp"), None),
        P(("fsdp", "dp"), None),
        P("fsdp", None, None),
        P("fsdp"),
        P("fsdp"),
        P("fsdp"),
    )
    return jax.shard_map(
        functools.partial(shards, mesh.shape["fsdp"], mesh.shape["dp"]),
        mesh=mesh,
        in_specs=placed,
        out_specs=(P(("fsdp", "dp"), None), P(("fsdp", "dp"), None), P("fsdp", None, None)),
        check_vma=False,
    )
```
